32 devices in a mesh: dp: 8 (over z, core), ctx: 4 (over y, x).
Axes of the slice: x: 2, y: 2, z: 4, core: 2. Of those that a mesh axis runs over, the one named last changes fastest.
Arguments:
- state_rows: bfloat16 [12288, 2048], P(('dp', 'ctx')), parts along dimension 0, may hold values from -6 to 6
- query_vectors: bfloat16 [8, 12288, 128], P(None, ('dp', 'ctx')), parts along dimension 1, may hold values from -6 to 6
- key_vectors: bfloat16 [8, 12288, 128], P(None, ('dp', 'ctx')), parts along dimension 1, may hold values from -6 to 6
- value_vectors: bfloat16 [8, 12288, 128], P(None, ('dp', 'ctx')), parts along dimension 1, may hold values from -24 to 24
- halt_counts: int32 [12288], P(('dp', 'ctx')), parts along dimension 0, may hold values from 1 to 6, as said below
- out_weight: bfloat16 [8, 128, 2048], replicated, may hold values from -0.75 to 0.75
- norm_gain: bfloat16 [2048], replicated, may hold values from 0.099609375 to 1.8984375
Outputs:
- new_state: bfloat16 [12288, 2048], P(('dp', 'ctx')), parts along dimension 0
The draws below stay inside these ranges and needn't reach their ends.
There are 8 independent parts, one for each index of `dp`. The reference program is written for one: setup_inputs(seed, part) draws one part's arguments, and reference() takes and returns one part's arrays. A program takes and returns all parts, laid end to end along the dimension named above; an argument that names none is the same for every part. Nothing has to cross between parts.
Inputs may be any that keep to these rules, and one draw needn't show every extreme that they name: halt_counts is equal within each aligned tile of 128 positions; exactly 3 tiles of a document have counts above 2, and on some device of ctx all 3 tiles do.
All inputs are finite; a program needn't handle non-finite values.
Results may differ from the reference program's by a relative error of at most 0.008.
Values may be sent and summed in bfloat16 or wider, within the bound.
A program may use at most 128 MiB of HBM per device.

```python
import jax
import jax.numpy as jnp
from jax import lax

D = 2048
HEADS = 8
DH = 128
TILE = 128
STEP = 2
MAXSTEPS = 6
LEN = 1536
TILES_DEV = 3
ACTIVE = 3
HW = 1024
N_CTX = 4


def drawn_pair(key):
    key_query, key_key = jax.random.split(jax.random.fold_in(key, 7), 2)
    queries = jnp.clip(jax.random.normal(key_query, (HEADS, LEN, DH), jnp.float32), -6.0, 6.0)
    keys_all = jnp.clip(jax.random.normal(key_key, (HEADS, LEN, DH), jnp.float32), -6.0, 6.0)
    return (queries, keys_all)


def draw_query_vectors(key, part):
    return drawn_pair(key)[0].astype(jnp.bfloat16)


def draw_key_vectors(key, part):
    return drawn_pair(key)[1].astype(jnp.bfloat16)


def draw_halt_counts(key, part):
    key_priority, key_high, key_low, key_full = jax.random.split(jax.random.fold_in(key, 11), 4)
    tile_total = TILES_DEV * N_CTX
    full_device = jax.random.randint(key_full, (), 0, N_CTX)
    priority = jax.random.permutation(key_priority, tile_total).astype(jnp.int32)
    tile_device = jnp.arange(tile_total) // TILES_DEV
    priority = jnp.where(tile_device == full_device, -1, priority)
    ordering = jnp.argsort(priority, stable=True)
    active = jnp.zeros((tile_total,), jnp.int32).at[ordering[:ACTIVE]].set(1)
    high_counts = jax.random.randint(key_high, (tile_total,), STEP + 1, MAXSTEPS + 1)
    low_counts = jax.random.randint(key_low, (tile_total,), 1, STEP + 1)
    tile_counts = jnp.where(active == 1, high_counts, low_counts).astype(jnp.int32)
    return jnp.repeat(tile_counts, TILE, total_repeat_length=LEN)


def shard_levels(key, extent, shards, smallest, largest):
    gain = 1.0
    for position, parts in shards:
        heights = jax.random.uniform(jax.random.fold_in(jax.random.fold_in(key, 6), position), (parts,), jnp.float32, smallest / len(shards), largest / len(shards))
        gain = gain * jnp.repeat(jnp.exp(heights), extent[position] // parts).reshape((-1,) + (1,) * (len(extent) - 1 - position))
    return gain


def scatter_about(key, dims, deviation, bound, cuts=(), kind=jnp.bfloat16):
    result = jax.random.normal(key, dims, jnp.float32) * deviation
    if len(cuts) > 0:
        result = shard_levels(key, dims, cuts, -0.22, 0.18) * result
    return jnp.clip(result, min=-bound, max=bound).astype(kind)


def setup_inputs(seed: int = 0, part: int = 0) -> dict:
    key_list = jax.random.split(jax.random.key(seed), 8)
    own_keys = jax.random.split(jax.random.fold_in(key_list[7], part), 8)
    state_rows = scatter_about(own_keys[0], (LEN, D), 1.0, 6.0, ((0, 4),))
    query_vectors = draw_query_vectors(jax.random.fold_in(jax.random.fold_in(key_list[7], part), 71), part)
    key_vectors = draw_key_vectors(jax.random.fold_in(jax.random.fold_in(key_list[7], part), 71), part)
    value_vectors = scatter_about(own_keys[3], (HEADS, LEN, DH), 4.0, 24.0, ((1, 4),))
    halt_counts = draw_halt_counts(jax.random.fold_in(jax.random.fold_in(key_list[7], part), 71), part)
    out_weight = scatter_about(key_list[5], (HEADS, DH, D), (HW // 16) ** -0.5, 0.75)
    norm_gain = jnp.clip(1.0 + 0.18 * jax.random.normal(key_list[6], (D,), jnp.float32), 0.099609375, 1.8984375).astype(jnp.bfloat16)
    return {"state_rows": state_rows, "query_vectors": query_vectors, "key_vectors": key_vectors, "value_vectors": value_vectors, "halt_counts": halt_counts, "out_weight": out_weight, "norm_gain": norm_gain}


def reference(state_rows, query_vectors, key_vectors, value_vectors, halt_counts, out_weight, norm_gain):
    score_scale = DH ** (-0.5)

    def per_head(head_items):
        query_head, key_head, value_head = head_items
        scores = lax.dot_general(query_head, key_head, (((1,), (1,)), ((), ())), preferred_element_type=jnp.float32) * score_scale
        new_max = lax.optimization_barrier(jnp.max(scores, axis=1, keepdims=True))
        exponents = jnp.exp(scores - new_max)
        weight_sum = lax.optimization_barrier(jnp.sum(exponents, axis=1))
        weighted = jnp.dot(exponents.astype(jnp.bfloat16), value_head, preferred_element_type=jnp.float32)
        return (weighted / weight_sum[:, None]).astype(jnp.bfloat16)
    attended = lax.map(per_head, (query_vectors, key_vectors, value_vectors))
    update = jnp.einsum('hqd,hde->qe', attended.astype(jnp.float32), out_weight.astype(jnp.float32))
    mixed_sum = state_rows.astype(jnp.float32) + update
    normed = mixed_sum * lax.rsqrt(lax.optimization_barrier(jnp.mean(mixed_sum * mixed_sum, axis=-1, keepdims=True)) + 1e-06) * norm_gain.astype(jnp.float32)
    active = (halt_counts > STEP)[:, None]
    return jnp.where(active, normed.astype(jnp.bfloat16), state_rows)
```

```python
import functools

import jax
import jax.numpy as jnp
from jax import lax
from jax.experimental import pallas as pl
from jax.experimental.pallas import tpu as pltpu
from jax.sharding import PartitionSpec as P

STEP = 2
TILE = 128
LOG2E = 1.4426950408889634


def peer_of(me, step, n):
    peer = 0
    bit = 1
    while bit < n:
        digit = (me // bit) % 2
        if step & bit:
            digit = (digit + 1) % 2
        peer = peer + digit * bit
        bit *= 2
    return peer


def split_kernel(
    n,
    share,
    halt_ref,
    q_hbm,
    k_hbm,
    v_hbm,
    state_hbm,
    w_hbm,
    gain_ref,
    out_ref,
    q_buf,
    k_buf,
    v_buf,
    flag_out,
    flag_buf,
    state_buf,
    w_buf,
    probs,
    inv_sum,
    att_buf,
    update,
    send_sem,
    recv_sem,
    flag_send,
    flag_recv,
    att_send,
    att_recv,
    local_sem,
    w_sem,
    state_sem,
):
    me = lax.axis_index("ctx")
    rows, width = q_hbm.shape[1], q_hbm.shape[2]
    blocks = rows // TILE
    scale = width ** (-0.5) * LOG2E
    peers = [peer_of(me, step, n) for step in range(n)]
    order = list(range(n - 1, 0, -1))
    tensors = ((k_hbm, k_buf), (q_hbm, q_buf), (v_hbm, v_buf))
    own_rows = pl.ds(pl.multiple_of(me * rows, rows), rows)
    own_lanes = pl.ds(pl.multiple_of(me * width, width), width)

    flag = jnp.full(flag_out.shape, halt_ref[0] > STEP).astype(jnp.float32)
    flag_out[...] = flag

    own = {}
    for h in range(share):
        for index, (src, buf) in enumerate(tensors):
            own[index, h] = pltpu.make_async_copy(
                src.at[me * share + h], buf.at[h, own_rows], local_sem.at[index, h]
            )
            own[index, h].start()

    barrier = pltpu.get_barrier_semaphore()
    for step in range(1, n):
        pl.semaphore_signal(
            barrier, inc=1, device_id={"ctx": peers[step]}, device_id_type=pl.DeviceIdType.MESH
        )
    pl.semaphore_wait(barrier, n - 1)

    def remote(src, dst, send, recv, step):
        copy = pltpu.make_async_remote_copy(
            src_ref=src,
            dst_ref=dst,
            send_sem=send,
            recv_sem=recv,
            device_id={"ctx": peers[step]},
            device_id_type=pl.DeviceIdType.MESH,
        )
        copy.start()
        return copy

    sends, flags, gathers = {}, {}, {}
    for h in range(share):
        for index, (src, buf) in enumerate(tensors):
            for step in order:
                sends[index, h, step] = remote(
                    src.at[peers[step] * share + h],
                    buf.at[h, own_rows],
                    send_sem.at[index, h, step],
                    recv_sem.at[index, h, step],
                    step,
                )
            if h == 0 and index == 0:
                for step in order:
                    flags[step] = remote(
                        flag_out, flag_buf.at[me], flag_send.at[step], flag_recv.at[step], step
                    )

    w_copies = []
    for head in range(n * share):
        w_copies.append(
            pltpu.make_async_copy(
                w_hbm.at[head],
                w_buf.at[head % share, pl.ds((head // share) * width, width)],
                w_sem.at[head],
            )
        )
        w_copies[-1].start()
    state_copy = pltpu.make_async_copy(state_hbm, state_buf, state_sem)
    state_copy.start()

    def arrived(index, h):
        own[index, h].wait()
        for step in order:
            sends[index, h, step].wait_recv()

    def gather(h, block):
        if block is None:
            cut, slot = pl.ds(0, rows), 0
        else:
            cut, slot = pl.ds(block * TILE, TILE), block
        for step in order:
            gathers[h, slot, step] = remote(
                att_buf.at[h, cut, own_lanes],
                att_buf.at[h, cut, own_lanes],
                att_send.at[h, slot, step],
                att_recv.at[h, slot, step],
                step,
            )

    for h in range(share):
        arrived(0, h)
        arrived(1, h)
        if h == 0:
            for step in order:
                flags[step].wait_recv()
        for block in range(blocks):
            base = block * TILE
            chosen = q_buf[h, pl.ds(pl.multiple_of(me * rows, rows) + base, TILE), :].astype(jnp.float32) * flag[0:1, :]
            for step in order:
                start = pl.multiple_of(peers[step] * rows, rows) + base
                term = q_buf[h, pl.ds(start, TILE), :].astype(jnp.float32)
                chosen = chosen + term * flag_buf[peers[step], 0:1, :]
            scores = lax.dot_general(
                chosen.astype(jnp.bfloat16),
                k_buf[h],
                (((1,), (1,)), ((), ())),
                preferred_element_type=jnp.float32,
            )
            top = jnp.max(scores, axis=1, keepdims=True)
            weights = jnp.exp2((scores - top) * scale)
            total = jnp.sum(weights, axis=1, keepdims=True)
            probs[base : base + TILE, :] = weights.astype(jnp.bfloat16)
            inv_sum[base : base + TILE, :] = jnp.broadcast_to(1.0 / total, (TILE, width))
        arrived(2, h)
        last = h == share - 1
        for block in range(blocks):
            cut = slice(block * TILE, (block + 1) * TILE)
            weighted = jnp.dot(probs[cut, :], v_buf[h], preferred_element_type=jnp.float32)
            att_buf[h, cut, own_lanes] = (weighted * inv_sum[cut, :]).astype(jnp.bfloat16)
            if last:
                gather(h, block)
        if not last:
            gather(h, None)

    for copy in w_copies:
        copy.wait()
    state_copy.wait()

    for h in range(share - 1):
        for step in order:
            gathers[h, 0, step].wait_recv()

        def body(block, carry, h=h):
            cut = pl.ds(pl.multiple_of(block * TILE, TILE), TILE)
            product = jnp.dot(att_buf[h, cut, :], w_buf[h], preferred_element_type=jnp.float32)
            if h == 0:
                update[cut, :] = state_buf[cut, :].astype(jnp.float32) + product
            else:
                update[cut, :] = update[cut, :] + product
            return carry

        lax.fori_loop(0, blocks, body, 0)

    gain = gain_ref[...].astype(jnp.float32).reshape(1, -1)
    h = share - 1
    for block in range(blocks):
        for step in order:
            gathers[h, block, step].wait_recv()
        cut = slice(block * TILE, (block + 1) * TILE)
        mixed = jnp.dot(att_buf[h, cut, :], w_buf[h], preferred_element_type=jnp.float32)
        residual = update if share > 1 else state_buf
        mixed = residual[cut, :].astype(jnp.float32) + mixed
        mean = jnp.mean(mixed * mixed, axis=-1, keepdims=True)
        normed = mixed * lax.rsqrt(mean + 1e-06) * gain
        active = jnp.full(normed.shape, halt_ref[block * TILE] > STEP)
        kept = state_buf[cut, :].astype(jnp.float32)
        out_ref[cut, :] = jnp.where(active, normed, kept).astype(out_ref.dtype)

    for group in (sends, flags, gathers):
        for copy in group.values():
            copy.wait_send()


def split_heads(n, state_rows, q, k, v, halt_counts, out_weight, norm_gain):
    heads, rows, width = q.shape
    share = heads // n
    features = state_rows.shape[1]
    bf16, f32 = jnp.bfloat16, jnp.float32
    hbm = pl.BlockSpec(memory_space=pltpu.MemorySpace.HBM)
    vmem = pl.BlockSpec(memory_space=pltpu.VMEM)
    block = pltpu.VMEM((share, n * rows, width), bf16)
    dma = pltpu.SemaphoreType.DMA
    new_state = pl.pallas_call(
        functools.partial(split_kernel, n, share),
        out_shape=jax.ShapeDtypeStruct((rows, features), bf16),
        in_specs=[pl.BlockSpec(memory_space=pltpu.SMEM)] + [hbm] * 5 + [vmem],
        out_specs=vmem,
        scratch_shapes=[
            block,
            block,
            block,
            pltpu.VMEM((8, 128), f32),
            pltpu.VMEM((n, 8, 128), f32),
            pltpu.VMEM((rows, features), bf16),
            pltpu.VMEM((share, n * width, features), bf16),
            pltpu.VMEM((rows, n * rows), bf16),
            pltpu.VMEM((rows, width), f32),
            pltpu.VMEM((share, rows, n * width), bf16),
            pltpu.VMEM((rows, features), f32),
            dma((3, share, n)),
            dma((3, share, n)),
            dma((n,)),
            dma((n,)),
            dma((share, rows // TILE, n)),
            dma((share, rows // TILE, n)),
            dma((3, share)),
            dma((heads,)),
            dma,
        ],
        compiler_params=pltpu.CompilerParams(
            collective_id=0, has_side_effects=True, vmem_limit_bytes=24 * 1024 * 1024
        ),
    )(halt_counts, *[pltpu.with_memory_space_constraint(x, pltpu.HBM) for x in (q, k, v, state_rows, out_weight)], norm_gain)
    return new_state


def fold_heads(carry, queries, key_piece, value_piece, score_scale):
    running_max, running_sum, weighted = carry

    def per_head(head_items):
        query_head, key_head, value_head, max_head, sum_head, weighted_head = head_items
        scores = (
            lax.dot_general(
                query_head, key_head, (((1,), (1,)), ((), ())), preferred_element_type=jnp.float32
            )
            * score_scale
        )
        new_max = jnp.maximum(max_head, jnp.max(scores, axis=1))
        shrink = jnp.exp(max_head - new_max)
        exponents = jnp.exp(scores - new_max[:, None])
        sum_head = sum_head * shrink + jnp.sum(exponents, axis=1)
        weighted_head = weighted_head * shrink[:, None] + jnp.dot(
            exponents.astype(jnp.bfloat16), value_head, preferred_element_type=jnp.float32
        )
        return (new_max, sum_head, weighted_head)

    return lax.map(per_head, (queries, key_piece, value_piece, running_max, running_sum, weighted))


def empty_carry(head_count, query_count, head_width):
    return (
        jnp.full((head_count, query_count), -1e30, jnp.float32),
        jnp.zeros((head_count, query_count), jnp.float32),
        jnp.zeros((head_count, query_count, head_width), jnp.float32),
    )


def attend_keys(query_vectors, key_vectors, value_vectors, score_scale):
    head_count, row_count, head_width = query_vectors.shape
    initial = empty_carry(head_count, row_count, head_width)
    running_max, running_sum, weighted = fold_heads(
        initial,
        query_vectors,
        lax.all_gather(key_vectors, "ctx", axis=1, tiled=True),
        lax.all_gather(value_vectors, "ctx", axis=1, tiled=True),
        score_scale,
    )
    return (weighted / running_sum[..., None]).astype(jnp.bfloat16)


def on_device(
    state_rows, query_vectors, key_vectors, value_vectors, halt_counts, out_weight, norm_gain
):
    head_count, row_count, head_width = query_vectors.shape
    score_scale = head_width ** (-0.5)
    attended = attend_keys(query_vectors, key_vectors, value_vectors, score_scale)
    update = jnp.einsum("hqd,hde->qe", attended, out_weight, preferred_element_type=jnp.float32)
    mixed_sum = state_rows.astype(jnp.float32) + update
    normed = (
        mixed_sum
        * lax.rsqrt(jnp.mean(mixed_sum * mixed_sum, axis=-1, keepdims=True) + 1e-06)
        * norm_gain.astype(jnp.float32)
    )
    active = (halt_counts > STEP)[:, None]
    return jnp.where(active, normed.astype(jnp.bfloat16), state_rows)


def solution(mesh):
    n_ctx = mesh.shape["ctx"]

    def per_device(state_rows, q, k, v, halt_counts, out_weight, norm_gain):
        heads, rows, _ = q.shape
        one_owner = rows == (n_ctx - 1) * TILE
        if one_owner and heads % n_ctx == 0 and n_ctx & (n_ctx - 1) == 0:
            return split_heads(n_ctx, state_rows, q, k, v, halt_counts, out_weight, norm_gain)
        return on_device(state_rows, q, k, v, halt_counts, out_weight, norm_gain)

    placed = (
        P(("dp", "ctx"), None),
        P(None, ("dp", "ctx"), None),
        P(None, ("dp", "ctx"), None),
        P(None, ("dp", "ctx"), None),
        P(("dp", "ctx")),
        P(),
        P(),
    )
    return jax.shard_map(
        per_device, mesh=mesh, in_specs=placed, out_specs=P(("dp", "ctx"), None), check_vma=False
    )
```

```python
import functools

import jax
import jax.numpy as jnp
from jax import lax
from jax.experimental import pallas as pl
from jax.experimental.pallas import tpu as pltpu
from jax.sharding import PartitionSpec as P

STEP = 2
TILE = 128
LOG2E = 1.4426950408889634


def square_kernel(
    share,
    halt_hbm,
    q_hbm,
    k_hbm,
    v_hbm,
    state_hbm,
    w_hbm,
    gain_hbm,
    out_ref,
    halt,
    gain_buf,
    q_buf,
    q_near,
    q_mid,
    q_far,
    k_buf,
    v_buf,
    own_acc,
    own_stat,
    part_out,
    part_in,
    stat_out,
    stat_in,
    att_own,
    att_in,
    state_buf,
    w_own,
    w_in,
    update,
    halt_sem,
    gain_sem,
    state_sem,
    q_sem,
    kv_sem,
    w_sem,
    send_sem,
    recv_sem,
):
    me = lax.axis_index("ctx")
    bits = (me % 2, me // 2)
    peer = (bits[1] * 2 + 1 - bits[0], (1 - bits[1]) * 2 + bits[0])
    rows, width = q_hbm.shape[1], q_hbm.shape[2]
    features = state_hbm.shape[1]
    scale = width ** (-0.5) * LOG2E
    axes = (0, 1)

    def head(s, a, owner):
        side = bits[s] if owner == 0 else 1 - bits[s]
        return (s * 2 + side) * share + a

    def local(src, dst, sem):
        copy = pltpu.make_async_copy(src, dst, sem)
        copy.start()
        return copy

    def remote(src, dst, kind, s, a, axis):
        copy = pltpu.make_async_remote_copy(
            src_ref=src,
            dst_ref=dst,
            send_sem=send_sem.at[kind, s, a],
            recv_sem=recv_sem.at[kind, s, a],
            device_id={"ctx": peer[axis]},
            device_id_type=pl.DeviceIdType.MESH,
        )
        copy.start()
        copies.append(copy)
        return copy

    copies = []
    halt_copy = local(halt_hbm, halt, halt_sem)
    q_copy = {}
    for owner in (1, 0):
        for a in range(share):
            for s in axes:
                q_copy[s, a, owner] = local(
                    q_hbm.at[head(s, a, owner)], q_buf.at[s, a, owner], q_sem.at[s, a, owner]
                )

    barrier = pltpu.get_barrier_semaphore()
    for s in axes:
        pl.semaphore_signal(
            barrier, inc=1, device_id={"ctx": peer[s]}, device_id_type=pl.DeviceIdType.MESH
        )

    halt_copy.wait()
    flag = jnp.full((1, width), halt[0] > STEP).astype(jnp.bfloat16)

    near, far, keys, values, parts, stats, gathers = {}, {}, {}, {}, {}, {}, {}
    for a in range(share):
        for s in axes:
            q_copy[s, a, 1].wait()
            q_buf[s, a, 1] = q_buf[s, a, 1] * flag
    pl.semaphore_wait(barrier, 2)

    def send_keys(a):
        for s in axes:
            keys[s, a] = remote(k_hbm.at[head(s, a, 1)], k_buf.at[s, a, 1], 2, s, a, s)

    def send_values(a):
        for s in axes:
            values[s, a] = remote(v_hbm.at[head(s, a, 1)], v_buf.at[s, a, 1], 3, s, a, s)

    def pass_on(a):
        for s in axes:
            q_copy[s, a, 0].wait()
            near[s, a].wait_recv()
            q_mid[s, a] = q_buf[s, a, 0] * flag + q_near[s, a]
            far[s, a] = remote(q_mid.at[s, a], q_far.at[s, a], 1, s, a, 1 - s)

    for a in range(share):
        for s in axes:
            near[s, a] = remote(q_buf.at[s, a, 1], q_near.at[s, a], 0, s, a, s)
    send_keys(0)

    own_kv = {}
    for a in range(share):
        for s in axes:
            for i, (src, buf) in enumerate(((k_hbm, k_buf), (v_hbm, v_buf))):
                own_kv[i, s, a] = local(
                    src.at[head(s, a, 0)], buf.at[s, a, 0], kv_sem.at[i, s, a]
                )
    w_copies = []
    for a in range(share):
        for owner, buf in enumerate((w_own, w_in)):
            for s in axes:
                w_copies.append(
                    local(
                        w_hbm.at[head(s, a, owner)],
                        buf.at[a, pl.ds(s * width, width)],
                        w_sem.at[owner, s, a],
                    )
                )
    state_copy = local(state_hbm, state_buf, state_sem)
    gain_copy = local(gain_hbm, gain_buf, gain_sem)

    for a in range(share):
        pass_on(a)
        send_values(a)
        if a + 1 < share:
            send_keys(a + 1)

    def attend(s, a):
        far[s, a].wait_recv()
        own_kv[0, s, a].wait()
        keys[s, a].wait_recv()
        query = q_mid[s, a] + q_far[s, a]
        scores = lax.dot_general(
            k_buf[s, a].reshape(2 * rows, width),
            query,
            (((1,), (1,)), ((), ())),
            preferred_element_type=jnp.float32,
        )
        top = jnp.max(scores, axis=0, keepdims=True)
        weights = jnp.exp2((scores - top) * scale)
        total = jnp.sum(weights, axis=0, keepdims=True)
        own_kv[1, s, a].wait()
        values[s, a].wait_recv()
        weighted = lax.dot_general(
            v_buf[s, a].reshape(2 * rows, width),
            weights.astype(jnp.bfloat16),
            (((0,), (0,)), ((), ())),
            preferred_element_type=jnp.float32,
        )
        stat = jnp.concatenate([top, total], axis=0)
        own_acc[s, a] = weighted
        own_stat[s, a] = stat
        part_out[s, a] = (weighted * (1.0 / total)).astype(jnp.bfloat16)
        stat_out[s, a] = stat
        parts[s, a] = remote(part_out.at[s, a], part_in.at[s, a], 4, s, a, 1 - s)
        stats[s, a] = remote(stat_out.at[s, a], stat_in.at[s, a], 5, s, a, 1 - s)

    def combine(s, a):
        parts[s, a].wait_recv()
        stats[s, a].wait_recv()
        top, total = own_stat[s, a, 0:1], own_stat[s, a, 1:2]
        top_in, total_in = stat_in[s, a, 0:1], stat_in[s, a, 1:2]
        both = jnp.maximum(top, top_in)
        shrink = jnp.exp2((top - both) * scale)
        total_in = total_in * jnp.exp2((top_in - both) * scale)
        inverse = 1.0 / (total * shrink + total_in)
        attended = own_acc[s, a] * (shrink * inverse)
        attended = attended + part_in[s, a].astype(jnp.float32) * (total_in * inverse)
        att_own[s, a] = attended.T.astype(jnp.bfloat16)
        gathers[s, a] = remote(att_own.at[s, a], att_in.at[s, a], 6, s, a, s)

    def both_axes(buf, a, cut):
        return jnp.concatenate([buf[s, a, cut] for s in axes], axis=1)

    chunk = min(4 * TILE, features)

    def project(buf, weight, a, first):
        left = both_axes(buf, a, slice(None))

        def body(step, carry):
            cut = pl.ds(pl.multiple_of(step * chunk, chunk), chunk)
            product = jnp.dot(left, weight[a, :, cut], preferred_element_type=jnp.float32)
            if first:
                update[:, cut] = state_buf[:, cut].astype(jnp.float32) + product
            else:
                update[:, cut] = update[:, cut] + product
            return carry

        lax.fori_loop(0, features // chunk, body, 0)

    for a in range(share):
        for s in axes:
            attend(s, a)
    for copy in w_copies:
        copy.wait()
    state_copy.wait()
    gain_copy.wait()
    for a in range(share):
        for s in axes:
            combine(s, a)
        project(att_own, w_own, a, a == 0)
    for a in range(share - 1):
        for s in axes:
            gathers[s, a].wait_recv()
        project(att_in, w_in, a, False)

    gain = gain_buf[...].astype(jnp.float32).reshape(1, -1)
    a = share - 1
    for s in axes:
        gathers[s, a].wait_recv()
    for block in range(rows // TILE):
        cut = slice(block * TILE, (block + 1) * TILE)
        product = jnp.dot(both_axes(att_in, a, cut), w_in[a], preferred_element_type=jnp.float32)
        mixed = update[cut, :] + product
        mean = jnp.mean(mixed * mixed, axis=-1, keepdims=True)
        normed = mixed * lax.rsqrt(mean + 1e-06) * gain
        active = jnp.full(normed.shape, halt[block * TILE] > STEP)
        kept = state_buf[cut, :].astype(jnp.float32)
        out_ref[cut, :] = jnp.where(active, normed, kept).astype(out_ref.dtype)

    for copy in copies:
        copy.wait_send()


def on_square(state_rows, q, k, v, halt_counts, out_weight, norm_gain):
    heads, rows, width = q.shape
    share = heads // 4
    features = state_rows.shape[1]
    bf16, f32 = jnp.bfloat16, jnp.float32
    hbm = pl.BlockSpec(memory_space=pltpu.MemorySpace.HBM)
    vmem = pl.BlockSpec(memory_space=pltpu.VMEM)
    dma = pltpu.SemaphoreType.DMA
    operands = (halt_counts, q, k, v, state_rows, out_weight, norm_gain)
    return pl.pallas_call(
        functools.partial(square_kernel, share),
        out_shape=jax.ShapeDtypeStruct((rows, features), bf16),
        in_specs=[hbm] * len(operands),
        out_specs=vmem,
        scratch_shapes=[
            pltpu.SMEM((rows,), jnp.int32),
            pltpu.VMEM((features,), bf16),
            pltpu.VMEM((2, share, 2, rows, width), bf16),
            pltpu.VMEM((2, share, rows, width), bf16),
            pltpu.VMEM((2, share, rows, width), bf16),
            pltpu.VMEM((2, share, rows, width), bf16),
            pltpu.VMEM((2, share, 2, rows, width), bf16),
            pltpu.VMEM((2, share, 2, rows, width), bf16),
            pltpu.VMEM((2, share, width, rows), f32),
            pltpu.VMEM((2, share, 2, rows), f32),
            pltpu.VMEM((2, share, width, rows), bf16),
            pltpu.VMEM((2, share, width, rows), bf16),
            pltpu.VMEM((2, share, 2, rows), f32),
            pltpu.VMEM((2, share, 2, rows), f32),
            pltpu.VMEM((2, share, rows, width), bf16),
            pltpu.VMEM((2, share, rows, width), bf16),
            pltpu.VMEM((rows, features), bf16),
            pltpu.VMEM((share, 2 * width, features), bf16),
            pltpu.VMEM((share, 2 * width, features), bf16),
            pltpu.VMEM((rows, features), f32),
            dma,
            dma,
            dma,
            dma((2, share, 2)),
            dma((2, 2, share)),
            dma((2, 2, share)),
            dma((7, 2, share)),
            dma((7, 2, share)),
        ],
        compiler_params=pltpu.CompilerParams(
            collective_id=0, has_side_effects=True, vmem_limit_bytes=28 * 1024 * 1024
        ),
    )(*[pltpu.with_memory_space_constraint(x, pltpu.HBM) for x in operands])


def fold_heads(carry, queries, key_piece, value_piece, score_scale):
    running_max, running_sum, weighted = carry

    def per_head(head_items):
        query_head, key_head, value_head, max_head, sum_head, weighted_head = head_items
        scores = (
            lax.dot_general(
                query_head, key_head, (((1,), (1,)), ((), ())), preferred_element_type=jnp.float32
            )
            * score_scale
        )
        new_max = jnp.maximum(max_head, jnp.max(scores, axis=1))
        shrink = jnp.exp(max_head - new_max)
        exponents = jnp.exp(scores - new_max[:, None])
        sum_head = sum_head * shrink + jnp.sum(exponents, axis=1)
        weighted_head = weighted_head * shrink[:, None] + jnp.dot(
            exponents.astype(jnp.bfloat16), value_head, preferred_element_type=jnp.float32
        )
        return (new_max, sum_head, weighted_head)

    return lax.map(per_head, (queries, key_piece, value_piece, running_max, running_sum, weighted))


def empty_carry(head_count, query_count, head_width):
    return (
        jnp.full((head_count, query_count), -1e30, jnp.float32),
        jnp.zeros((head_count, query_count), jnp.float32),
        jnp.zeros((head_count, query_count, head_width), jnp.float32),
    )


def attend_keys(query_vectors, key_vectors, value_vectors, score_scale):
    head_count, row_count, head_width = query_vectors.shape
    initial = empty_carry(head_count, row_count, head_width)
    running_max, running_sum, weighted = fold_heads(
        initial,
        query_vectors,
        lax.all_gather(key_vectors, "ctx", axis=1, tiled=True),
        lax.all_gather(value_vectors, "ctx", axis=1, tiled=True),
        score_scale,
    )
    return (weighted / running_sum[..., None]).astype(jnp.bfloat16)


def on_device(
    state_rows, query_vectors, key_vectors, value_vectors, halt_counts, out_weight, norm_gain
):
    head_count, row_count, head_width = query_vectors.shape
    score_scale = head_width ** (-0.5)
    attended = attend_keys(query_vectors, key_vectors, value_vectors, score_scale)
    update = jnp.einsum("hqd,hde->qe", attended, out_weight, preferred_element_type=jnp.float32)
    mixed_sum = state_rows.astype(jnp.float32) + update
    normed = (
        mixed_sum
        * lax.rsqrt(jnp.mean(mixed_sum * mixed_sum, axis=-1, keepdims=True) + 1e-06)
        * norm_gain.astype(jnp.float32)
    )
    active = (halt_counts > STEP)[:, None]
    return jnp.where(active, normed.astype(jnp.bfloat16), state_rows)


def solution(mesh):
    n_ctx = mesh.shape["ctx"]

    def per_device(state_rows, q, k, v, halt_counts, out_weight, norm_gain):
        heads, rows, _ = q.shape
        one_owner = rows == (n_ctx - 1) * TILE
        if one_owner and heads % n_ctx == 0 and n_ctx == 4:
            return on_square(state_rows, q, k, v, halt_counts, out_weight, norm_gain)
        return on_device(state_rows, q, k, v, halt_counts, out_weight, norm_gain)

    placed = (
        P(("dp", "ctx"), None),
        P(None, ("dp", "ctx"), None),
        P(None, ("dp", "ctx"), None),
        P(None, ("dp", "ctx"), None),
        P(("dp", "ctx")),
        P(),
        P(),
    )
    return jax.shard_map(
        per_device, mesh=mesh, in_specs=placed, out_specs=P(("dp", "ctx"), None), check_vma=False
    )
```

```python
import functools

import jax
import jax.numpy as jnp
from jax import lax
from jax.experimental import pallas as pl
from jax.experimental.pallas import tpu as pltpu
from jax.sharding import PartitionSpec as P

STEP = 2
TILE = 128
LAG = 3
LOG2E = 1.4426950408889634


def star_kernel(
    halt_hbm,
    q_hbm,
    k_hbm,
    v_hbm,
    state_hbm,
    w_hbm,
    gain_hbm,
    out_ref,
    halt,
    gain_buf,
    flag_out,
    flag_in,
    q_buf,
    k_buf,
    v_buf,
    slot_out,
    slot_in,
    stat_out,
    stat_in,
    own_acc,
    att_buf,
    state_buf,
    w_buf,
    update,
    halt_sem,
    gain_sem,
    state_sem,
    qkv_sem,
    w_sem,
    flag_send,
    flag_recv,
    slot_send,
    slot_recv,
    stat_send,
    stat_recv,
):
    me = lax.axis_index("ctx")
    bits = (me % 2, me // 2)
    peer = (bits[1] * 2 + 1 - bits[0], (1 - bits[1]) * 2 + bits[0])
    heads, rows, width = q_hbm.shape
    features = state_hbm.shape[1]
    half = heads // 2
    blocks = rows // TILE
    scale = width ** (-0.5) * LOG2E
    axes = (0, 1)
    f32, bf16 = jnp.float32, jnp.bfloat16

    def local(src, dst, sem):
        copy = pltpu.make_async_copy(src, dst, sem)
        copy.start()
        return copy

    copies = []

    def remote(src, dst, send, recv, axis):
        copy = pltpu.make_async_remote_copy(
            src_ref=src,
            dst_ref=dst,
            send_sem=send,
            recv_sem=recv,
            device_id={"ctx": peer[axis]},
            device_id_type=pl.DeviceIdType.MESH,
        )
        copy.start()
        copies.append(copy)
        return copy

    def near_head(s, axis):
        return s // 2 + (half if (s + axis) % 2 == 0 else 0)

    halt_copy = local(halt_hbm, halt, halt_sem)
    own = {}
    for i in range(half):
        for h in (half + i, i):
            for n, (src, buf) in enumerate(((q_hbm, q_buf), (k_hbm, k_buf), (v_hbm, v_buf))):
                own[n, h] = local(src.at[h], buf.at[h], qkv_sem.at[n, h])
    loaded = set()

    def ready(n, h):
        if (n, h) not in loaded:
            own[n, h].wait()
            loaded.add((n, h))

    barrier = pltpu.get_barrier_semaphore()
    for axis in axes:
        pl.semaphore_signal(
            barrier, inc=1, device_id={"ctx": peer[axis]}, device_id_type=pl.DeviceIdType.MESH
        )
    halt_copy.wait()
    flag = jnp.full(flag_out.shape, halt[0] > STEP).astype(f32)
    flag_out[...] = flag

    def mask(value):
        return jnp.broadcast_to(value[0:1, :].astype(bf16), (rows, width)) > 0.5

    is_owner = mask(flag)

    def early(s, axis):
        h = near_head(s, axis)
        other = s // 2 + (half if axis == 0 else 0)
        ready(0, h)
        ready(1 + s % 2, other)
        return jnp.where(is_owner, q_buf[h], (k_buf, v_buf)[s % 2][other])

    slots, stats = {}, {}

    def send(s, axis):
        slots[s, axis] = remote(
            slot_out.at[s, axis],
            slot_in.at[s, axis],
            slot_send.at[s, axis],
            slot_recv.at[s, axis],
            axis,
        )

    for s in range(LAG):
        for axis in axes:
            slot_out[s, axis] = early(s, axis).reshape(blocks, TILE, width)
        if s == 0:
            pl.semaphore_wait(barrier, 2)
            flags = [
                remote(flag_out, flag_in.at[axis], flag_send.at[axis], flag_recv.at[axis], axis)
                for axis in axes
            ]
        for axis in axes:
            send(s, axis)

    w_copies = []
    for i in range(half):
        for side in (0, 1):
            w_copies.append(
                local(
                    w_hbm.at[i + side * half],
                    w_buf.at[i, pl.ds(side * width, width)],
                    w_sem.at[i, side],
                )
            )
    state_copy = local(state_hbm, state_buf, state_sem)
    gain_copy = local(gain_hbm, gain_buf, gain_sem)

    for axis in axes:
        flags[axis].wait_recv()
    owner_at = [mask(flag_in[axis]) for axis in axes]
    beside = flag_in[0] + flag_in[1]
    is_beside = mask(beside)
    bias = jnp.concatenate([(beside[0:1, :] - 1.0) * 1e30] * blocks, axis=1)

    def received(s, axis):
        return slot_in[s, axis].reshape(rows, width)

    def step(s):
        i = s // 2
        low, high = (i, half + i) if s % 2 == 0 else (half + i, i)
        for n in range(3):
            ready(n, low)
            ready(n, high)
        query = jnp.where(
            owner_at[0], received(s, 0), jnp.where(owner_at[1], received(s, 1), q_buf[low])
        )
        key = jnp.where(owner_at[0], k_buf[high], k_buf[low])
        value = jnp.where(owner_at[0], v_buf[high], v_buf[low])

        def score(keys):
            return lax.dot_general(
                keys, query, (((1,), (1,)), ((), ())), preferred_element_type=f32
            )

        def weigh(values, weights):
            return lax.dot_general(
                values, weights.astype(bf16), (((0,), (0,)), ((), ())), preferred_element_type=f32
            )

        scores = score(key)
        top = jnp.max(scores, axis=0, keepdims=True)
        if s % 2 == 1:
            far_key = jnp.where(owner_at[0], received(s - 1, 1), received(s - 1, 0))
            far_value = jnp.where(owner_at[0], received(s, 1), received(s, 0))
            far_value = jnp.where(is_beside, far_value, jnp.zeros_like(far_value))
            far_scores = score(far_key) + bias
            top = jnp.maximum(top, jnp.max(far_scores, axis=0, keepdims=True))
        weights = jnp.exp2((scores - top) * scale)
        total = jnp.sum(weights, axis=0, keepdims=True)
        weighted = weigh(value, weights)
        if s % 2 == 1:
            far_weights = jnp.exp2((far_scores - top) * scale)
            total = total + jnp.sum(far_weights, axis=0, keepdims=True)
            weighted = weighted + weigh(far_value, far_weights)
        weighted = weighted * (1.0 / total)
        own_acc[s] = weighted
        stat_out[s] = jnp.concatenate([top, total], axis=0)
        part = weighted.astype(bf16)
        for axis in axes:
            slot = s + LAG
            if slot < heads:
                block = early(slot, axis)
            for tile in range(blocks):
                piece = part[:, tile * TILE : (tile + 1) * TILE]
                if slot < heads:
                    cut = slice(tile * TILE, (tile + 1) * TILE)
                    piece = jnp.where(is_beside[cut], piece, block[cut])
                slot_out[slot, axis, tile] = piece
        for axis in axes:
            stats[s, axis] = remote(
                stat_out.at[s],
                stat_in.at[s, axis],
                stat_send.at[s, axis],
                stat_recv.at[s, axis],
                axis,
            )
            send(slot, axis)

    def combine(i):
        for side in (0, 1):
            first, last = 2 * i + side, 2 * i + 1 - side
            sources = ((stat_out[first], own_acc[first]),)
            for s, axis in ((first, 1), (last, 0)):
                block = jnp.concatenate(
                    [slot_in[s + LAG, axis, tile] for tile in range(blocks)], axis=1
                )
                sources += ((stat_in[s, axis], block.astype(f32)),)
            top = functools.reduce(jnp.maximum, [stat[0:1] for stat, _ in sources])
            sums = [stat[1:2] * jnp.exp2((stat[0:1] - top) * scale) for stat, _ in sources]
            inverse = 1.0 / functools.reduce(jnp.add, sums)
            attended = functools.reduce(
                jnp.add, [part * (total * inverse) for total, (_, part) in zip(sums, sources)]
            )
            att_buf[i, :, side * width : (side + 1) * width] = attended.T.astype(bf16)

    chunk = min(4 * TILE, features)

    def project(i):
        left = att_buf[i]

        def body(n, carry):
            cut = pl.ds(pl.multiple_of(n * chunk, chunk), chunk)
            product = jnp.dot(left, w_buf[i, :, cut], preferred_element_type=f32)
            if i == 0:
                update[:, cut] = state_buf[:, cut].astype(f32) + product
            else:
                update[:, cut] = update[:, cut] + product
            return carry

        lax.fori_loop(0, features // chunk, body, 0)

    for s in range(heads + LAG):
        for axis in axes:
            slots[s, axis].wait_recv()
            if s >= LAG:
                stats[s - LAG, axis].wait_recv()
        if s < heads:
            step(s)
        if s == LAG:
            for copy in w_copies:
                copy.wait()
            state_copy.wait()
            gain_copy.wait()
        if s > LAG and (s - LAG) % 2 == 1:
            i = (s - LAG) // 2
            combine(i)
            if i < half - 1:
                project(i)

    gain = gain_buf[...].astype(f32).reshape(1, -1)
    i = half - 1
    for block in range(blocks):
        cut = slice(block * TILE, (block + 1) * TILE)
        product = jnp.dot(att_buf[i, cut, :], w_buf[i], preferred_element_type=f32)
        mixed = update[cut, :] + product
        mean = jnp.mean(mixed * mixed, axis=-1, keepdims=True)
        normed = mixed * lax.rsqrt(mean + 1e-06) * gain
        active = jnp.full(normed.shape, halt[block * TILE] > STEP)
        kept = state_buf[cut, :].astype(f32)
        out_ref[cut, :] = jnp.where(active, normed, kept).astype(out_ref.dtype)

    for copy in copies:
        copy.wait_send()


def on_star(state_rows, q, k, v, halt_counts, out_weight, norm_gain):
    heads, rows, width = q.shape
    features = state_rows.shape[1]
    half, blocks, slots = heads // 2, rows // TILE, heads + LAG
    bf16, f32 = jnp.bfloat16, jnp.float32
    hbm = pl.BlockSpec(memory_space=pltpu.MemorySpace.HBM)
    vmem = pl.BlockSpec(memory_space=pltpu.VMEM)
    dma = pltpu.SemaphoreType.DMA
    operands = (halt_counts, q, k, v, state_rows, out_weight, norm_gain)
    return pl.pallas_call(
        star_kernel,
        out_shape=jax.ShapeDtypeStruct((rows, features), bf16),
        in_specs=[hbm] * len(operands),
        out_specs=vmem,
        scratch_shapes=[
            pltpu.SMEM((rows,), jnp.int32),
            pltpu.VMEM((features,), bf16),
            pltpu.VMEM((8, width), f32),
            pltpu.VMEM((2, 8, width), f32),
            pltpu.VMEM((heads, rows, width), bf16),
            pltpu.VMEM((heads, rows, width), bf16),
            pltpu.VMEM((heads, rows, width), bf16),
            pltpu.VMEM((slots, 2, blocks, TILE, width), bf16),
            pltpu.VMEM((slots, 2, blocks, TILE, width), bf16),
            pltpu.VMEM((heads, 2, rows), f32),
            pltpu.VMEM((heads, 2, 2, rows), f32),
            pltpu.VMEM((heads, width, rows), f32),
            pltpu.VMEM((half, rows, 2 * width), bf16),
            pltpu.VMEM((rows, features), bf16),
            pltpu.VMEM((half, 2 * width, features), bf16),
            pltpu.VMEM((rows, features), f32),
            dma,
            dma,
            dma,
            dma((3, heads)),
            dma((half, 2)),
            dma((2,)),
            dma((2,)),
            dma((slots, 2)),
            dma((slots, 2)),
            dma((heads, 2)),
            dma((heads, 2)),
        ],
        compiler_params=pltpu.CompilerParams(
            collective_id=0, has_side_effects=True, vmem_limit_bytes=32 * 1024 * 1024
        ),
    )(*[pltpu.with_memory_space_constraint(x, pltpu.HBM) for x in operands])


def fold_heads(carry, queries, key_piece, value_piece, score_scale):
    running_max, running_sum, weighted = carry

    def per_head(head_items):
        query_head, key_head, value_head, max_head, sum_head, weighted_head = head_items
        scores = (
            lax.dot_general(
                query_head, key_head, (((1,), (1,)), ((), ())), preferred_element_type=jnp.float32
            )
            * score_scale
        )
        new_max = jnp.maximum(max_head, jnp.max(scores, axis=1))
        shrink = jnp.exp(max_head - new_max)
        exponents = jnp.exp(scores - new_max[:, None])
        sum_head = sum_head * shrink + jnp.sum(exponents, axis=1)
        weighted_head = weighted_head * shrink[:, None] + jnp.dot(
            exponents.astype(jnp.bfloat16), value_head, preferred_element_type=jnp.float32
        )
        return (new_max, sum_head, weighted_head)

    return lax.map(per_head, (queries, key_piece, value_piece, running_max, running_sum, weighted))


def empty_carry(head_count, query_count, head_width):
    return (
        jnp.full((head_count, query_count), -1e30, jnp.float32),
        jnp.zeros((head_count, query_count), jnp.float32),
        jnp.zeros((head_count, query_count, head_width), jnp.float32),
    )


def attend_keys(query_vectors, key_vectors, value_vectors, score_scale):
    head_count, row_count, head_width = query_vectors.shape
    initial = empty_carry(head_count, row_count, head_width)
    running_max, running_sum, weighted = fold_heads(
        initial,
        query_vectors,
        lax.all_gather(key_vectors, "ctx", axis=1, tiled=True),
        lax.all_gather(value_vectors, "ctx", axis=1, tiled=True),
        score_scale,
    )
    return (weighted / running_sum[..., None]).astype(jnp.bfloat16)


def on_device(
    state_rows, query_vectors, key_vectors, value_vectors, halt_counts, out_weight, norm_gain
):
    head_count, row_count, head_width = query_vectors.shape
    score_scale = head_width ** (-0.5)
    attended = attend_keys(query_vectors, key_vectors, value_vectors, score_scale)
    update = jnp.einsum("hqd,hde->qe", attended, out_weight, preferred_element_type=jnp.float32)
    mixed_sum = state_rows.astype(jnp.float32) + update
    normed = (
        mixed_sum
        * lax.rsqrt(jnp.mean(mixed_sum * mixed_sum, axis=-1, keepdims=True) + 1e-06)
        * norm_gain.astype(jnp.float32)
    )
    active = (halt_counts > STEP)[:, None]
    return jnp.where(active, normed.astype(jnp.bfloat16), state_rows)


def solution(mesh):
    n_ctx = mesh.shape["ctx"]

    def per_device(state_rows, q, k, v, halt_counts, out_weight, norm_gain):
        heads, rows, width = q.shape
        one_owner = rows == (n_ctx - 1) * TILE
        if one_owner and heads % 2 == 0 and heads > LAG and width == TILE and n_ctx == 4:
            return on_star(state_rows, q, k, v, halt_counts, out_weight, norm_gain)
        return on_device(state_rows, q, k, v, halt_counts, out_weight, norm_gain)

    placed = (
        P(("dp", "ctx"), None),
        P(None, ("dp", "ctx"), None),
        P(None, ("dp", "ctx"), None),
        P(None, ("dp", "ctx"), None),
        P(("dp", "ctx")),
        P(),
        P(),
    )
    return jax.shard_map(
        per_device, mesh=mesh, in_specs=placed, out_specs=P(("dp", "ctx"), None), check_vma=False
    )
```

```python
import functools

import jax
import jax.numpy as jnp
from jax import lax
from jax.experimental import pallas as pl
from jax.experimental.pallas import tpu as pltpu
from jax.sharding import PartitionSpec as P

STEP = 2
TILE = 128
LAG = 3
SLOTS = 3 * LAG + 1
LOG2E = 1.4426950408889634


def slot_orders(heads):
    half = heads // 2
    first = [half]
    singles = [heads - 1, 0]
    for j in range(half - 1):
        first += [j + 1] + singles[j : j + 1]
    return first, [(h + half) % heads for h in first]


def star_kernel(
    halt_hbm,
    q_hbm,
    k_hbm,
    v_hbm,
    state_hbm,
    w_hbm,
    gain_hbm,
    out_ref,
    halt,
    gain_buf,
    flag_out,
    flag_in,
    qkv_buf,
    slot_out,
    slot_in,
    stat_out,
    stat_in,
    own_part,
    own_stat,
    att_buf,
    state_buf,
    w_buf,
    update,
    halt_sem,
    gain_sem,
    state_sem,
    w_sem,
    flag_send,
    flag_recv,
    slot_send,
    stat_send,
    qkv_sem,
    slot_recv,
    stat_recv,
):
    me = lax.axis_index("ctx")
    bits = (me % 2, me // 2)
    peer = (bits[1] * 2 + 1 - bits[0], (1 - bits[1]) * 2 + bits[0])
    heads, rows, width = q_hbm.shape
    features = state_hbm.shape[1]
    half = heads // 2
    early = heads - 2
    blocks = rows // TILE
    scale = width ** (-0.5) * LOG2E
    axes = (0, 1)
    orders = slot_orders(heads)
    f32, bf16 = jnp.float32, jnp.bfloat16

    def local(src, dst, sem):
        copy = pltpu.make_async_copy(src, dst, sem)
        copy.start()
        return copy

    def remote(src, dst, send, recv, axis):
        return pltpu.make_async_remote_copy(
            src_ref=src,
            dst_ref=dst,
            send_sem=send,
            recv_sem=recv,
            device_id={"ctx": peer[axis]},
            device_id_type=pl.DeviceIdType.MESH,
        )

    halt_copy = local(halt_hbm, halt, halt_sem)
    for i in range(half):
        for side in (0, 1):
            for n, operand in enumerate((q_hbm, k_hbm, v_hbm)):
                local(operand.at[side * half + i], qkv_buf.at[i, side, n], qkv_sem.at[i])
    loaded = set()

    def own(n, h):
        i = h % half
        if i not in loaded:
            pltpu.make_async_copy(qkv_buf.at[i], qkv_buf.at[i], qkv_sem.at[i]).wait()
            loaded.add(i)
        return qkv_buf[i, h // half, n]

    barrier = pltpu.get_barrier_semaphore()
    for axis in axes:
        pl.semaphore_signal(
            barrier, inc=1, device_id={"ctx": peer[axis]}, device_id_type=pl.DeviceIdType.MESH
        )
    halt_copy.wait()
    flag = jnp.full(flag_out.shape, halt[0] > STEP).astype(f32)
    flag_out[...] = flag

    def mask(value):
        return jnp.broadcast_to(value[0:1, :].astype(bf16), (rows, width)) > 0.5

    is_owner = mask(flag)

    def opening(s, axis):
        other = orders[1 - axis][2 * (s // 2) + 1]
        return jnp.where(is_owner, own(0, orders[axis][s]), own(1 + s % 2, other))

    def send(s):
        for axis in axes:
            remote(
                slot_out.at[s, axis], slot_in.at[s, axis], slot_send, slot_recv.at[s], axis
            ).start()

    for s in range(LAG):
        for axis in axes:
            slot_out[s, axis] = opening(s, axis).reshape(blocks, TILE, width)
        if s == 0:
            pl.semaphore_wait(barrier, 2)
            for axis in axes:
                remote(flag_out, flag_in.at[axis], flag_send.at[axis], flag_recv, axis).start()
        send(s)

    for side in (0, 1):
        local(
            w_hbm.at[pl.ds(side * half, half)], w_buf.at[:, pl.ds(side * width, width)], w_sem
        )
    state_copy = local(state_hbm, state_buf, state_sem)
    gain_copy = local(gain_hbm, gain_buf, gain_sem)

    remote(flag_in, flag_in, flag_send.at[0], flag_recv, 0).wait_recv()
    owner_at = [mask(flag_in[axis]) for axis in axes]
    beside = flag_in[0] + flag_in[1]
    is_beside = mask(beside)

    def bias(valid):
        return jnp.concatenate([(valid[0:1, :] - 1.0) * 1e30] * blocks, axis=1)

    def received(s, axis):
        return slot_in[s, axis].reshape(rows, width)

    def attend(query, keys, values):
        scores = lax.dot_general(
            keys, query, (((1,), (1,)), ((), ())), preferred_element_type=f32
        )
        top = jnp.max(scores, axis=0, keepdims=True)
        weights = jnp.exp2((scores - top) * scale)
        total = jnp.sum(weights, axis=0, keepdims=True)
        weighted = lax.dot_general(
            values, weights.astype(bf16), (((0,), (0,)), ((), ())), preferred_element_type=f32
        )
        return top, total, weighted * (1.0 / total)

    def merge(sources):
        top = functools.reduce(jnp.maximum, [source[0] for source in sources])
        sums = [total * jnp.exp2((source - top) * scale) for source, total, _ in sources]
        total = functools.reduce(jnp.add, sums)
        inverse = 1.0 / total
        parts = [part * (each * inverse) for each, (_, _, part) in zip(sums, sources)]
        return top, total, functools.reduce(jnp.add, parts)

    def put(s, results):
        for axis in axes:
            top, total, part = results[axis]
            part = part.astype(bf16)
            stat_out[s - LAG - 1, axis] = jnp.concatenate([top, total], axis=0)
            block = opening(s, axis) if s < early else None
            for tile in range(blocks):
                cut = slice(tile * TILE, (tile + 1) * TILE)
                piece = part[:, cut]
                if s < early:
                    piece = jnp.where(is_beside[cut], piece, block[cut])
                slot_out[s, axis, tile] = piece
            remote(
                stat_out.at[s - LAG - 1, axis],
                stat_in.at[s - LAG - 1, axis],
                stat_send,
                stat_recv.at[s - LAG - 1],
                axis,
            ).start()
        send(s)

    def keep(h, result):
        own_stat[h] = jnp.concatenate(result[:2], axis=0)
        own_part[h] = result[2]

    def kept(h):
        return own_stat[h, 0:1], own_stat[h, 1:2], own_part[h]

    def sent(s, axis):
        block = jnp.concatenate([slot_in[s, axis, tile] for tile in range(blocks)], axis=1)
        stat = stat_in[s - LAG - 1, axis]
        return stat[0:1], stat[1:2], block.astype(f32)

    def select(value, first, second):
        line = jnp.concatenate([value[0:1, :]] * blocks, axis=1)
        return tuple(
            jnp.where(jnp.broadcast_to(line, a.shape) > 0.5, a, b) for a, b in zip(first, second)
        )

    def step(s):
        high, low = orders[0][s], orders[1][s]
        query = jnp.where(
            owner_at[0], received(s, 0), jnp.where(owner_at[1], received(s, 1), own(0, low))
        )
        key = jnp.where(owner_at[0], own(1, high), own(1, low))
        value = jnp.where(owner_at[0], own(2, high), own(2, low))
        if s % 2 == 0:
            result = attend(query, key, value)
            keep(low, result)
            if s > 0:
                put(s + LAG, (result, result))
            else:
                for axis in axes:
                    block = jnp.where(owner_at[1 - axis], query, opening(LAG, axis))
                    slot_out[LAG, axis] = block.reshape(blocks, TILE, width)
                send(LAG)
            return
        far_key = jnp.where(owner_at[0], received(s - 1, 1), received(s - 1, 0))
        far_value = jnp.where(owner_at[0], received(s, 1), received(s, 0))
        far_query = query
        valid = beside if s > LAG else beside + flag
        if s == LAG:
            far, near = orders[0][0], orders[1][0]
            take = mask(flag + beside)
            query = jnp.where(take, query, received(s, 1))
            key = jnp.where(take, key, own(1, far))
            value = jnp.where(take, value, own(2, far))
            far_query = jnp.where(take, far_query, received(s, 0))
            far_key = jnp.where(take, far_key, own(1, near))
            far_value = jnp.where(take, far_value, own(2, near))
        nearby = attend(query, key, value)
        distant = attend(far_query, far_key, far_value)
        result = merge((nearby, (distant[0] + bias(valid),) + distant[1:]))
        keep(low, result)
        if s == LAG:
            put(
                s + LAG,
                (select(beside, result, distant), select(beside, result, nearby)),
            )
        else:
            put(s + LAG, (result, result))
        if s <= LAG:
            nearby = attend(own(0, high), own(1, high), own(2, high))
            distant = attend(own(0, high), received(s - 1, 1), received(s, 1))
            keep(high, merge((nearby, distant)))

    def finish_first():
        near, far = orders[1][0], 2 * LAG
        result = merge((kept(near), select(flag_in[0], sent(far, 1), sent(far, 0))))
        put(SLOTS - 1, (result, result))

    def combine(i):
        for side in (0, 1):
            h = i + side * half
            sources = [kept(h)]
            for axis in axes:
                if h in orders[axis]:
                    s = orders[axis].index(h)
                    sources.append(sent(s + LAG if s > 0 else SLOTS - 1, axis))
            attended = merge(sources)[2]
            att_buf[i, :, side * width : (side + 1) * width] = attended.T.astype(bf16)

    chunk = min(4 * TILE, features)

    def project(i, initial):
        left = att_buf[i]

        def body(n, carry):
            cut = pl.ds(pl.multiple_of(n * chunk, chunk), chunk)
            product = jnp.dot(left, w_buf[i, :, cut], preferred_element_type=f32)
            if initial:
                update[:, cut] = state_buf[:, cut].astype(f32) + product
            else:
                update[:, cut] = update[:, cut] + product
            return carry

        lax.fori_loop(0, features // chunk, body, 0)

    for s in range(SLOTS):
        remote(slot_in.at[s], slot_in.at[s], slot_send, slot_recv.at[s], 0).wait_recv()
        if s > LAG:
            stat = s - LAG - 1
            remote(
                stat_in.at[stat], stat_in.at[stat], stat_send, stat_recv.at[stat], 0
            ).wait_recv()
        if s < early:
            step(s)
        elif s == early:
            finish_first()
        if s > LAG and s % 2 == 0:
            i = s // 2 - 1
            if i == 1:
                pltpu.make_async_copy(w_buf, w_buf, w_sem).wait()
                state_copy.wait()
                gain_copy.wait()
            combine(i)
            project(i, i == 1)
    combine(0)

    gain = gain_buf[...].astype(f32).reshape(1, -1)
    for block in range(blocks):
        cut = slice(block * TILE, (block + 1) * TILE)
        product = jnp.dot(att_buf[0, cut, :], w_buf[0], preferred_element_type=f32)
        mixed = update[cut, :] + product
        mean = jnp.mean(mixed * mixed, axis=-1, keepdims=True)
        normed = mixed * lax.rsqrt(mean + 1e-06) * gain
        active = jnp.full(normed.shape, halt[block * TILE] > STEP)
        unchanged = state_buf[cut, :].astype(f32)
        out_ref[cut, :] = jnp.where(active, normed, unchanged).astype(out_ref.dtype)

    remote(slot_out, slot_in, slot_send, slot_recv.at[0], 0).wait_send()
    remote(stat_out, stat_in, stat_send, stat_recv.at[0], 0).wait_send()
    for axis in axes:
        remote(flag_out, flag_in.at[axis], flag_send.at[axis], flag_recv, axis).wait_send()


def on_star(state_rows, q, k, v, halt_counts, out_weight, norm_gain):
    heads, rows, width = q.shape
    features = state_rows.shape[1]
    half, blocks, stats = heads // 2, rows // TILE, SLOTS - LAG - 1
    bf16, f32 = jnp.bfloat16, jnp.float32
    hbm = pl.BlockSpec(memory_space=pltpu.MemorySpace.HBM)
    vmem = pl.BlockSpec(memory_space=pltpu.VMEM)
    dma = pltpu.SemaphoreType.DMA
    operands = (halt_counts, q, k, v, state_rows, out_weight, norm_gain)
    return pl.pallas_call(
        star_kernel,
        out_shape=jax.ShapeDtypeStruct((rows, features), bf16),
        in_specs=[hbm] * len(operands),
        out_specs=vmem,
        scratch_shapes=[
            pltpu.SMEM((rows,), jnp.int32),
            pltpu.VMEM((features,), bf16),
            pltpu.VMEM((8, width), f32),
            pltpu.VMEM((2, 8, width), f32),
            pltpu.VMEM((half, 2, 3, rows, width), bf16),
            pltpu.VMEM((SLOTS, 2, blocks, TILE, width), bf16),
            pltpu.VMEM((SLOTS, 2, blocks, TILE, width), bf16),
            pltpu.VMEM((stats, 2, 2, rows), f32),
            pltpu.VMEM((stats, 2, 2, rows), f32),
            pltpu.VMEM((heads, width, rows), f32),
            pltpu.VMEM((heads, 2, rows), f32),
            pltpu.VMEM((half, rows, 2 * width), bf16),
            pltpu.VMEM((rows, features), bf16),
            pltpu.VMEM((half, 2 * width, features), bf16),
            pltpu.VMEM((rows, features), f32),
            dma,
            dma,
            dma,
            dma,
            dma((2,)),
            dma,
            dma,
            dma,
            dma((half,)),
            dma((SLOTS,)),
            dma((stats,)),
        ],
        compiler_params=pltpu.CompilerParams(
            collective_id=0, has_side_effects=True, vmem_limit_bytes=32 * 1024 * 1024
        ),
    )(*[pltpu.with_memory_space_constraint(x, pltpu.HBM) for x in operands])


def fold_heads(carry, queries, key_piece, value_piece, score_scale):
    running_max, running_sum, weighted = carry

    def per_head(head_items):
        query_head, key_head, value_head, max_head, sum_head, weighted_head = head_items
        scores = (
            lax.dot_general(
                query_head, key_head, (((1,), (1,)), ((), ())), preferred_element_type=jnp.float32
            )
            * score_scale
        )
        new_max = jnp.maximum(max_head, jnp.max(scores, axis=1))
        shrink = jnp.exp(max_head - new_max)
        exponents = jnp.exp(scores - new_max[:, None])
        sum_head = sum_head * shrink + jnp.sum(exponents, axis=1)
        weighted_head = weighted_head * shrink[:, None] + jnp.dot(
            exponents.astype(jnp.bfloat16), value_head, preferred_element_type=jnp.float32
        )
        return (new_max, sum_head, weighted_head)

    return lax.map(per_head, (queries, key_piece, value_piece, running_max, running_sum, weighted))


def empty_carry(head_count, query_count, head_width):
    return (
        jnp.full((head_count, query_count), -1e30, jnp.float32),
        jnp.zeros((head_count, query_count), jnp.float32),
        jnp.zeros((head_count, query_count, head_width), jnp.float32),
    )


def attend_keys(query_vectors, key_vectors, value_vectors, score_scale):
    head_count, row_count, head_width = query_vectors.shape
    initial = empty_carry(head_count, row_count, head_width)
    running_max, running_sum, weighted = fold_heads(
        initial,
        query_vectors,
        lax.all_gather(key_vectors, "ctx", axis=1, tiled=True),
        lax.all_gather(value_vectors, "ctx", axis=1, tiled=True),
        score_scale,
    )
    return (weighted / running_sum[..., None]).astype(jnp.bfloat16)


def on_device(
    state_rows, query_vectors, key_vectors, value_vectors, halt_counts, out_weight, norm_gain
):
    head_count, row_count, head_width = query_vectors.shape
    score_scale = head_width ** (-0.5)
    attended = attend_keys(query_vectors, key_vectors, value_vectors, score_scale)
    update = jnp.einsum("hqd,hde->qe", attended, out_weight, preferred_element_type=jnp.float32)
    mixed_sum = state_rows.astype(jnp.float32) + update
    normed = (
        mixed_sum
        * lax.rsqrt(jnp.mean(mixed_sum * mixed_sum, axis=-1, keepdims=True) + 1e-06)
        * norm_gain.astype(jnp.float32)
    )
    active = (halt_counts > STEP)[:, None]
    return jnp.where(active, normed.astype(jnp.bfloat16), state_rows)


def solution(mesh):
    n_ctx = mesh.shape["ctx"]

    def per_device(state_rows, q, k, v, halt_counts, out_weight, norm_gain):
        heads, rows, width = q.shape
        one_owner = rows == (n_ctx - 1) * TILE
        if one_owner and heads - 2 == 2 * LAG and width == TILE and n_ctx == 4:
            return on_star(state_rows, q, k, v, halt_counts, out_weight, norm_gain)
        return on_device(state_rows, q, k, v, halt_counts, out_weight, norm_gain)

    placed = (
        P(("dp", "ctx"), None),
        P(None, ("dp", "ctx"), None),
        P(None, ("dp", "ctx"), None),
        P(None, ("dp", "ctx"), None),
        P(("dp", "ctx")),
        P(),
        P(),
    )
    return jax.shard_map(
        per_device, mesh=mesh, in_specs=placed, out_specs=P(("dp", "ctx"), None), check_vma=False
    )
```

```python
import functools

import jax
import jax.numpy as jnp
from jax import lax
from jax.experimental import pallas as pl
from jax.experimental.pallas import tpu as pltpu
from jax.sharding import PartitionSpec as P

STEP = 2
TILE = 128
LAG = 3
SLOTS = 3 * LAG + 1
LOG2E = 1.4426950408889634


def slot_orders(heads):
    half = heads // 2
    first = [half]
    singles = [heads - 1, 0]
    for j in range(half - 1):
        first += [j + 1] + singles[j : j + 1]
    return first, [(h + half) % heads for h in first]


def star_kernel(
    halt_hbm,
    q_hbm,
    k_hbm,
    v_hbm,
    state_hbm,
    w_hbm,
    gain_hbm,
    out_ref,
    halt,
    gain_buf,
    flag_out,
    flag_in,
    qkv_buf,
    slot_out,
    slot_in,
    stat_out,
    stat_in,
    own_part,
    own_stat,
    att_buf,
    state_buf,
    w_buf,
    update,
    halt_sem,
    gain_sem,
    state_sem,
    w_sem,
    flag_send,
    flag_recv,
    slot_send,
    stat_send,
    qkv_sem,
    slot_recv,
    tile_recv,
    stat_recv,
):
    me = lax.axis_index("ctx")
    bits = (me % 2, me // 2)
    peer = (bits[1] * 2 + 1 - bits[0], (1 - bits[1]) * 2 + bits[0])
    heads, rows, width = q_hbm.shape
    features = state_hbm.shape[1]
    half = heads // 2
    early = heads - 2
    blocks = rows // TILE
    scale = width ** (-0.5) * LOG2E
    axes = (0, 1)
    orders = slot_orders(heads)
    f32, bf16 = jnp.float32, jnp.bfloat16

    def local(src, dst, sem):
        copy = pltpu.make_async_copy(src, dst, sem)
        copy.start()
        return copy

    def remote(src, dst, send, recv, axis):
        return pltpu.make_async_remote_copy(
            src_ref=src,
            dst_ref=dst,
            send_sem=send,
            recv_sem=recv,
            device_id={"ctx": peer[axis]},
            device_id_type=pl.DeviceIdType.MESH,
        )

    barrier = pltpu.get_barrier_semaphore()
    for axis in axes:
        pl.semaphore_signal(
            barrier, inc=1, device_id={"ctx": peer[axis]}, device_id_type=pl.DeviceIdType.MESH
        )
    halt_copy = local(halt_hbm, halt, halt_sem)

    def choices(s, axis):
        return (0, orders[axis][s]), (1 + s % 2, orders[1 - axis][2 * (s // 2) + 1])

    group_of = {}
    for s in range(LAG):
        for axis in axes:
            for block in choices(s, axis):
                group_of[block] = min(s, 1)
    for block in [(n, h) for h in range(heads) for n in range(3)]:
        group_of.setdefault(block, 2)
    for (n, h), group in group_of.items():
        local((q_hbm, k_hbm, v_hbm)[n].at[h], qkv_buf.at[n * heads + h], qkv_sem.at[group])
    loaded = set()

    def own(n, h):
        group = group_of[n, h]
        if group not in loaded:
            whole = qkv_buf.at[pl.ds(0, list(group_of.values()).count(group))]
            pltpu.make_async_copy(whole, whole, qkv_sem.at[group]).wait()
            loaded.add(group)
        return qkv_buf[n * heads + h]

    halt_copy.wait()
    flag = jnp.full(flag_out.shape, halt[0] > STEP).astype(f32)
    flag_out[...] = flag

    def mask(value):
        return jnp.broadcast_to(value[0:1, :].astype(bf16), (rows, width)) > 0.5

    is_owner = mask(flag)

    def opening(s, axis):
        mine, other = choices(s, axis)
        return jnp.where(is_owner, own(*mine), own(*other))

    def send(s):
        if s < SLOTS - 2:
            for axis in axes:
                remote(
                    slot_out.at[s, axis], slot_in.at[s, axis], slot_send, slot_recv.at[s], axis
                ).start()
            return
        for tile in range(blocks):
            for axis in axes:
                remote(
                    slot_out.at[s, axis, tile],
                    slot_in.at[s, axis, tile],
                    slot_send,
                    tile_recv.at[s - SLOTS + 2, tile],
                    axis,
                ).start()

    def wait_tile(s, tile):
        landed = slot_in.at[s, pl.ds(0, 2), tile]
        remote(landed, landed, slot_send, tile_recv.at[s - SLOTS + 2, tile], 0).wait_recv()

    def wait_stat(s):
        stat = s - LAG - 1
        remote(
            stat_in.at[stat], stat_in.at[stat], stat_send, stat_recv.at[stat], 0
        ).wait_recv()

    for s in range(LAG):
        for axis in axes:
            slot_out[s, axis] = opening(s, axis).reshape(blocks, TILE, width)
        if s == 0:
            pl.semaphore_wait(barrier, 2)
            for axis in axes:
                remote(flag_out, flag_in.at[axis], flag_send.at[axis], flag_recv, axis).start()
        send(s)

    for side in (0, 1):
        local(
            w_hbm.at[pl.ds(side * half, half)], w_buf.at[:, pl.ds(side * width, width)], w_sem
        )
    state_copy = local(state_hbm, state_buf, state_sem)
    gain_copy = local(gain_hbm, gain_buf, gain_sem)

    remote(flag_in, flag_in, flag_send.at[0], flag_recv, 0).wait_recv()
    owner_at = [mask(flag_in[axis]) for axis in axes]
    beside = flag_in[0] + flag_in[1]
    is_beside = mask(beside)

    def bias(valid):
        return jnp.concatenate([(valid[0:1, :] - 1.0) * 1e30] * blocks, axis=1)

    def received(s, axis):
        return slot_in[s, axis].reshape(rows, width)

    def attend(query, keys, values):
        scores = lax.dot_general(
            keys, query, (((1,), (1,)), ((), ())), preferred_element_type=f32
        )
        top = jnp.max(scores, axis=0, keepdims=True)
        weights = jnp.exp2((scores - top) * scale)
        total = jnp.sum(weights, axis=0, keepdims=True)
        weighted = lax.dot_general(
            values, weights.astype(bf16), (((0,), (0,)), ((), ())), preferred_element_type=f32
        )
        return top, total, weighted * (1.0 / total)

    def merge(sources):
        top = functools.reduce(jnp.maximum, [source[0] for source in sources])
        sums = [total * jnp.exp2((source - top) * scale) for source, total, _ in sources]
        total = functools.reduce(jnp.add, sums)
        inverse = 1.0 / total
        parts = [part * (each * inverse) for each, (_, _, part) in zip(sums, sources)]
        return top, total, functools.reduce(jnp.add, parts)

    def put(s, results):
        for axis in axes:
            top, total, part = results[axis]
            part = part.astype(bf16)
            stat_out[s - LAG - 1, axis] = jnp.concatenate([top, total], axis=0)
            block = opening(s, axis) if s < early else None
            for tile in range(blocks):
                cut = slice(tile * TILE, (tile + 1) * TILE)
                piece = part[:, cut]
                if s < early:
                    piece = jnp.where(is_beside[cut], piece, block[cut])
                slot_out[s, axis, tile] = piece
            remote(
                stat_out.at[s - LAG - 1, axis],
                stat_in.at[s - LAG - 1, axis],
                stat_send,
                stat_recv.at[s - LAG - 1],
                axis,
            ).start()
        send(s)

    def keep(h, result):
        own_stat[h] = jnp.concatenate(result[:2], axis=0)
        own_part[h] = result[2]

    def cut_of(tiles):
        return slice(tiles[0] * TILE, (tiles[-1] + 1) * TILE)

    def kept(h, tiles=range(blocks)):
        cut = cut_of(tiles)
        return own_stat[h, 0:1, cut], own_stat[h, 1:2, cut], own_part[h, :, cut]

    def sent(s, axis, tiles=range(blocks)):
        cut, stat = cut_of(tiles), s - LAG - 1
        block = jnp.concatenate([slot_in[s, axis, tile] for tile in tiles], axis=1)
        top, total = stat_in[stat, axis, 0:1, cut], stat_in[stat, axis, 1:2, cut]
        return top, total, block.astype(f32)

    def select(value, first, second):
        line = jnp.concatenate([value[0:1, :]] * blocks, axis=1)
        return tuple(
            jnp.where(jnp.broadcast_to(line, a.shape) > 0.5, a, b) for a, b in zip(first, second)
        )

    def step(s):
        high, low = orders[0][s], orders[1][s]
        query = jnp.where(
            owner_at[0], received(s, 0), jnp.where(owner_at[1], received(s, 1), own(0, low))
        )
        key = jnp.where(owner_at[0], own(1, high), own(1, low))
        value = jnp.where(owner_at[0], own(2, high), own(2, low))
        if s % 2 == 0:
            result = attend(query, key, value)
            keep(low, result)
            if s > 0:
                put(s + LAG, (result, result))
            else:
                for axis in axes:
                    block = jnp.where(owner_at[1 - axis], query, opening(LAG, axis))
                    slot_out[LAG, axis] = block.reshape(blocks, TILE, width)
                send(LAG)
            return
        far_key = jnp.where(owner_at[0], received(s - 1, 1), received(s - 1, 0))
        far_value = jnp.where(owner_at[0], received(s, 1), received(s, 0))
        far_query = query
        valid = beside if s > LAG else beside + flag
        if s == LAG:
            far, near = orders[0][0], orders[1][0]
            take = mask(flag + beside)
            query = jnp.where(take, query, received(s, 1))
            key = jnp.where(take, key, own(1, far))
            value = jnp.where(take, value, own(2, far))
            far_query = jnp.where(take, far_query, received(s, 0))
            far_key = jnp.where(take, far_key, own(1, near))
            far_value = jnp.where(take, far_value, own(2, near))
        nearby = attend(query, key, value)
        distant = attend(far_query, far_key, far_value)
        result = merge((nearby, (distant[0] + bias(valid),) + distant[1:]))
        keep(low, result)
        if s == LAG:
            put(
                s + LAG,
                (select(beside, result, distant), select(beside, result, nearby)),
            )
        else:
            put(s + LAG, (result, result))
        if s <= LAG:
            nearby = attend(own(0, high), own(1, high), own(2, high))
            distant = attend(own(0, high), received(s - 1, 1), received(s, 1))
            keep(high, merge((nearby, distant)))

    def finish_first():
        near, far = orders[1][0], 2 * LAG
        result = merge((kept(near), select(flag_in[0], sent(far, 1), sent(far, 0))))
        put(SLOTS - 1, (result, result))

    def combine(i, tiles=range(blocks)):
        for side in (0, 1):
            h = i + side * half
            sources = [kept(h, tiles)]
            for axis in axes:
                if h in orders[axis]:
                    s = orders[axis].index(h)
                    sources.append(sent(s + LAG if s > 0 else SLOTS - 1, axis, tiles))
            attended = merge(sources)[2]
            att_buf[i, cut_of(tiles), side * width : (side + 1) * width] = attended.T.astype(bf16)

    chunk = min(4 * TILE, features)

    def project(i, initial):
        left = att_buf[i]

        def body(n, carry):
            cut = pl.ds(pl.multiple_of(n * chunk, chunk), chunk)
            product = jnp.dot(left, w_buf[i, :, cut], preferred_element_type=f32)
            if initial:
                update[:, cut] = state_buf[:, cut].astype(f32) + product
            else:
                update[:, cut] = update[:, cut] + product
            return carry

        lax.fori_loop(0, features // chunk, body, 0)

    for s in range(SLOTS - 2):
        remote(slot_in.at[s], slot_in.at[s], slot_send, slot_recv.at[s], 0).wait_recv()
        if s > LAG:
            wait_stat(s)
        if s < early:
            step(s)
        elif s == early:
            finish_first()
        if s > LAG and s % 2 == 0:
            i = s // 2 - 1
            if i == 1:
                pltpu.make_async_copy(w_buf, w_buf, w_sem).wait()
                state_copy.wait()
                gain_copy.wait()
            combine(i)
            project(i, i == 1)

    strips = [slice(n, n + 2 * TILE) for n in range(0, features, 2 * TILE)]

    def add_product(i, tiles):
        cut = cut_of(tiles)
        left = att_buf[i, cut, :]
        squares = jnp.zeros((len(tiles) * TILE, TILE), f32)
        for strip in strips:
            mixed = update[cut, strip] + jnp.dot(
                left, w_buf[i, :, strip], preferred_element_type=f32
            )
            update[cut, strip] = mixed
            squares = squares + mixed[:, :TILE] * mixed[:, :TILE]
            squares = squares + mixed[:, TILE:] * mixed[:, TILE:]
        return squares

    wait_stat(SLOTS - 2)
    for tile in range(blocks):
        wait_tile(SLOTS - 2, tile)
        combine(half - 1, [tile])
        add_product(half - 1, [tile])

    wait_stat(SLOTS - 1)
    for tiles in ([0], list(range(1, blocks))):
        for tile in tiles:
            wait_tile(SLOTS - 1, tile)
        combine(0, tiles)
        squares = add_product(0, tiles)
        inverse = lax.rsqrt(jnp.sum(squares, axis=-1, keepdims=True) / features + 1e-06)
        for strip in strips:
            gain = gain_buf[strip].astype(f32).reshape(1, -1)
            for tile in tiles:
                cut, own_cut = cut_of([tile]), cut_of([tile - tiles[0]])
                active = jnp.full((TILE, 2 * TILE), halt[tile * TILE] > STEP).astype(bf16) > 0.5
                normed = (update[cut, strip] * inverse[own_cut] * gain).astype(bf16)
                out_ref[cut, strip] = jnp.where(active, normed, state_buf[cut, strip])

    remote(slot_out, slot_in, slot_send, slot_recv.at[0], 0).wait_send()
    remote(stat_out, stat_in, stat_send, stat_recv.at[0], 0).wait_send()
    for axis in axes:
        remote(flag_out, flag_in.at[axis], flag_send.at[axis], flag_recv, axis).wait_send()


def on_star(state_rows, q, k, v, halt_counts, out_weight, norm_gain):
    heads, rows, width = q.shape
    features = state_rows.shape[1]
    half, blocks, stats = heads // 2, rows // TILE, SLOTS - LAG - 1
    bf16, f32 = jnp.bfloat16, jnp.float32
    hbm = pl.BlockSpec(memory_space=pltpu.MemorySpace.HBM)
    vmem = pl.BlockSpec(memory_space=pltpu.VMEM)
    dma = pltpu.SemaphoreType.DMA
    operands = (halt_counts, q, k, v, state_rows, out_weight, norm_gain)
    return pl.pallas_call(
        star_kernel,
        out_shape=jax.ShapeDtypeStruct((rows, features), bf16),
        in_specs=[hbm] * len(operands),
        out_specs=vmem,
        scratch_shapes=[
            pltpu.SMEM((rows,), jnp.int32),
            pltpu.VMEM((features,), bf16),
            pltpu.VMEM((8, width), f32),
            pltpu.VMEM((2, 8, width), f32),
            pltpu.VMEM((3 * heads, rows, width), bf16),
            pltpu.VMEM((SLOTS, 2, blocks, TILE, width), bf16),
            pltpu.VMEM((SLOTS, 2, blocks, TILE, width), bf16),
            pltpu.VMEM((stats, 2, 2, rows), f32),
            pltpu.VMEM((stats, 2, 2, rows), f32),
            pltpu.VMEM((heads, width, rows), f32),
            pltpu.VMEM((heads, 2, rows), f32),
            pltpu.VMEM((half, rows, 2 * width), bf16),
            pltpu.VMEM((rows, features), bf16),
            pltpu.VMEM((half, 2 * width, features), bf16),
            pltpu.VMEM((rows, features), f32),
            dma,
            dma,
            dma,
            dma,
            dma((2,)),
            dma,
            dma,
            dma,
            dma((3,)),
            dma((SLOTS - 2,)),
            dma((2, blocks)),
            dma((stats,)),
        ],
        compiler_params=pltpu.CompilerParams(
            collective_id=0, has_side_effects=True, vmem_limit_bytes=32 * 1024 * 1024
        ),
    )(*[pltpu.with_memory_space_constraint(x, pltpu.HBM) for x in operands])


def fold_heads(carry, queries, key_piece, value_piece, score_scale):
    running_max, running_sum, weighted = carry

    def per_head(head_items):
        query_head, key_head, value_head, max_head, sum_head, weighted_head = head_items
        scores = (
            lax.dot_general(
                query_head, key_head, (((1,), (1,)), ((), ())), preferred_element_type=jnp.float32
            )
            * score_scale
        )
        new_max = jnp.maximum(max_head, jnp.max(scores, axis=1))
        shrink = jnp.exp(max_head - new_max)
        exponents = jnp.exp(scores - new_max[:, None])
        sum_head = sum_head * shrink + jnp.sum(exponents, axis=1)
        weighted_head = weighted_head * shrink[:, None] + jnp.dot(
            exponents.astype(jnp.bfloat16), value_head, preferred_element_type=jnp.float32
        )
        return (new_max, sum_head, weighted_head)

    return lax.map(per_head, (queries, key_piece, value_piece, running_max, running_sum, weighted))


def empty_carry(head_count, query_count, head_width):
    return (
        jnp.full((head_count, query_count), -1e30, jnp.float32),
        jnp.zeros((head_count, query_count), jnp.float32),
        jnp.zeros((head_count, query_count, head_width), jnp.float32),
    )


def attend_keys(query_vectors, key_vectors, value_vectors, score_scale):
    head_count, row_count, head_width = query_vectors.shape
    initial = empty_carry(head_count, row_count, head_width)
    running_max, running_sum, weighted = fold_heads(
        initial,
        query_vectors,
        lax.all_gather(key_vectors, "ctx", axis=1, tiled=True),
        lax.all_gather(value_vectors, "ctx", axis=1, tiled=True),
        score_scale,
    )
    return (weighted / running_sum[..., None]).astype(jnp.bfloat16)


def on_device(
    state_rows, query_vectors, key_vectors, value_vectors, halt_counts, out_weight, norm_gain
):
    head_count, row_count, head_width = query_vectors.shape
    score_scale = head_width ** (-0.5)
    attended = attend_keys(query_vectors, key_vectors, value_vectors, score_scale)
    update = jnp.einsum("hqd,hde->qe", attended, out_weight, preferred_element_type=jnp.float32)
    mixed_sum = state_rows.astype(jnp.float32) + update
    normed = (
        mixed_sum
        * lax.rsqrt(jnp.mean(mixed_sum * mixed_sum, axis=-1, keepdims=True) + 1e-06)
        * norm_gain.astype(jnp.float32)
    )
    active = (halt_counts > STEP)[:, None]
    return jnp.where(active, normed.astype(jnp.bfloat16), state_rows)


def solution(mesh):
    n_ctx = mesh.shape["ctx"]

    def per_device(state_rows, q, k, v, halt_counts, out_weight, norm_gain):
        heads, rows, width = q.shape
        one_owner = rows == (n_ctx - 1) * TILE
        if one_owner and heads - 2 == 2 * LAG and width == TILE and n_ctx == 4:
            return on_star(state_rows, q, k, v, halt_counts, out_weight, norm_gain)
        return on_device(state_rows, q, k, v, halt_counts, out_weight, norm_gain)

    placed = (
        P(("dp", "ctx"), None),
        P(None, ("dp", "ctx"), None),
        P(None, ("dp", "ctx"), None),
        P(None, ("dp", "ctx"), None),
        P(("dp", "ctx")),
        P(),
        P(),
    )
    return jax.shard_map(
        per_device, mesh=mesh, in_specs=placed, out_specs=P(("dp", "ctx"), None), check_vma=False
    )
```

```python
import functools

import jax
import jax.numpy as jnp
from jax import lax
from jax.experimental import pallas as pl
from jax.experimental.pallas import tpu as pltpu
from jax.sharding import PartitionSpec as P

STEP = 2
TILE = 128
LAG = 3
SLOTS = 3 * LAG + 1
LOG2E = 1.4426950408889634


def slot_orders(heads):
    half = heads // 2
    first = [half]
    singles = [heads - 1, 0]
    for j in range(half - 1):
        first += [j + 1] + singles[j : j + 1]
    return first, [(h + half) % heads for h in first]


def star_kernel(
    halt_hbm,
    q_hbm,
    k_hbm,
    v_hbm,
    state_hbm,
    w_hbm,
    gain_hbm,
    first_ref,
    left_ref,
    update,
    w_last,
    state_buf,
    gain_buf,
    active_ref,
    halt,
    flag_out,
    flag_in,
    qkv_buf,
    slot_out,
    slot_in,
    stat_out,
    stat_in,
    own_part,
    own_stat,
    att_buf,
    w_buf,
    halt_sem,
    gain_sem,
    state_sem,
    w_sem,
    flag_send,
    flag_recv,
    slot_send,
    stat_send,
    qkv_sem,
    slot_recv,
    tile_recv,
    stat_recv,
):
    me = lax.axis_index("ctx")
    bits = (me % 2, me // 2)
    peer = (bits[1] * 2 + 1 - bits[0], (1 - bits[1]) * 2 + bits[0])
    heads, rows, width = q_hbm.shape
    features = state_hbm.shape[1]
    half = heads // 2
    early = heads - 2
    blocks = rows // TILE
    scale = width ** (-0.5) * LOG2E
    axes = (0, 1)
    orders = slot_orders(heads)
    f32, bf16 = jnp.float32, jnp.bfloat16

    def local(src, dst, sem):
        copy = pltpu.make_async_copy(src, dst, sem)
        copy.start()
        return copy

    def remote(src, dst, send, recv, axis):
        return pltpu.make_async_remote_copy(
            src_ref=src,
            dst_ref=dst,
            send_sem=send,
            recv_sem=recv,
            device_id={"ctx": peer[axis]},
            device_id_type=pl.DeviceIdType.MESH,
        )

    barrier = pltpu.get_barrier_semaphore()
    for axis in axes:
        pl.semaphore_signal(
            barrier, inc=1, device_id={"ctx": peer[axis]}, device_id_type=pl.DeviceIdType.MESH
        )
    halt_copy = local(halt_hbm, halt, halt_sem)

    def choices(s, axis):
        return (0, orders[axis][s]), (1 + s % 2, orders[1 - axis][2 * (s // 2) + 1])

    group_of = {}
    for s in range(LAG):
        for axis in axes:
            for block in choices(s, axis):
                group_of[block] = min(s, 1)
    for block in [(n, h) for h in range(heads) for n in range(3)]:
        group_of.setdefault(block, 2)
    for (n, h), group in group_of.items():
        local((q_hbm, k_hbm, v_hbm)[n].at[h], qkv_buf.at[n * heads + h], qkv_sem.at[group])
    loaded = set()

    def own(n, h):
        group = group_of[n, h]
        if group not in loaded:
            whole = qkv_buf.at[pl.ds(0, list(group_of.values()).count(group))]
            pltpu.make_async_copy(whole, whole, qkv_sem.at[group]).wait()
            loaded.add(group)
        return qkv_buf[n * heads + h]

    halt_copy.wait()
    flag = jnp.full(flag_out.shape, halt[0] > STEP).astype(f32)
    flag_out[...] = flag

    def mask(value):
        return jnp.broadcast_to(value[0:1, :].astype(bf16), (rows, width)) > 0.5

    is_owner = mask(flag)

    def opening(s, axis):
        mine, other = choices(s, axis)
        return jnp.where(is_owner, own(*mine), own(*other))

    def send(s):
        if s < SLOTS - 2:
            for axis in axes:
                remote(
                    slot_out.at[s, axis], slot_in.at[s, axis], slot_send, slot_recv.at[s], axis
                ).start()
            return
        for tile in range(blocks):
            for axis in axes:
                remote(
                    slot_out.at[s, axis, tile],
                    slot_in.at[s, axis, tile],
                    slot_send,
                    tile_recv.at[s - SLOTS + 2, tile],
                    axis,
                ).start()

    def wait_tile(s, tile):
        landed = slot_in.at[s, pl.ds(0, 2), tile]
        remote(landed, landed, slot_send, tile_recv.at[s - SLOTS + 2, tile], 0).wait_recv()

    def wait_stat(s):
        stat = s - LAG - 1
        remote(
            stat_in.at[stat], stat_in.at[stat], stat_send, stat_recv.at[stat], 0
        ).wait_recv()

    for s in range(LAG):
        for axis in axes:
            slot_out[s, axis] = opening(s, axis).reshape(blocks, TILE, width)
        if s == 0:
            pl.semaphore_wait(barrier, 2)
            for axis in axes:
                remote(flag_out, flag_in.at[axis], flag_send.at[axis], flag_recv, axis).start()
        send(s)

    for side in (0, 1):
        cut = pl.ds(side * width, width)
        local(w_hbm.at[pl.ds(side * half + 1, half - 1)], w_buf.at[:, cut], w_sem.at[0])
        local(w_hbm.at[side * half], w_last.at[cut], w_sem.at[1])
    state_copy = local(state_hbm, state_buf, state_sem)
    gain_copy = local(gain_hbm, gain_buf, gain_sem)

    remote(flag_in, flag_in, flag_send.at[0], flag_recv, 0).wait_recv()
    owner_at = [mask(flag_in[axis]) for axis in axes]
    beside = flag_in[0] + flag_in[1]
    is_beside = mask(beside)

    def bias(valid):
        return jnp.concatenate([(valid[0:1, :] - 1.0) * 1e30] * blocks, axis=1)

    def received(s, axis):
        return slot_in[s, axis].reshape(rows, width)

    def attend(query, keys, values):
        scores = lax.dot_general(
            keys, query, (((1,), (1,)), ((), ())), preferred_element_type=f32
        )
        top = jnp.max(scores, axis=0, keepdims=True)
        weights = jnp.exp2((scores - top) * scale)
        total = jnp.sum(weights, axis=0, keepdims=True)
        weighted = lax.dot_general(
            values, weights.astype(bf16), (((0,), (0,)), ((), ())), preferred_element_type=f32
        )
        return top * scale + jnp.log2(total), weighted * (1.0 / total)

    def merge(sources):
        top = functools.reduce(jnp.maximum, [level for level, _ in sources])
        sums = [jnp.exp2(level - top) for level, _ in sources]
        total = functools.reduce(jnp.add, sums)
        inverse = 1.0 / total
        parts = [part * (each * inverse) for each, (_, part) in zip(sums, sources)]
        return top + jnp.log2(total), functools.reduce(jnp.add, parts)

    def put(s, results):
        for axis in axes:
            stat_out[s - LAG - 1, axis], part = results[axis]
            part = part.astype(bf16)
            block = opening(s, axis) if s < early else None
            for tile in range(blocks):
                cut = slice(tile * TILE, (tile + 1) * TILE)
                piece = part[:, cut]
                if s < early:
                    piece = jnp.where(is_beside[cut], piece, block[cut])
                slot_out[s, axis, tile] = piece
            remote(
                stat_out.at[s - LAG - 1, axis],
                stat_in.at[s - LAG - 1, axis],
                stat_send,
                stat_recv.at[s - LAG - 1],
                axis,
            ).start()
        send(s)

    def keep(h, result):
        own_stat[h], own_part[h] = result

    def cut_of(tiles):
        return slice(tiles[0] * TILE, (tiles[-1] + 1) * TILE)

    def kept(h, tiles=range(blocks)):
        cut = cut_of(tiles)
        return own_stat[h, :, cut], own_part[h, :, cut]

    def sent(s, axis, tiles=range(blocks)):
        cut, stat = cut_of(tiles), s - LAG - 1
        block = jnp.concatenate([slot_in[s, axis, tile] for tile in tiles], axis=1)
        return stat_in[stat, axis, :, cut], block.astype(f32)

    def select(value, first, second):
        line = jnp.concatenate([value[0:1, :]] * blocks, axis=1)
        return tuple(
            jnp.where(jnp.broadcast_to(line, a.shape) > 0.5, a, b) for a, b in zip(first, second)
        )

    def step(s):
        high, low = orders[0][s], orders[1][s]
        query = jnp.where(
            owner_at[0], received(s, 0), jnp.where(owner_at[1], received(s, 1), own(0, low))
        )
        key = jnp.where(owner_at[0], own(1, high), own(1, low))
        value = jnp.where(owner_at[0], own(2, high), own(2, low))
        if s % 2 == 0:
            result = attend(query, key, value)
            keep(low, result)
            if s > 0:
                put(s + LAG, (result, result))
            else:
                for axis in axes:
                    block = jnp.where(owner_at[1 - axis], query, opening(LAG, axis))
                    slot_out[LAG, axis] = block.reshape(blocks, TILE, width)
                send(LAG)
            return
        far_key = jnp.where(owner_at[0], received(s - 1, 1), received(s - 1, 0))
        far_value = jnp.where(owner_at[0], received(s, 1), received(s, 0))
        far_query = query
        valid = beside if s > LAG else beside + flag
        if s == LAG:
            far, near = orders[0][0], orders[1][0]
            take = mask(flag + beside)
            query = jnp.where(take, query, received(s, 1))
            key = jnp.where(take, key, own(1, far))
            value = jnp.where(take, value, own(2, far))
            far_query = jnp.where(take, far_query, received(s, 0))
            far_key = jnp.where(take, far_key, own(1, near))
            far_value = jnp.where(take, far_value, own(2, near))
        nearby = attend(query, key, value)
        distant = attend(far_query, far_key, far_value)
        result = merge((nearby, (distant[0] + bias(valid), distant[1])))
        keep(low, result)
        if s == LAG:
            put(
                s + LAG,
                (select(beside, result, distant), select(beside, result, nearby)),
            )
        else:
            put(s + LAG, (result, result))
        if s <= LAG:
            nearby = attend(own(0, high), own(1, high), own(2, high))
            distant = attend(own(0, high), received(s - 1, 1), received(s, 1))
            keep(high, merge((nearby, distant)))

    def finish_first():
        near, far = orders[1][0], 2 * LAG
        result = merge((kept(near), select(flag_in[0], sent(far, 1), sent(far, 0))))
        put(SLOTS - 1, (result, result))

    def combine(i, tiles=range(blocks)):
        for side in (0, 1):
            h = i + side * half
            sources = [kept(h, tiles)]
            for axis in axes:
                if h in orders[axis]:
                    s = orders[axis].index(h)
                    sources.append(sent(s + LAG if s > 0 else SLOTS - 1, axis, tiles))
            attended = merge(sources)[1]
            att_buf[i, cut_of(tiles), side * width : (side + 1) * width] = attended.T.astype(bf16)

    chunk = min(4 * TILE, features)

    def project(i, initial):
        left = att_buf[i]

        def body(n, carry):
            cut = pl.ds(pl.multiple_of(n * chunk, chunk), chunk)
            product = jnp.dot(left, w_buf[i - 1, :, cut], preferred_element_type=f32)
            if initial:
                update[:, cut] = state_buf[:, cut].astype(f32) + product
            else:
                update[:, cut] = update[:, cut] + product
            return carry

        lax.fori_loop(0, features // chunk, body, 0)

    for s in range(SLOTS - 2):
        remote(slot_in.at[s], slot_in.at[s], slot_send, slot_recv.at[s], 0).wait_recv()
        if s > LAG:
            wait_stat(s)
        if s < early:
            step(s)
        elif s == early:
            finish_first()
        if s > LAG and s % 2 == 0:
            i = s // 2 - 1
            if i == 1:
                pltpu.make_async_copy(w_buf, w_buf, w_sem.at[0]).wait()
                pltpu.make_async_copy(w_last, w_last, w_sem.at[1]).wait()
                state_copy.wait()
                gain_copy.wait()
            combine(i)
            project(i, i == 1)

    wait_stat(SLOTS - 2)
    for tile in range(blocks):
        wait_tile(SLOTS - 2, tile)
        combine(half - 1, [tile])
        cut = cut_of([tile])
        add_product(att_buf[half - 1, cut, :], w_buf.at[half - 2], update.at[cut], update.at[cut])
        active = jnp.full(active_ref.shape[1:], halt[tile * TILE] > STEP)
        active_ref[tile] = active.astype(f32)

    wait_stat(SLOTS - 1)
    wait_tile(SLOTS - 1, 0)
    combine(0, [0])
    cut = cut_of([0])
    squares = add_product(att_buf[0, cut, :], w_last, update.at[cut], update.at[cut])
    normalize(squares, update.at[cut], gain_buf, active_ref[0], state_buf.at[cut], first_ref)
    rest = list(range(1, blocks))
    for tile in rest:
        wait_tile(SLOTS - 1, tile)
    combine(0, rest)
    left_ref[...] = att_buf[0, cut_of(rest), :]

    remote(slot_out, slot_in, slot_send, slot_recv.at[0], 0).wait_send()
    remote(stat_out, stat_in, stat_send, stat_recv.at[0], 0).wait_send()
    for axis in axes:
        remote(flag_out, flag_in.at[axis], flag_send.at[axis], flag_recv, axis).wait_send()


def strips_of(ref):
    return [slice(n, n + 2 * TILE) for n in range(0, ref.shape[1], 2 * TILE)]


def add_product(left, weight, base, mixed):
    squares = jnp.zeros((left.shape[0], TILE), jnp.float32)
    for strip in strips_of(base):
        product = jnp.dot(left, weight[:, strip], preferred_element_type=jnp.float32)
        total = base[:, strip] + product
        mixed[:, strip] = total
        squares = squares + total[:, :TILE] * total[:, :TILE]
        squares = squares + total[:, TILE:] * total[:, TILE:]
    return squares


def normalize(squares, mixed, gain_ref, active, state, out):
    mean = jnp.sum(squares, axis=-1, keepdims=True) / mixed.shape[1]
    inverse = lax.rsqrt(mean + 1e-06)
    chosen = jnp.broadcast_to(active[0:1, :].astype(jnp.bfloat16), (TILE, TILE))
    chosen = jnp.concatenate([chosen, chosen], axis=1) > 0.5
    for strip in strips_of(mixed):
        gain = gain_ref[strip].astype(jnp.float32).reshape(1, -1)
        normed = (mixed[:, strip] * inverse * gain).astype(jnp.bfloat16)
        out[:, strip] = jnp.where(chosen, normed, state[:, strip])


def finish_kernel(
    first_ref, left_ref, update, w_last, state_ref, gain_ref, active_ref, out_hbm, mixed, done, sem
):
    def store(source, tile):
        copy = pltpu.make_async_copy(source, out_hbm.at[pl.ds(tile * TILE, TILE)], sem.at[tile])
        copy.start()
        return copy

    copies = [store(first_ref, 0)]
    squares = add_product(left_ref[...], w_last, update.at[pl.ds(TILE, mixed.shape[0])], mixed)
    for tile in range(mixed.shape[0] // TILE):
        cut, full = pl.ds(tile * TILE, TILE), pl.ds((tile + 1) * TILE, TILE)
        normalize(
            squares[tile * TILE : (tile + 1) * TILE],
            mixed.at[cut],
            gain_ref,
            active_ref[tile + 1],
            state_ref.at[full],
            done.at[cut],
        )
        copies.append(store(done.at[cut], tile + 1))
    for copy in copies:
        copy.wait()


def on_star(state_rows, q, k, v, halt_counts, out_weight, norm_gain):
    heads, rows, width = q.shape
    features = state_rows.shape[1]
    half, blocks, stats = heads // 2, rows // TILE, SLOTS - LAG - 1
    bf16, f32 = jnp.bfloat16, jnp.float32
    hbm = pl.BlockSpec(memory_space=pltpu.MemorySpace.HBM)
    vmem = pl.BlockSpec(memory_space=pltpu.VMEM)
    dma = pltpu.SemaphoreType.DMA
    operands = (halt_counts, q, k, v, state_rows, out_weight, norm_gain)
    handed = (
        ((TILE, features), bf16),
        ((rows - TILE, 2 * width), bf16),
        ((rows, features), f32),
        ((2 * width, features), bf16),
        ((rows, features), bf16),
        ((features,), bf16),
        ((blocks, 8, TILE), f32),
    )
    results = pl.pallas_call(
        star_kernel,
        out_shape=[jax.ShapeDtypeStruct(*each) for each in handed],
        in_specs=[hbm] * len(operands),
        out_specs=[vmem] * len(handed),
        scratch_shapes=[
            pltpu.SMEM((rows,), jnp.int32),
            pltpu.VMEM((8, width), f32),
            pltpu.VMEM((2, 8, width), f32),
            pltpu.VMEM((3 * heads, rows, width), bf16),
            pltpu.VMEM((SLOTS, 2, blocks, TILE, width), bf16),
            pltpu.VMEM((SLOTS, 2, blocks, TILE, width), bf16),
            pltpu.VMEM((stats, 2, 1, rows), f32),
            pltpu.VMEM((stats, 2, 1, rows), f32),
            pltpu.VMEM((heads, width, rows), f32),
            pltpu.VMEM((heads, 1, rows), f32),
            pltpu.VMEM((half, rows, 2 * width), bf16),
            pltpu.VMEM((half - 1, 2 * width, features), bf16),
            dma,
            dma,
            dma,
            dma((2,)),
            dma((2,)),
            dma,
            dma,
            dma,
            dma((3,)),
            dma((SLOTS - 2,)),
            dma((2, blocks)),
            dma((stats,)),
        ],
        compiler_params=pltpu.CompilerParams(
            collective_id=0, has_side_effects=True, vmem_limit_bytes=32 * 1024 * 1024
        ),
    )(*[pltpu.with_memory_space_constraint(x, pltpu.HBM) for x in operands])
    return pl.pallas_call(
        finish_kernel,
        out_shape=jax.ShapeDtypeStruct((rows, features), bf16),
        in_specs=[vmem] * len(handed),
        out_specs=hbm,
        scratch_shapes=[
            pltpu.VMEM((rows - TILE, features), f32),
            pltpu.VMEM((rows - TILE, features), bf16),
            dma((blocks,)),
        ],
        compiler_params=pltpu.CompilerParams(vmem_limit_bytes=8 * 1024 * 1024),
    )(*results)


def fold_heads(carry, queries, key_piece, value_piece, score_scale):
    running_max, running_sum, weighted = carry

    def per_head(head_items):
        query_head, key_head, value_head, max_head, sum_head, weighted_head = head_items
        scores = (
            lax.dot_general(
                query_head, key_head, (((1,), (1,)), ((), ())), preferred_element_type=jnp.float32
            )
            * score_scale
        )
        new_max = jnp.maximum(max_head, jnp.max(scores, axis=1))
        shrink = jnp.exp(max_head - new_max)
        exponents = jnp.exp(scores - new_max[:, None])
        sum_head = sum_head * shrink + jnp.sum(exponents, axis=1)
        weighted_head = weighted_head * shrink[:, None] + jnp.dot(
            exponents.astype(jnp.bfloat16), value_head, preferred_element_type=jnp.float32
        )
        return (new_max, sum_head, weighted_head)

    return lax.map(per_head, (queries, key_piece, value_piece, running_max, running_sum, weighted))


def empty_carry(head_count, query_count, head_width):
    return (
        jnp.full((head_count, query_count), -1e30, jnp.float32),
        jnp.zeros((head_count, query_count), jnp.float32),
        jnp.zeros((head_count, query_count, head_width), jnp.float32),
    )


def attend_keys(query_vectors, key_vectors, value_vectors, score_scale):
    head_count, row_count, head_width = query_vectors.shape
    initial = empty_carry(head_count, row_count, head_width)
    running_max, running_sum, weighted = fold_heads(
        initial,
        query_vectors,
        lax.all_gather(key_vectors, "ctx", axis=1, tiled=True),
        lax.all_gather(value_vectors, "ctx", axis=1, tiled=True),
        score_scale,
    )
    return (weighted / running_sum[..., None]).astype(jnp.bfloat16)


def on_device(
    state_rows, query_vectors, key_vectors, value_vectors, halt_counts, out_weight, norm_gain
):
    head_count, row_count, head_width = query_vectors.shape
    score_scale = head_width ** (-0.5)
    attended = attend_keys(query_vectors, key_vectors, value_vectors, score_scale)
    update = jnp.einsum("hqd,hde->qe", attended, out_weight, preferred_element_type=jnp.float32)
    mixed_sum = state_rows.astype(jnp.float32) + update
    normed = (
        mixed_sum
        * lax.rsqrt(jnp.mean(mixed_sum * mixed_sum, axis=-1, keepdims=True) + 1e-06)
        * norm_gain.astype(jnp.float32)
    )
    active = (halt_counts > STEP)[:, None]
    return jnp.where(active, normed.astype(jnp.bfloat16), state_rows)


def solution(mesh):
    n_ctx = mesh.shape["ctx"]

    def per_device(state_rows, q, k, v, halt_counts, out_weight, norm_gain):
        heads, rows, width = q.shape
        one_owner = rows == (n_ctx - 1) * TILE
        if one_owner and heads - 2 == 2 * LAG and width == TILE and n_ctx == 4:
            return on_star(state_rows, q, k, v, halt_counts, out_weight, norm_gain)
        return on_device(state_rows, q, k, v, halt_counts, out_weight, norm_gain)

    placed = (
        P(("dp", "ctx"), None),
        P(None, ("dp", "ctx"), None),
        P(None, ("dp", "ctx"), None),
        P(None, ("dp", "ctx"), None),
        P(("dp", "ctx")),
        P(),
        P(),
    )
    return jax.shard_map(
        per_device, mesh=mesh, in_specs=placed, out_specs=P(("dp", "ctx"), None), check_vma=False
    )
```

```python
import functools

import jax
import jax.numpy as jnp
from jax import lax
from jax.experimental import pallas as pl
from jax.experimental.pallas import tpu as pltpu
from jax.sharding import PartitionSpec as P

STEP = 2
TILE = 128
LEAD = 8
LOG2E = 1.4426950408889634


def head_orders(heads):
    half = heads // 2
    singles = [0, heads - 1, heads - 2]
    first = []
    for j in range(half - 1):
        first += [singles[j], j + 1]
    first.append(half)
    return first, [(h + half) % heads for h in first]


def star_kernel(
    halt_hbm,
    q_hbm,
    k_hbm,
    v_hbm,
    state_hbm,
    w_hbm,
    gain_hbm,
    first_ref,
    left_ref,
    update,
    w_last,
    state_buf,
    gain_buf,
    active_ref,
    halt,
    flag_out,
    flag_in,
    qkv_buf,
    tile_out,
    tile_in,
    far_part,
    stat_out,
    stat_in,
    own_part,
    own_stat,
    att_buf,
    w_buf,
    halt_sem,
    gain_sem,
    state_sem,
    w_sem,
    flag_send,
    flag_recv,
    tile_send,
    stat_send,
    qkv_sem,
    tile_recv,
    stat_recv,
):
    me = lax.axis_index("ctx")
    bits = (me % 2, me // 2)
    peer = (bits[1] * 2 + 1 - bits[0], (1 - bits[1]) * 2 + bits[0])
    heads, rows, width = q_hbm.shape
    features = state_hbm.shape[1]
    half = heads // 2
    steps = heads - 1
    inputs = heads - 2
    blocks = rows // TILE
    meeting = blocks
    scale = width ** (-0.5) * LOG2E
    axes = (0, 1)
    orders = head_orders(heads)
    f32, bf16 = jnp.float32, jnp.bfloat16

    def local(src, dst, sem):
        copy = pltpu.make_async_copy(src, dst, sem)
        copy.start()
        return copy

    def remote(src, dst, send, recv, axis):
        return pltpu.make_async_remote_copy(
            src_ref=src,
            dst_ref=dst,
            send_sem=send,
            recv_sem=recv,
            device_id={"ctx": peer[axis]},
            device_id_type=pl.DeviceIdType.MESH,
        )

    barrier = pltpu.get_barrier_semaphore()
    for axis in axes:
        pl.semaphore_signal(
            barrier, inc=1, device_id={"ctx": peer[axis]}, device_id_type=pl.DeviceIdType.MESH
        )
    halt_copy = local(halt_hbm, halt, halt_sem)

    def choices(b, axis):
        return (0, orders[axis][b]), (1 + b % 2, orders[1 - axis][2 * (b // 2) + 1])

    group_of = {}
    for b in range(blocks):
        for axis in axes:
            for block in choices(b, axis):
                group_of[block] = min(b, 1)
    for block in [(n, h) for h in range(heads) for n in range(3)]:
        group_of.setdefault(block, 2)
    for (n, h), group in group_of.items():
        local((q_hbm, k_hbm, v_hbm)[n].at[h], qkv_buf.at[n * heads + h], qkv_sem.at[group])
    loaded = set()

    def own(n, h):
        group = group_of[n, h]
        if group not in loaded:
            whole = qkv_buf.at[pl.ds(0, list(group_of.values()).count(group))]
            pltpu.make_async_copy(whole, whole, qkv_sem.at[group]).wait()
            loaded.add(group)
        return qkv_buf[n * heads + h]

    halt_copy.wait()
    flag = jnp.full(flag_out.shape, halt[0] > STEP).astype(f32)
    flag_out[...] = flag

    def mask(value):
        return jnp.broadcast_to(value[0:1, :].astype(bf16), (rows, width)) > 0.5

    is_owner = mask(flag)

    def cut_of(tiles):
        return slice(tiles[0] * TILE, (tiles[-1] + 1) * TILE)

    def input_tile(u, axis):
        b, cut = u // blocks, cut_of([u % blocks])
        if b < inputs:
            mine, other = choices(b, axis)
            return jnp.where(is_owner[cut], own(*mine)[cut], own(*other)[cut])
        return jnp.where(is_owner[cut], own(0, orders[axis][b])[cut], far_part[axis, :, cut])

    groups = [(u, min(blocks, LEAD - u)) for u in range(0, LEAD, blocks)]
    for p in range(steps):
        groups += [(LEAD + blocks * p, 1), (LEAD + blocks * p + 1, blocks - 1)]

    def send(n):
        start, count = groups[n]
        for axis in axes:
            remote(
                tile_out.at[axis, pl.ds(start, count)],
                tile_in.at[axis, pl.ds(start, count)],
                tile_send,
                tile_recv.at[n],
                axis,
            ).start()

    waited = []

    def wait_tiles(u):
        while sum(count for _, count in groups[: len(waited)]) <= u:
            n = len(waited)
            start, count = groups[n]
            landed = tile_in.at[pl.ds(0, 2), pl.ds(start, count)]
            remote(landed, landed, tile_send, tile_recv.at[n], 0).wait_recv()
            waited.append(n)

    known = []

    def wait_stats(p):
        while len(known) <= p:
            n = len(known)
            remote(stat_in.at[n], stat_in.at[n], stat_send, stat_recv.at[n], 0).wait_recv()
            known.append(n)

    for n, (start, count) in enumerate(groups[: len(range(0, LEAD, blocks))]):
        for axis in axes:
            for u in range(start, start + count):
                tile_out[axis, u] = input_tile(u, axis)
        if n == 0:
            pl.semaphore_wait(barrier, 2)
            for axis in axes:
                remote(flag_out, flag_in.at[axis], flag_send.at[axis], flag_recv, axis).start()
        send(n)

    for side in (0, 1):
        cut = pl.ds(side * width, width)
        local(w_hbm.at[pl.ds(side * half + 1, half - 1)], w_buf.at[:, cut], w_sem.at[0])
        local(w_hbm.at[side * half], w_last.at[cut], w_sem.at[1])
    state_copy = local(state_hbm, state_buf, state_sem)
    gain_copy = local(gain_hbm, gain_buf, gain_sem)

    remote(flag_in, flag_in, flag_send.at[0], flag_recv, 0).wait_recv()
    owner_at = [mask(flag_in[axis]) for axis in axes]
    beside = flag_in[0] + flag_in[1]
    is_beside = mask(beside)

    def bias(valid):
        return jnp.concatenate([(valid[0:1, :] - 1.0) * 1e30] * blocks, axis=1)

    def received(b, axis):
        return tile_in[axis, b * blocks : (b + 1) * blocks].reshape(rows, width)

    def attend(query, keys, values):
        scores = lax.dot_general(
            keys, query, (((1,), (1,)), ((), ())), preferred_element_type=f32
        )
        top = jnp.max(scores, axis=0, keepdims=True)
        weights = jnp.exp2((scores - top) * scale)
        total = jnp.sum(weights, axis=0, keepdims=True)
        weighted = lax.dot_general(
            values, weights.astype(bf16), (((0,), (0,)), ((), ())), preferred_element_type=f32
        )
        return top * scale + jnp.log2(total), weighted * (1.0 / total)

    def merge(sources):
        top = functools.reduce(jnp.maximum, [level for level, _ in sources])
        sums = [jnp.exp2(level - top) for level, _ in sources]
        total = functools.reduce(jnp.add, sums)
        inverse = 1.0 / total
        parts = [part * (each * inverse) for each, (_, part) in zip(sums, sources)]
        return top + jnp.log2(total), functools.reduce(jnp.add, parts)

    def put(p, level, part, query=None):
        part = part.astype(bf16)
        for axis in axes:
            stat_out[p, axis] = level[axis]
            for tile in range(blocks):
                u, cut = LEAD + blocks * p + tile, cut_of([tile])
                piece = part[:, cut]
                if query is not None:
                    piece = jnp.where(owner_at[1 - axis][cut], query[cut], piece)
                if u < steps * blocks:
                    piece = jnp.where(is_beside[cut], piece, input_tile(u, axis))
                tile_out[axis, u] = piece
            remote(
                stat_out.at[p, axis], stat_in.at[p, axis], stat_send, stat_recv.at[p], axis
            ).start()
        first = len(groups) - 2 * (steps - p)
        send(first)
        send(first + 1)

    def keep(h, result):
        own_stat[h], own_part[h] = result

    def kept(h, tiles=range(blocks)):
        cut = cut_of(tiles)
        return own_stat[h, :, cut], own_part[h, :, cut]

    def sent(p, axis, tiles=range(blocks), start=None):
        start = LEAD + blocks * p if start is None else start
        block = jnp.concatenate([tile_in[axis, start + tile] for tile in tiles], axis=1)
        return stat_in[p, axis, :, cut_of(tiles)], block.astype(f32)

    def select(value, first, second):
        line = jnp.concatenate([value[0:1, :]] * blocks, axis=1)
        return tuple(
            jnp.where(jnp.broadcast_to(line, a.shape) > 0.5, a, b) for a, b in zip(first, second)
        )

    def step(s):
        high, low = orders[0][s], orders[1][s]
        query = jnp.where(
            owner_at[0], received(s, 0), jnp.where(owner_at[1], received(s, 1), own(0, low))
        )
        key = jnp.where(owner_at[0], own(1, high), own(1, low))
        value = jnp.where(owner_at[0], own(2, high), own(2, low))
        if s % 2 == 0:
            result = attend(query, key, value)
            keep(low, result)
            if s == inputs:
                start, p = s * blocks, meeting
                far = select(
                    flag_in[0], sent(p, 1, start=start), sent(p, 0, start=start)
                )
                result = merge((result, far))
            put(s, [result[0]] * 2, result[1], query if s == 0 else None)
            return
        far_key = jnp.where(owner_at[0], received(s - 1, 1), received(s - 1, 0))
        far_value = jnp.where(owner_at[0], received(s, 1), received(s, 0))
        far_query = query
        valid = beside + flag if s == 1 else beside
        if s == meeting:
            one, two = (
                jnp.concatenate([tile_in[axis, LEAD + tile] for tile in range(blocks)], axis=0)
                for axis in axes
            )
            take = mask(flag + beside)
            query = jnp.where(take, query, two)
            key = jnp.where(take, key, own(1, orders[0][0]))
            value = jnp.where(take, value, own(2, orders[0][0]))
            far_query = jnp.where(take, far_query, one)
            far_key = jnp.where(take, far_key, own(1, orders[1][0]))
            far_value = jnp.where(take, far_value, own(2, orders[1][0]))
        nearby = attend(query, key, value)
        distant = attend(far_query, far_key, far_value)
        result = merge((nearby, (distant[0] + bias(valid), distant[1])))
        keep(low, result)
        level = [result[0]] * 2
        if s == meeting:
            for axis, each in enumerate((nearby, distant)):
                far_part[axis] = each[1].astype(bf16)
                level[axis] = select(beside, result[:1], each[:1])[0]
        put(s, level, result[1])
        if s == 1:
            nearby = attend(own(0, high), own(1, high), own(2, high))
            distant = attend(own(0, high), received(s - 1, 1), received(s, 1))
            keep(high, merge((nearby, distant)))

    def combine(i, tiles=range(blocks)):
        for side in (0, 1):
            h = i + side * half
            sources = [kept(h, tiles)]
            for axis in axes:
                if h in orders[axis]:
                    sources.append(sent(orders[axis].index(h), axis, tiles))
            attended = merge(sources)[1]
            att_buf[i, cut_of(tiles), side * width : (side + 1) * width] = attended.T.astype(bf16)

    chunk = min(4 * TILE, features)

    def project(i, initial):
        left = att_buf[i]

        def body(n, carry):
            cut = pl.ds(pl.multiple_of(n * chunk, chunk), chunk)
            product = jnp.dot(left, w_buf[i - 1, :, cut], preferred_element_type=f32)
            if initial:
                update[:, cut] = state_buf[:, cut].astype(f32) + product
            else:
                update[:, cut] = update[:, cut] + product
            return carry

        lax.fori_loop(0, features // chunk, body, 0)

    def result_tile(p, tile):
        return LEAD + blocks * p + tile

    for s in range(steps):
        wait_tiles((s + 1) * blocks - 1)
        if s == inputs:
            wait_stats(meeting)
        step(s)
        if s == half:
            pltpu.make_async_copy(w_buf, w_buf, w_sem.at[0]).wait()
            pltpu.make_async_copy(w_last, w_last, w_sem.at[1]).wait()
            state_copy.wait()
            gain_copy.wait()
            wait_stats(1)
            combine(1)
            project(1, True)
    for i in range(2, half - 1):
        p = max(order.index(i) for order in orders)
        wait_tiles(result_tile(p, blocks - 1))
        wait_stats(p)
        combine(i)
        project(i, False)

    i, p, rest = half - 1, steps - 2, list(range(1, blocks))
    for tiles in ([0], rest):
        wait_tiles(result_tile(p, tiles[-1]))
        wait_stats(p)
        combine(i, tiles)
        cut = cut_of(tiles)
        add_product(att_buf[i, cut, :], w_buf.at[i - 1], update.at[cut], update.at[cut])
        for tile in tiles:
            active = jnp.full(active_ref.shape[1:], halt[tile * TILE] > STEP)
            active_ref[tile] = active.astype(f32)

    p = steps - 1
    wait_stats(p)
    wait_tiles(result_tile(p, 0))
    combine(0, [0])
    cut = cut_of([0])
    squares = add_product(att_buf[0, cut, :], w_last, update.at[cut], update.at[cut])
    normalize(squares, update.at[cut], gain_buf, active_ref[0], state_buf.at[cut], first_ref)
    wait_tiles(result_tile(p, blocks - 1))
    combine(0, rest)
    left_ref[...] = att_buf[0, cut_of(rest), :]

    remote(tile_out, tile_in, tile_send, tile_recv.at[0], 0).wait_send()
    remote(stat_out, stat_in, stat_send, stat_recv.at[0], 0).wait_send()
    for axis in axes:
        remote(flag_out, flag_in.at[axis], flag_send.at[axis], flag_recv, axis).wait_send()


def strips_of(ref):
    return [slice(n, n + 4 * TILE) for n in range(0, ref.shape[1], 4 * TILE)]


def add_product(left, weight, base, mixed):
    squares = jnp.zeros((left.shape[0], TILE), jnp.float32)
    for strip in strips_of(base):
        product = jnp.dot(left, weight[:, strip], preferred_element_type=jnp.float32)
        total = base[:, strip] + product
        mixed[:, strip] = total
        for n in range(0, total.shape[1], TILE):
            squares = squares + total[:, n : n + TILE] * total[:, n : n + TILE]
    return squares


def normalize(squares, mixed, gain_ref, active, state, out):
    mean = jnp.sum(squares, axis=-1, keepdims=True) / mixed.shape[1]
    inverse = lax.rsqrt(mean + 1e-06)
    chosen = jnp.broadcast_to(active[0:1, :].astype(jnp.bfloat16), (TILE, TILE))
    chosen = jnp.concatenate([chosen] * 4, axis=1) > 0.5
    for strip in strips_of(mixed):
        gain = gain_ref[strip].astype(jnp.float32).reshape(1, -1)
        normed = (mixed[:, strip] * inverse * gain).astype(jnp.bfloat16)
        out[:, strip] = jnp.where(chosen, normed, state[:, strip])


def finish_kernel(
    first_ref, left_ref, update, w_last, state_ref, gain_ref, active_ref, out_hbm, mixed, done, sem
):
    def store(source, tile):
        copy = pltpu.make_async_copy(source, out_hbm.at[pl.ds(tile * TILE, TILE)], sem.at[tile])
        copy.start()
        return copy

    copies = [store(first_ref, 0)]
    squares = add_product(left_ref[...], w_last, update.at[pl.ds(TILE, mixed.shape[0])], mixed)
    for tile in range(mixed.shape[0] // TILE):
        cut, full = pl.ds(tile * TILE, TILE), pl.ds((tile + 1) * TILE, TILE)
        normalize(
            squares[tile * TILE : (tile + 1) * TILE],
            mixed.at[cut],
            gain_ref,
            active_ref[tile + 1],
            state_ref.at[full],
            done.at[cut],
        )
        copies.append(store(done.at[cut], tile + 1))
    for copy in copies:
        copy.wait()


def on_star(state_rows, q, k, v, halt_counts, out_weight, norm_gain):
    heads, rows, width = q.shape
    features = state_rows.shape[1]
    half, blocks, steps = heads // 2, rows // TILE, heads - 1
    tiles = LEAD + steps * blocks
    groups = pl.cdiv(LEAD, blocks) + 2 * steps
    bf16, f32 = jnp.bfloat16, jnp.float32
    hbm = pl.BlockSpec(memory_space=pltpu.MemorySpace.HBM)
    vmem = pl.BlockSpec(memory_space=pltpu.VMEM)
    dma = pltpu.SemaphoreType.DMA
    operands = (halt_counts, q, k, v, state_rows, out_weight, norm_gain)
    handed = (
        ((TILE, features), bf16),
        ((rows - TILE, 2 * width), bf16),
        ((rows, features), f32),
        ((2 * width, features), bf16),
        ((rows, features), bf16),
        ((features,), bf16),
        ((blocks, 8, TILE), f32),
    )
    results = pl.pallas_call(
        star_kernel,
        out_shape=[jax.ShapeDtypeStruct(*each) for each in handed],
        in_specs=[hbm] * len(operands),
        out_specs=[vmem] * len(handed),
        scratch_shapes=[
            pltpu.SMEM((rows,), jnp.int32),
            pltpu.VMEM((8, width), f32),
            pltpu.VMEM((2, 8, width), f32),
            pltpu.VMEM((3 * heads, rows, width), bf16),
            pltpu.VMEM((2, tiles, TILE, width), bf16),
            pltpu.VMEM((2, tiles, TILE, width), bf16),
            pltpu.VMEM((2, width, rows), bf16),
            pltpu.VMEM((steps, 2, 1, rows), f32),
            pltpu.VMEM((steps, 2, 1, rows), f32),
            pltpu.VMEM((heads, width, rows), f32),
            pltpu.VMEM((heads, 1, rows), f32),
            pltpu.VMEM((half, rows, 2 * width), bf16),
            pltpu.VMEM((half - 1, 2 * width, features), bf16),
            dma,
            dma,
            dma,
            dma((2,)),
            dma((2,)),
            dma,
            dma,
            dma,
            dma((3,)),
            dma((groups,)),
            dma((steps,)),
        ],
        compiler_params=pltpu.CompilerParams(
            collective_id=0, has_side_effects=True, vmem_limit_bytes=32 * 1024 * 1024
        ),
    )(*[pltpu.with_memory_space_constraint(x, pltpu.HBM) for x in operands])
    return pl.pallas_call(
        finish_kernel,
        out_shape=jax.ShapeDtypeStruct((rows, features), bf16),
        in_specs=[vmem] * len(handed),
        out_specs=hbm,
        scratch_shapes=[
            pltpu.VMEM((rows - TILE, features), f32),
            pltpu.VMEM((rows - TILE, features), bf16),
            dma((blocks,)),
        ],
        compiler_params=pltpu.CompilerParams(vmem_limit_bytes=8 * 1024 * 1024),
    )(*results)


def fold_heads(carry, queries, key_piece, value_piece, score_scale):
    running_max, running_sum, weighted = carry

    def per_head(head_items):
        query_head, key_head, value_head, max_head, sum_head, weighted_head = head_items
        scores = (
            lax.dot_general(
                query_head, key_head, (((1,), (1,)), ((), ())), preferred_element_type=jnp.float32
            )
            * score_scale
        )
        new_max = jnp.maximum(max_head, jnp.max(scores, axis=1))
        shrink = jnp.exp(max_head - new_max)
        exponents = jnp.exp(scores - new_max[:, None])
        sum_head = sum_head * shrink + jnp.sum(exponents, axis=1)
        weighted_head = weighted_head * shrink[:, None] + jnp.dot(
            exponents.astype(jnp.bfloat16), value_head, preferred_element_type=jnp.float32
        )
        return (new_max, sum_head, weighted_head)

    return lax.map(per_head, (queries, key_piece, value_piece, running_max, running_sum, weighted))


def empty_carry(head_count, query_count, head_width):
    return (
        jnp.full((head_count, query_count), -1e30, jnp.float32),
        jnp.zeros((head_count, query_count), jnp.float32),
        jnp.zeros((head_count, query_count, head_width), jnp.float32),
    )


def attend_keys(query_vectors, key_vectors, value_vectors, score_scale):
    head_count, row_count, head_width = query_vectors.shape
    initial = empty_carry(head_count, row_count, head_width)
    running_max, running_sum, weighted = fold_heads(
        initial,
        query_vectors,
        lax.all_gather(key_vectors, "ctx", axis=1, tiled=True),
        lax.all_gather(value_vectors, "ctx", axis=1, tiled=True),
        score_scale,
    )
    return (weighted / running_sum[..., None]).astype(jnp.bfloat16)


def on_device(
    state_rows, query_vectors, key_vectors, value_vectors, halt_counts, out_weight, norm_gain
):
    head_count, row_count, head_width = query_vectors.shape
    score_scale = head_width ** (-0.5)
    attended = attend_keys(query_vectors, key_vectors, value_vectors, score_scale)
    update = jnp.einsum("hqd,hde->qe", attended, out_weight, preferred_element_type=jnp.float32)
    mixed_sum = state_rows.astype(jnp.float32) + update
    normed = (
        mixed_sum
        * lax.rsqrt(jnp.mean(mixed_sum * mixed_sum, axis=-1, keepdims=True) + 1e-06)
        * norm_gain.astype(jnp.float32)
    )
    active = (halt_counts > STEP)[:, None]
    return jnp.where(active, normed.astype(jnp.bfloat16), state_rows)


def solution(mesh):
    n_ctx = mesh.shape["ctx"]

    def per_device(state_rows, q, k, v, halt_counts, out_weight, norm_gain):
        heads, rows, width = q.shape
        one_owner = rows == (n_ctx - 1) * TILE
        if one_owner and heads == LEAD and width == TILE and n_ctx == 4:
            return on_star(state_rows, q, k, v, halt_counts, out_weight, norm_gain)
        return on_device(state_rows, q, k, v, halt_counts, out_weight, norm_gain)

    placed = (
        P(("dp", "ctx"), None),
        P(None, ("dp", "ctx"), None),
        P(None, ("dp", "ctx"), None),
        P(None, ("dp", "ctx"), None),
        P(("dp", "ctx")),
        P(),
        P(),
    )
    return jax.shard_map(
        per_device, mesh=mesh, in_specs=placed, out_specs=P(("dp", "ctx"), None), check_vma=False
    )
```

```python
import functools

import jax
import jax.numpy as jnp
from jax import lax
from jax.experimental import pallas as pl
from jax.experimental.pallas import tpu as pltpu
from jax.sharding import PartitionSpec as P

STEP = 2
TILE = 128
LEAD = 8
LOG2E = 1.4426950408889634


def head_orders(heads):
    half = heads // 2
    singles = [0, heads - 1, heads - 2]
    first = []
    for j in range(half - 1):
        first += [singles[j], j + 1]
    first.append(half)
    return first, [(h + half) % heads for h in first]


def star_kernel(
    halt_hbm,
    q_hbm,
    k_hbm,
    v_hbm,
    state_hbm,
    w_hbm,
    gain_hbm,
    first_ref,
    left_ref,
    update,
    w_last,
    state_buf,
    gain_buf,
    active_ref,
    halt,
    flag_out,
    flag_in,
    qkv_buf,
    tile_out,
    tile_in,
    far_part,
    stat_out,
    stat_in,
    own_part,
    own_stat,
    att_buf,
    w_buf,
    halt_sem,
    gain_sem,
    state_sem,
    w_sem,
    flag_send,
    flag_recv,
    tile_send,
    stat_send,
    qkv_sem,
    tile_recv,
    stat_recv,
):
    me = lax.axis_index("ctx")
    bits = (me % 2, me // 2)
    peer = (bits[1] * 2 + 1 - bits[0], (1 - bits[1]) * 2 + bits[0])
    heads, rows, width = q_hbm.shape
    features = state_hbm.shape[1]
    half = heads // 2
    steps = heads - 1
    inputs = heads - 2
    blocks = rows // TILE
    meeting = blocks
    scale = width ** (-0.5) * LOG2E
    axes = (0, 1)
    orders = head_orders(heads)
    f32, bf16 = jnp.float32, jnp.bfloat16

    def local(src, dst, sem):
        copy = pltpu.make_async_copy(src, dst, sem)
        copy.start()
        return copy

    def remote(src, dst, send, recv, axis):
        return pltpu.make_async_remote_copy(
            src_ref=src,
            dst_ref=dst,
            send_sem=send,
            recv_sem=recv,
            device_id={"ctx": peer[axis]},
            device_id_type=pl.DeviceIdType.MESH,
        )

    barrier = pltpu.get_barrier_semaphore()
    for axis in axes:
        pl.semaphore_signal(
            barrier, inc=1, device_id={"ctx": peer[axis]}, device_id_type=pl.DeviceIdType.MESH
        )
    halt_copy = local(halt_hbm, halt, halt_sem)

    def choices(b, axis):
        return (0, orders[axis][b]), (1 + b % 2, orders[1 - axis][2 * (b // 2) + 1])

    group_of = {}
    for b in range(blocks):
        for axis in axes:
            for block in choices(b, axis):
                group_of[block] = min(b, 1)
    for block in [(n, h) for h in range(heads) for n in range(3)]:
        group_of.setdefault(block, 2)
    for (n, h), group in group_of.items():
        local((q_hbm, k_hbm, v_hbm)[n].at[h], qkv_buf.at[n * heads + h], qkv_sem.at[group])
    loaded = set()

    def own(n, h):
        group = group_of[n, h]
        if group not in loaded:
            whole = qkv_buf.at[pl.ds(0, list(group_of.values()).count(group))]
            pltpu.make_async_copy(whole, whole, qkv_sem.at[group]).wait()
            loaded.add(group)
        return qkv_buf[n * heads + h]

    halt_copy.wait()
    flag = jnp.full(flag_out.shape, halt[0] > STEP).astype(f32)
    flag_out[...] = flag

    def mask(value):
        return jnp.broadcast_to(value[0:1, :].astype(bf16), (rows, width)) > 0.5

    is_owner = mask(flag)

    def cut_of(tiles):
        return slice(tiles[0] * TILE, (tiles[-1] + 1) * TILE)

    def input_tile(u, axis):
        b, cut = u // blocks, cut_of([u % blocks])
        if b < inputs:
            mine, other = choices(b, axis)
            return jnp.where(is_owner[cut], own(*mine)[cut], own(*other)[cut])
        return jnp.where(is_owner[cut], own(0, orders[axis][b])[cut], far_part[axis, :, cut])

    groups = [(u, min(blocks, LEAD - u)) for u in range(0, LEAD, blocks)]
    for p in range(steps):
        groups += [(LEAD + blocks * p, 1), (LEAD + blocks * p + 1, blocks - 1)]

    def send(n):
        start, count = groups[n]
        for axis in axes:
            remote(
                tile_out.at[axis, pl.ds(start, count)],
                tile_in.at[axis, pl.ds(start, count)],
                tile_send,
                tile_recv.at[n],
                axis,
            ).start()

    waited = []

    def wait_tiles(u):
        while sum(count for _, count in groups[: len(waited)]) <= u:
            n = len(waited)
            start, count = groups[n]
            landed = tile_in.at[pl.ds(0, 2), pl.ds(start, count)]
            remote(landed, landed, tile_send, tile_recv.at[n], 0).wait_recv()
            waited.append(n)

    known = []

    def wait_stats(p):
        while len(known) <= p:
            n = len(known)
            remote(stat_in.at[n], stat_in.at[n], stat_send, stat_recv.at[n], 0).wait_recv()
            known.append(n)

    for n, (start, count) in enumerate(groups[: len(range(0, LEAD, blocks))]):
        for axis in axes:
            for u in range(start, start + count):
                tile_out[axis, u] = input_tile(u, axis)
        if n == 0:
            pl.semaphore_wait(barrier, 2)
            for axis in axes:
                remote(flag_out, flag_in.at[axis], flag_send.at[axis], flag_recv, axis).start()
        send(n)

    for side in (0, 1):
        cut = pl.ds(side * width, width)
        local(w_hbm.at[pl.ds(side * half + 1, half - 1)], w_buf.at[:, cut], w_sem.at[0])
        local(w_hbm.at[side * half], w_last.at[cut], w_sem.at[1])
    state_copy = local(state_hbm, state_buf, state_sem)
    gain_copy = local(gain_hbm, gain_buf, gain_sem)

    remote(flag_in, flag_in, flag_send.at[0], flag_recv, 0).wait_recv()
    owner_at = [mask(flag_in[axis]) for axis in axes]
    beside = flag_in[0] + flag_in[1]
    is_beside = mask(beside)

    def bias(valid):
        return jnp.concatenate([(valid[0:1, :] - 1.0) * 1e30] * blocks, axis=1)

    def received(b, axis):
        return tile_in[axis, b * blocks : (b + 1) * blocks].reshape(rows, width)

    def attend(query, keys, values):
        scores = lax.dot_general(
            keys, query, (((1,), (1,)), ((), ())), preferred_element_type=f32
        )
        top = jnp.max(scores, axis=0, keepdims=True)
        weights = jnp.exp2((scores - top) * scale)
        total = jnp.sum(weights, axis=0, keepdims=True)
        weighted = lax.dot_general(
            values, weights.astype(bf16), (((0,), (0,)), ((), ())), preferred_element_type=f32
        )
        return top * scale + jnp.log2(total), weighted * (1.0 / total)

    def merge(sources):
        top = functools.reduce(jnp.maximum, [level for level, _ in sources])
        sums = [jnp.exp2(level - top) for level, _ in sources]
        total = functools.reduce(jnp.add, sums)
        inverse = 1.0 / total
        parts = [part * (each * inverse) for each, (_, part) in zip(sums, sources)]
        return top + jnp.log2(total), functools.reduce(jnp.add, parts)

    def put(p, level, part, query=None):
        part = part.astype(bf16)
        for axis in axes:
            stat_out[p, axis] = level[axis]
            for tile in range(blocks):
                u, cut = LEAD + blocks * p + tile, cut_of([tile])
                piece = part[:, cut]
                if query is not None:
                    piece = jnp.where(owner_at[1 - axis][cut], query[cut], piece)
                if u < steps * blocks:
                    piece = jnp.where(is_beside[cut], piece, input_tile(u, axis))
                tile_out[axis, u] = piece
            remote(
                stat_out.at[p, axis], stat_in.at[p, axis], stat_send, stat_recv.at[p], axis
            ).start()
        first = len(groups) - 2 * (steps - p)
        send(first)
        send(first + 1)

    def keep(h, result):
        own_stat[h], own_part[h] = result

    def kept(h, tiles=range(blocks)):
        cut = cut_of(tiles)
        return own_stat[h, :, cut], own_part[h, :, cut]

    def sent(p, axis, tiles=range(blocks), start=None):
        start = LEAD + blocks * p if start is None else start
        block = jnp.concatenate([tile_in[axis, start + tile] for tile in tiles], axis=1)
        return stat_in[p, axis, :, cut_of(tiles)], block.astype(f32)

    def select(value, first, second):
        line = jnp.concatenate([value[0:1, :]] * blocks, axis=1)
        return tuple(
            jnp.where(jnp.broadcast_to(line, a.shape) > 0.5, a, b) for a, b in zip(first, second)
        )

    def step(s):
        high, low = orders[0][s], orders[1][s]
        query = jnp.where(
            owner_at[0], received(s, 0), jnp.where(owner_at[1], received(s, 1), own(0, low))
        )
        key = jnp.where(owner_at[0], own(1, high), own(1, low))
        value = jnp.where(owner_at[0], own(2, high), own(2, low))
        if s % 2 == 0:
            result = attend(query, key, value)
            keep(low, result)
            if s == inputs:
                start, p = s * blocks, meeting
                far = select(
                    flag_in[0], sent(p, 1, start=start), sent(p, 0, start=start)
                )
                result = merge((result, far))
            put(s, [result[0]] * 2, result[1], query if s == 0 else None)
            return
        far_key = jnp.where(owner_at[0], received(s - 1, 1), received(s - 1, 0))
        far_value = jnp.where(owner_at[0], received(s, 1), received(s, 0))
        far_query = query
        valid = beside + flag if s == 1 else beside
        if s == meeting:
            one, two = (
                jnp.concatenate([tile_in[axis, LEAD + tile] for tile in range(blocks)], axis=0)
                for axis in axes
            )
            take = mask(flag + beside)
            query = jnp.where(take, query, two)
            key = jnp.where(take, key, own(1, orders[0][0]))
            value = jnp.where(take, value, own(2, orders[0][0]))
            far_query = jnp.where(take, far_query, one)
            far_key = jnp.where(take, far_key, own(1, orders[1][0]))
            far_value = jnp.where(take, far_value, own(2, orders[1][0]))
        nearby = attend(query, key, value)
        distant = attend(far_query, far_key, far_value)
        result = merge((nearby, (distant[0] + bias(valid), distant[1])))
        keep(low, result)
        level = [result[0]] * 2
        if s == meeting:
            for axis, each in enumerate((nearby, distant)):
                far_part[axis] = each[1].astype(bf16)
                level[axis] = select(beside, result[:1], each[:1])[0]
        put(s, level, result[1])
        if s == 1:
            nearby = attend(own(0, high), own(1, high), own(2, high))
            distant = attend(own(0, high), received(s - 1, 1), received(s, 1))
            keep(high, merge((nearby, distant)))

    def combine(i, tiles=range(blocks)):
        for side in (0, 1):
            h = i + side * half
            sources = [kept(h, tiles)]
            for axis in axes:
                if h in orders[axis]:
                    sources.append(sent(orders[axis].index(h), axis, tiles))
            attended = merge(sources)[1]
            att_buf[i, cut_of(tiles), side * width : (side + 1) * width] = attended.T.astype(bf16)

    chunk = min(4 * TILE, features)

    def project(i, initial):
        left = att_buf[i]

        def body(n, carry):
            cut = pl.ds(pl.multiple_of(n * chunk, chunk), chunk)
            product = jnp.dot(left, w_buf[i - 1, :, cut], preferred_element_type=f32)
            if initial:
                update[:, cut] = state_buf[:, cut].astype(f32) + product
            else:
                update[:, cut] = update[:, cut] + product
            return carry

        lax.fori_loop(0, features // chunk, body, 0)

    def result_tile(p, tile):
        return LEAD + blocks * p + tile

    for s in range(steps):
        wait_tiles((s + 1) * blocks - 1)
        if s == inputs:
            wait_stats(meeting)
        step(s)
        if s == half:
            pltpu.make_async_copy(w_buf, w_buf, w_sem.at[0]).wait()
            pltpu.make_async_copy(w_last, w_last, w_sem.at[1]).wait()
            state_copy.wait()
            gain_copy.wait()
            wait_stats(1)
            combine(1)
            project(1, True)
    for i in range(2, half - 1):
        p = max(order.index(i) for order in orders)
        wait_tiles(result_tile(p, blocks - 1))
        wait_stats(p)
        combine(i)
        project(i, False)

    i, p, rest = half - 1, steps - 2, list(range(1, blocks))
    for tiles in ([0], rest):
        wait_tiles(result_tile(p, tiles[-1]))
        wait_stats(p)
        combine(i, tiles)
        cut = cut_of(tiles)
        add_product(att_buf[i, cut, :], w_buf.at[i - 1], update.at[cut], update.at[cut])
        for tile in tiles:
            active = jnp.full(active_ref.shape[1:], halt[tile * TILE] > STEP)
            active_ref[tile] = active.astype(f32)

    p = steps - 1
    wait_stats(p)
    wait_tiles(result_tile(p, 0))
    combine(0, [0])
    cut = cut_of([0])
    squares = add_product(att_buf[0, cut, :], w_last, update.at[cut], update.at[cut])
    normalize(squares, update.at[cut], gain_buf, active_ref[0], state_buf.at[cut], first_ref)
    wait_tiles(result_tile(p, blocks - 1))
    combine(0, rest)
    left_ref[...] = att_buf[0, cut_of(rest), :]

    remote(tile_out, tile_in, tile_send, tile_recv.at[0], 0).wait_send()
    remote(stat_out, stat_in, stat_send, stat_recv.at[0], 0).wait_send()
    for axis in axes:
        remote(flag_out, flag_in.at[axis], flag_send.at[axis], flag_recv, axis).wait_send()


def strips_of(ref):
    return [slice(n, n + 4 * TILE) for n in range(0, ref.shape[1], 4 * TILE)]


def add_product(left, weight, base, mixed):
    squares = jnp.zeros((left.shape[0], TILE), jnp.float32)
    for strip in strips_of(base):
        product = jnp.dot(left, weight[:, strip], preferred_element_type=jnp.float32)
        total = base[:, strip] + product
        mixed[:, strip] = total
        for n in range(0, total.shape[1], TILE):
            squares = squares + total[:, n : n + TILE] * total[:, n : n + TILE]
    return squares


def normalize(squares, mixed, gain_ref, active, state, out):
    mean = jnp.sum(squares, axis=-1, keepdims=True) / mixed.shape[1]
    inverse = lax.rsqrt(mean + 1e-06)
    chosen = jnp.broadcast_to(active[0:1, :].astype(jnp.bfloat16), (TILE, TILE))
    chosen = jnp.concatenate([chosen] * 4, axis=1) > 0.5
    for strip in strips_of(mixed):
        gain = gain_ref[strip].astype(jnp.float32).reshape(1, -1)
        normed = (mixed[:, strip] * inverse * gain).astype(jnp.bfloat16)
        out[:, strip] = jnp.where(chosen, normed, state[:, strip])


def finish_kernel(
    first_ref, left_ref, update, w_last, state_ref, gain_ref, active_ref, out_hbm, mixed, done, sem
):
    def store(source, tile):
        copy = pltpu.make_async_copy(source, out_hbm.at[pl.ds(tile * TILE, TILE)], sem.at[tile])
        copy.start()
        return copy

    tiles = range(1, 1 + mixed.shape[0] // TILE)
    first = store(first_ref, 0)
    some_active = jnp.max(active_ref[pl.ds(1, len(tiles))]) > 0.5

    @pl.when(some_active)
    def _():
        squares = add_product(left_ref[...], w_last, update.at[pl.ds(TILE, mixed.shape[0])], mixed)
        copies = []
        for tile in tiles:
            cut = pl.ds((tile - 1) * TILE, TILE)
            normalize(
                squares[(tile - 1) * TILE : tile * TILE],
                mixed.at[cut],
                gain_ref,
                active_ref[tile],
                state_ref.at[pl.ds(tile * TILE, TILE)],
                done.at[cut],
            )
            copies.append(store(done.at[cut], tile))
        for copy in copies:
            copy.wait()

    @pl.when(jnp.logical_not(some_active))
    def _():
        copies = [store(state_ref.at[pl.ds(tile * TILE, TILE)], tile) for tile in tiles]
        for copy in copies:
            copy.wait()

    first.wait()


def on_star(state_rows, q, k, v, halt_counts, out_weight, norm_gain):
    heads, rows, width = q.shape
    features = state_rows.shape[1]
    half, blocks, steps = heads // 2, rows // TILE, heads - 1
    tiles = LEAD + steps * blocks
    groups = pl.cdiv(LEAD, blocks) + 2 * steps
    bf16, f32 = jnp.bfloat16, jnp.float32
    hbm = pl.BlockSpec(memory_space=pltpu.MemorySpace.HBM)
    vmem = pl.BlockSpec(memory_space=pltpu.VMEM)
    dma = pltpu.SemaphoreType.DMA
    operands = (halt_counts, q, k, v, state_rows, out_weight, norm_gain)
    handed = (
        ((TILE, features), bf16),
        ((rows - TILE, 2 * width), bf16),
        ((rows, features), f32),
        ((2 * width, features), bf16),
        ((rows, features), bf16),
        ((features,), bf16),
        ((blocks, 8, TILE), f32),
    )
    results = pl.pallas_call(
        star_kernel,
        out_shape=[jax.ShapeDtypeStruct(*each) for each in handed],
        in_specs=[hbm] * len(operands),
        out_specs=[vmem] * len(handed),
        scratch_shapes=[
            pltpu.SMEM((rows,), jnp.int32),
            pltpu.VMEM((8, width), f32),
            pltpu.VMEM((2, 8, width), f32),
            pltpu.VMEM((3 * heads, rows, width), bf16),
            pltpu.VMEM((2, tiles, TILE, width), bf16),
            pltpu.VMEM((2, tiles, TILE, width), bf16),
            pltpu.VMEM((2, width, rows), bf16),
            pltpu.VMEM((steps, 2, 1, rows), f32),
            pltpu.VMEM((steps, 2, 1, rows), f32),
            pltpu.VMEM((heads, width, rows), f32),
            pltpu.VMEM((heads, 1, rows), f32),
            pltpu.VMEM((half, rows, 2 * width), bf16),
            pltpu.VMEM((half - 1, 2 * width, features), bf16),
            dma,
            dma,
            dma,
            dma((2,)),
            dma((2,)),
            dma,
            dma,
            dma,
            dma((3,)),
            dma((groups,)),
            dma((steps,)),
        ],
        compiler_params=pltpu.CompilerParams(
            collective_id=0, has_side_effects=True, vmem_limit_bytes=32 * 1024 * 1024
        ),
    )(*[pltpu.with_memory_space_constraint(x, pltpu.HBM) for x in operands])
    return pl.pallas_call(
        finish_kernel,
        out_shape=jax.ShapeDtypeStruct((rows, features), bf16),
        in_specs=[vmem] * len(handed),
        out_specs=hbm,
        scratch_shapes=[
            pltpu.VMEM((rows - TILE, features), f32),
            pltpu.VMEM((rows - TILE, features), bf16),
            dma((blocks,)),
        ],
        compiler_params=pltpu.CompilerParams(vmem_limit_bytes=8 * 1024 * 1024),
    )(*results)


def fold_heads(carry, queries, key_piece, value_piece, score_scale):
    running_max, running_sum, weighted = carry

    def per_head(head_items):
        query_head, key_head, value_head, max_head, sum_head, weighted_head = head_items
        scores = (
            lax.dot_general(
                query_head, key_head, (((1,), (1,)), ((), ())), preferred_element_type=jnp.float32
            )
            * score_scale
        )
        new_max = jnp.maximum(max_head, jnp.max(scores, axis=1))
        shrink = jnp.exp(max_head - new_max)
        exponents = jnp.exp(scores - new_max[:, None])
        sum_head = sum_head * shrink + jnp.sum(exponents, axis=1)
        weighted_head = weighted_head * shrink[:, None] + jnp.dot(
            exponents.astype(jnp.bfloat16), value_head, preferred_element_type=jnp.float32
        )
        return (new_max, sum_head, weighted_head)

    return lax.map(per_head, (queries, key_piece, value_piece, running_max, running_sum, weighted))


def empty_carry(head_count, query_count, head_width):
    return (
        jnp.full((head_count, query_count), -1e30, jnp.float32),
        jnp.zeros((head_count, query_count), jnp.float32),
        jnp.zeros((head_count, query_count, head_width), jnp.float32),
    )


def attend_keys(query_vectors, key_vectors, value_vectors, score_scale):
    head_count, row_count, head_width = query_vectors.shape
    initial = empty_carry(head_count, row_count, head_width)
    running_max, running_sum, weighted = fold_heads(
        initial,
        query_vectors,
        lax.all_gather(key_vectors, "ctx", axis=1, tiled=True),
        lax.all_gather(value_vectors, "ctx", axis=1, tiled=True),
        score_scale,
    )
    return (weighted / running_sum[..., None]).astype(jnp.bfloat16)


def on_device(
    state_rows, query_vectors, key_vectors, value_vectors, halt_counts, out_weight, norm_gain
):
    head_count, row_count, head_width = query_vectors.shape
    score_scale = head_width ** (-0.5)
    attended = attend_keys(query_vectors, key_vectors, value_vectors, score_scale)
    update = jnp.einsum("hqd,hde->qe", attended, out_weight, preferred_element_type=jnp.float32)
    mixed_sum = state_rows.astype(jnp.float32) + update
    normed = (
        mixed_sum
        * lax.rsqrt(jnp.mean(mixed_sum * mixed_sum, axis=-1, keepdims=True) + 1e-06)
        * norm_gain.astype(jnp.float32)
    )
    active = (halt_counts > STEP)[:, None]
    return jnp.where(active, normed.astype(jnp.bfloat16), state_rows)


def solution(mesh):
    n_ctx = mesh.shape["ctx"]

    def per_device(state_rows, q, k, v, halt_counts, out_weight, norm_gain):
        heads, rows, width = q.shape
        one_owner = rows == (n_ctx - 1) * TILE
        if one_owner and heads == LEAD and width == TILE and n_ctx == 4:
            return on_star(state_rows, q, k, v, halt_counts, out_weight, norm_gain)
        return on_device(state_rows, q, k, v, halt_counts, out_weight, norm_gain)

    placed = (
        P(("dp", "ctx"), None),
        P(None, ("dp", "ctx"), None),
        P(None, ("dp", "ctx"), None),
        P(None, ("dp", "ctx"), None),
        P(("dp", "ctx")),
        P(),
        P(),
    )
    return jax.shard_map(
        per_device, mesh=mesh, in_specs=placed, out_specs=P(("dp", "ctx"), None), check_vma=False
    )
```

```python
import functools

import jax
import jax.numpy as jnp
from jax import lax
from jax.experimental import pallas as pl
from jax.experimental.pallas import tpu as pltpu
from jax.sharding import PartitionSpec as P

STEP = 2
TILE = 128
LEAD = 8
STATS = 4
LOG2E = 1.4426950408889634


def head_orders(heads):
    half = heads // 2
    singles = [0, heads - 1, heads - 2]
    first = []
    for j in range(half - 1):
        first += [singles[j], j + 1]
    first.append(half)
    return first, [(h + half) % heads for h in first]


def tile_groups(steps, blocks):
    groups = [(u, min(blocks, LEAD - u)) for u in range(0, LEAD, blocks)]
    opening = len(groups)
    for p in range(steps):
        groups += [(LEAD + blocks * p, 1), (LEAD + blocks * p + 1, blocks - 1)]
    sems, last = [], {}
    for n in range(len(groups)):
        done = blocks * ((n - opening) // 2 - 1) - 1 if n >= opening else -1
        free = [sem for sem, end in last.items() if end <= done]
        sem = free[0] if free else len(last)
        sems.append(sem)
        last[sem] = sum(groups[n]) - 1
    return groups, sems


def star_kernel(
    halt_hbm,
    q_hbm,
    k_hbm,
    v_hbm,
    state_hbm,
    w_hbm,
    gain_hbm,
    first_ref,
    left_ref,
    update,
    w_last,
    state_buf,
    gain_buf,
    active_ref,
    halt,
    flag_out,
    flag_in,
    qkv_buf,
    tile_out,
    tile_in,
    far_part,
    stat_out,
    stat_in,
    own_part,
    own_stat,
    att_buf,
    w_buf,
    halt_sem,
    gain_sem,
    state_sem,
    w_sem,
    flag_send,
    flag_recv,
    tile_send,
    stat_send,
    qkv_sem,
    tile_recv,
    stat_recv,
):
    me = lax.axis_index("ctx")
    bits = (me % 2, me // 2)
    peer = (bits[1] * 2 + 1 - bits[0], (1 - bits[1]) * 2 + bits[0])
    heads, rows, width = q_hbm.shape
    features = state_hbm.shape[1]
    half = heads // 2
    steps = heads - 1
    inputs = heads - 2
    blocks = rows // TILE
    meeting = blocks
    scale = width ** (-0.5) * LOG2E
    axes = (0, 1)
    orders = head_orders(heads)
    f32, bf16 = jnp.float32, jnp.bfloat16

    def local(src, dst, sem):
        copy = pltpu.make_async_copy(src, dst, sem)
        copy.start()
        return copy

    def remote(src, dst, send, recv, axis):
        return pltpu.make_async_remote_copy(
            src_ref=src,
            dst_ref=dst,
            send_sem=send,
            recv_sem=recv,
            device_id={"ctx": peer[axis]},
            device_id_type=pl.DeviceIdType.MESH,
        )

    barrier = pltpu.get_barrier_semaphore()
    for axis in axes:
        pl.semaphore_signal(
            barrier, inc=1, device_id={"ctx": peer[axis]}, device_id_type=pl.DeviceIdType.MESH
        )
    halt_copy = local(halt_hbm, halt, halt_sem)

    def choices(b, axis):
        return (0, orders[axis][b]), (1 + b % 2, orders[1 - axis][2 * (b // 2) + 1])

    group_of = {}
    for b in range(blocks):
        for axis in axes:
            for block in choices(b, axis):
                group_of[block] = min(b, 1)
    for block in [(n, h) for h in range(heads) for n in range(3)]:
        group_of.setdefault(block, 2)
    for (n, h), group in group_of.items():
        local((q_hbm, k_hbm, v_hbm)[n].at[h], qkv_buf.at[n * heads + h], qkv_sem.at[group])
    loaded = set()

    def own(n, h):
        group = group_of[n, h]
        if group not in loaded:
            whole = qkv_buf.at[pl.ds(0, list(group_of.values()).count(group))]
            pltpu.make_async_copy(whole, whole, qkv_sem.at[group]).wait()
            loaded.add(group)
        return qkv_buf[n * heads + h]

    halt_copy.wait()
    flag = jnp.full(flag_out.shape, halt[0] > STEP).astype(f32)
    flag_out[...] = flag

    def mask(value):
        return jnp.broadcast_to(value[0:1, :].astype(bf16), (rows, width)) > 0.5

    is_owner = mask(flag)

    def cut_of(tiles):
        return slice(tiles[0] * TILE, (tiles[-1] + 1) * TILE)

    def input_tile(u, axis):
        b, cut = u // blocks, cut_of([u % blocks])
        if b < inputs:
            mine, other = choices(b, axis)
            return jnp.where(is_owner[cut], own(*mine)[cut], own(*other)[cut])
        return jnp.where(is_owner[cut], own(0, orders[axis][b])[cut], far_part[axis, :, cut])

    groups, group_sems = tile_groups(steps, blocks)

    def send(n):
        start, count = groups[n]
        for axis in axes:
            remote(
                tile_out.at[axis, pl.ds(start, count)],
                tile_in.at[axis, pl.ds(start, count)],
                tile_send,
                tile_recv.at[group_sems[n]],
                axis,
            ).start()

    waited = []

    def wait_tiles(u):
        while sum(count for _, count in groups[: len(waited)]) <= u:
            n = len(waited)
            start, count = groups[n]
            landed = tile_in.at[pl.ds(0, 2), pl.ds(start, count)]
            remote(landed, landed, tile_send, tile_recv.at[group_sems[n]], 0).wait_recv()
            waited.append(n)

    known = []

    def wait_stats(p):
        while len(known) <= p:
            n = len(known)
            remote(
                stat_in.at[n], stat_in.at[n], stat_send, stat_recv.at[n % STATS], 0
            ).wait_recv()
            known.append(n)

    for n, (start, count) in enumerate(groups[: len(range(0, LEAD, blocks))]):
        for axis in axes:
            for u in range(start, start + count):
                tile_out[axis, u] = input_tile(u, axis)
        if n == 0:
            pl.semaphore_wait(barrier, 2)
            for axis in axes:
                remote(flag_out, flag_in.at[axis], flag_send, flag_recv, axis).start()
        send(n)

    for side in (0, 1):
        cut = pl.ds(side * width, width)
        local(w_hbm.at[pl.ds(side * half + 1, half - 1)], w_buf.at[:, cut], w_sem.at[0])
        local(w_hbm.at[side * half], w_last.at[cut], w_sem.at[1])
    state_copy = local(state_hbm, state_buf, state_sem)
    gain_copy = local(gain_hbm, gain_buf, gain_sem)

    remote(flag_in, flag_in, flag_send, flag_recv, 0).wait_recv()
    owner_at = [mask(flag_in[axis]) for axis in axes]
    beside = flag_in[0] + flag_in[1]
    is_beside = mask(beside)

    def bias(valid):
        return jnp.concatenate([(valid[0:1, :] - 1.0) * 1e30] * blocks, axis=1)

    def received(b, axis):
        return tile_in[axis, b * blocks : (b + 1) * blocks].reshape(rows, width)

    def attend(query, keys, values):
        scores = lax.dot_general(
            keys, query, (((1,), (1,)), ((), ())), preferred_element_type=f32
        )
        top = jnp.max(scores, axis=0, keepdims=True)
        weights = jnp.exp2((scores - top) * scale)
        total = jnp.sum(weights, axis=0, keepdims=True)
        weighted = lax.dot_general(
            values, weights.astype(bf16), (((0,), (0,)), ((), ())), preferred_element_type=f32
        )
        return top * scale + jnp.log2(total), weighted * (1.0 / total)

    def merge(sources):
        top = functools.reduce(jnp.maximum, [level for level, _ in sources])
        sums = [jnp.exp2(level - top) for level, _ in sources]
        total = functools.reduce(jnp.add, sums)
        inverse = 1.0 / total
        parts = [part * (each * inverse) for each, (_, part) in zip(sums, sources)]
        return top + jnp.log2(total), functools.reduce(jnp.add, parts)

    def put(p, level, part, query=None):
        part = part.astype(bf16)
        for axis in axes:
            stat_out[p, axis] = level[axis]
            for tile in range(blocks):
                u, cut = LEAD + blocks * p + tile, cut_of([tile])
                piece = part[:, cut]
                if query is not None:
                    piece = jnp.where(owner_at[1 - axis][cut], query[cut], piece)
                if u < steps * blocks:
                    piece = jnp.where(is_beside[cut], piece, input_tile(u, axis))
                tile_out[axis, u] = piece
            remote(
                stat_out.at[p, axis],
                stat_in.at[p, axis],
                stat_send,
                stat_recv.at[p % STATS],
                axis,
            ).start()
        first = len(groups) - 2 * (steps - p)
        send(first)
        send(first + 1)

    def keep(h, result):
        own_stat[h], own_part[h] = result

    def kept(h, tiles=range(blocks)):
        cut = cut_of(tiles)
        return own_stat[h, :, cut], own_part[h, :, cut]

    def sent(p, axis, tiles=range(blocks), start=None):
        start = LEAD + blocks * p if start is None else start
        block = jnp.concatenate([tile_in[axis, start + tile] for tile in tiles], axis=1)
        return stat_in[p, axis, :, cut_of(tiles)], block.astype(f32)

    def select(value, first, second):
        line = jnp.concatenate([value[0:1, :]] * blocks, axis=1)
        return tuple(
            jnp.where(jnp.broadcast_to(line, a.shape) > 0.5, a, b) for a, b in zip(first, second)
        )

    def step(s):
        high, low = orders[0][s], orders[1][s]
        query = jnp.where(
            owner_at[0], received(s, 0), jnp.where(owner_at[1], received(s, 1), own(0, low))
        )
        key = jnp.where(owner_at[0], own(1, high), own(1, low))
        value = jnp.where(owner_at[0], own(2, high), own(2, low))
        if s % 2 == 0:
            result = attend(query, key, value)
            keep(low, result)
            if s == inputs:
                start, p = s * blocks, meeting
                far = select(
                    flag_in[0], sent(p, 1, start=start), sent(p, 0, start=start)
                )
                result = merge((result, far))
            put(s, [result[0]] * 2, result[1], query if s == 0 else None)
            return
        far_key = jnp.where(owner_at[0], received(s - 1, 1), received(s - 1, 0))
        far_value = jnp.where(owner_at[0], received(s, 1), received(s, 0))
        far_query = query
        valid = beside + flag if s == 1 else beside
        if s == meeting:
            one, two = (
                jnp.concatenate([tile_in[axis, LEAD + tile] for tile in range(blocks)], axis=0)
                for axis in axes
            )
            take = mask(flag + beside)
            query = jnp.where(take, query, two)
            key = jnp.where(take, key, own(1, orders[0][0]))
            value = jnp.where(take, value, own(2, orders[0][0]))
            far_query = jnp.where(take, far_query, one)
            far_key = jnp.where(take, far_key, own(1, orders[1][0]))
            far_value = jnp.where(take, far_value, own(2, orders[1][0]))
        nearby = attend(query, key, value)
        distant = attend(far_query, far_key, far_value)
        result = merge((nearby, (distant[0] + bias(valid), distant[1])))
        keep(low, result)
        level = [result[0]] * 2
        if s == meeting:
            for axis, each in enumerate((nearby, distant)):
                far_part[axis] = each[1].astype(bf16)
                level[axis] = select(beside, result[:1], each[:1])[0]
        put(s, level, result[1])
        if s == 1:
            nearby = attend(own(0, high), own(1, high), own(2, high))
            distant = attend(own(0, high), received(s - 1, 1), received(s, 1))
            keep(high, merge((nearby, distant)))

    def combine(i, tiles=range(blocks)):
        for side in (0, 1):
            h = i + side * half
            sources = [kept(h, tiles)]
            for axis in axes:
                if h in orders[axis]:
                    sources.append(sent(orders[axis].index(h), axis, tiles))
            attended = merge(sources)[1]
            att_buf[i, cut_of(tiles), side * width : (side + 1) * width] = attended.T.astype(bf16)

    chunk = min(4 * TILE, features)

    def project(i, initial):
        left = att_buf[i]

        def body(n, carry):
            cut = pl.ds(pl.multiple_of(n * chunk, chunk), chunk)
            product = jnp.dot(left, w_buf[i - 1, :, cut], preferred_element_type=f32)
            if initial:
                update[:, cut] = state_buf[:, cut].astype(f32) + product
            else:
                update[:, cut] = update[:, cut] + product
            return carry

        lax.fori_loop(0, features // chunk, body, 0)

    def result_tile(p, tile):
        return LEAD + blocks * p + tile

    for s in range(steps):
        wait_tiles((s + 1) * blocks - 1)
        wait_stats(meeting if s == inputs else s - 2)
        step(s)
        if s == half:
            pltpu.make_async_copy(w_buf, w_buf, w_sem.at[0]).wait()
            pltpu.make_async_copy(w_last, w_last, w_sem.at[1]).wait()
            state_copy.wait()
            gain_copy.wait()
            wait_stats(1)
            combine(1)
            project(1, True)
    for i in range(2, half - 1):
        p = max(order.index(i) for order in orders)
        wait_tiles(result_tile(p, blocks - 1))
        wait_stats(p)
        combine(i)
        project(i, False)

    i, p, rest = half - 1, steps - 2, list(range(1, blocks))
    for tiles in ([0], rest):
        wait_tiles(result_tile(p, tiles[-1]))
        wait_stats(p)
        combine(i, tiles)
        cut = cut_of(tiles)
        add_product(att_buf[i, cut, :], w_buf.at[i - 1], update.at[cut], update.at[cut])
        for tile in tiles:
            active = jnp.full(active_ref.shape[1:], halt[tile * TILE] > STEP)
            active_ref[tile] = active.astype(f32)

    p = steps - 1
    wait_stats(p)
    wait_tiles(result_tile(p, 0))
    combine(0, [0])
    cut = cut_of([0])
    squares = add_product(att_buf[0, cut, :], w_last, update.at[cut], update.at[cut])
    normalize(squares, update.at[cut], gain_buf, active_ref[0], state_buf.at[cut], first_ref)
    wait_tiles(result_tile(p, blocks - 1))
    combine(0, rest)
    left_ref[...] = att_buf[0, cut_of(rest), :]

    remote(tile_out, tile_in, tile_send, tile_recv.at[0], 0).wait_send()
    remote(stat_out, stat_in, stat_send, stat_recv.at[0], 0).wait_send()
    remote(flag_in, flag_in, flag_send, flag_recv, 0).wait_send()


def strips_of(ref):
    return [slice(n, n + 4 * TILE) for n in range(0, ref.shape[1], 4 * TILE)]


def add_product(left, weight, base, mixed):
    squares = jnp.zeros((left.shape[0], TILE), jnp.float32)
    for strip in strips_of(base):
        product = jnp.dot(left, weight[:, strip], preferred_element_type=jnp.float32)
        total = base[:, strip] + product
        mixed[:, strip] = total
        for n in range(0, total.shape[1], TILE):
            squares = squares + total[:, n : n + TILE] * total[:, n : n + TILE]
    return squares


def normalize(squares, mixed, gain_ref, active, state, out):
    mean = jnp.sum(squares, axis=-1, keepdims=True) / mixed.shape[1]
    inverse = lax.rsqrt(mean + 1e-06)
    chosen = jnp.broadcast_to(active[0:1, :].astype(jnp.bfloat16), (TILE, TILE))
    chosen = jnp.concatenate([chosen] * 4, axis=1) > 0.5
    for strip in strips_of(mixed):
        gain = gain_ref[strip].astype(jnp.float32).reshape(1, -1)
        normed = (mixed[:, strip] * inverse * gain).astype(jnp.bfloat16)
        out[:, strip] = jnp.where(chosen, normed, state[:, strip])


def finish_kernel(
    first_ref, left_ref, update, w_last, state_ref, gain_ref, active_ref, out_hbm, mixed, done, sem
):
    def store(source, tile):
        copy = pltpu.make_async_copy(source, out_hbm.at[pl.ds(tile * TILE, TILE)], sem.at[tile])
        copy.start()
        return copy

    tiles = range(1, 1 + mixed.shape[0] // TILE)
    first = store(first_ref, 0)
    some_active = jnp.max(active_ref[pl.ds(1, len(tiles))]) > 0.5

    @pl.when(some_active)
    def _():
        squares = add_product(left_ref[...], w_last, update.at[pl.ds(TILE, mixed.shape[0])], mixed)
        copies = []
        for tile in tiles:
            cut = pl.ds((tile - 1) * TILE, TILE)
            normalize(
                squares[(tile - 1) * TILE : tile * TILE],
                mixed.at[cut],
                gain_ref,
                active_ref[tile],
                state_ref.at[pl.ds(tile * TILE, TILE)],
                done.at[cut],
            )
            copies.append(store(done.at[cut], tile))
        for copy in copies:
            copy.wait()

    @pl.when(jnp.logical_not(some_active))
    def _():
        copies = [store(state_ref.at[pl.ds(tile * TILE, TILE)], tile) for tile in tiles]
        for copy in copies:
            copy.wait()

    first.wait()


def on_star(state_rows, q, k, v, halt_counts, out_weight, norm_gain):
    heads, rows, width = q.shape
    features = state_rows.shape[1]
    half, blocks, steps = heads // 2, rows // TILE, heads - 1
    tiles = LEAD + steps * blocks
    landings = 1 + max(tile_groups(steps, blocks)[1])
    bf16, f32 = jnp.bfloat16, jnp.float32
    hbm = pl.BlockSpec(memory_space=pltpu.MemorySpace.HBM)
    vmem = pl.BlockSpec(memory_space=pltpu.VMEM)
    dma = pltpu.SemaphoreType.DMA
    operands = (halt_counts, q, k, v, state_rows, out_weight, norm_gain)
    handed = (
        ((TILE, features), bf16),
        ((rows - TILE, 2 * width), bf16),
        ((rows, features), f32),
        ((2 * width, features), bf16),
        ((rows, features), bf16),
        ((features,), bf16),
        ((blocks, 8, TILE), f32),
    )
    results = pl.pallas_call(
        star_kernel,
        out_shape=[jax.ShapeDtypeStruct(*each) for each in handed],
        in_specs=[hbm] * len(operands),
        out_specs=[vmem] * len(handed),
        scratch_shapes=[
            pltpu.SMEM((rows,), jnp.int32),
            pltpu.VMEM((8, width), f32),
            pltpu.VMEM((2, 8, width), f32),
            pltpu.VMEM((3 * heads, rows, width), bf16),
            pltpu.VMEM((2, tiles, TILE, width), bf16),
            pltpu.VMEM((2, tiles, TILE, width), bf16),
            pltpu.VMEM((2, width, rows), bf16),
            pltpu.VMEM((steps, 2, 1, rows), f32),
            pltpu.VMEM((steps, 2, 1, rows), f32),
            pltpu.VMEM((heads, width, rows), f32),
            pltpu.VMEM((heads, 1, rows), f32),
            pltpu.VMEM((half, rows, 2 * width), bf16),
            pltpu.VMEM((half - 1, 2 * width, features), bf16),
            dma,
            dma,
            dma,
            dma((2,)),
            dma,
            dma,
            dma,
            dma,
            dma((3,)),
            dma((landings,)),
            dma((STATS,)),
        ],
        compiler_params=pltpu.CompilerParams(
            collective_id=0, has_side_effects=True, vmem_limit_bytes=32 * 1024 * 1024
        ),
    )(*[pltpu.with_memory_space_constraint(x, pltpu.HBM) for x in operands])
    return pl.pallas_call(
        finish_kernel,
        out_shape=jax.ShapeDtypeStruct((rows, features), bf16),
        in_specs=[vmem] * len(handed),
        out_specs=hbm,
        scratch_shapes=[
            pltpu.VMEM((rows - TILE, features), f32),
            pltpu.VMEM((rows - TILE, features), bf16),
            dma((blocks,)),
        ],
        compiler_params=pltpu.CompilerParams(vmem_limit_bytes=8 * 1024 * 1024),
    )(*results)


def fold_heads(carry, queries, key_piece, value_piece, score_scale):
    running_max, running_sum, weighted = carry

    def per_head(head_items):
        query_head, key_head, value_head, max_head, sum_head, weighted_head = head_items
        scores = (
            lax.dot_general(
                query_head, key_head, (((1,), (1,)), ((), ())), preferred_element_type=jnp.float32
            )
            * score_scale
        )
        new_max = jnp.maximum(max_head, jnp.max(scores, axis=1))
        shrink = jnp.exp(max_head - new_max)
        exponents = jnp.exp(scores - new_max[:, None])
        sum_head = sum_head * shrink + jnp.sum(exponents, axis=1)
        weighted_head = weighted_head * shrink[:, None] + jnp.dot(
            exponents.astype(jnp.bfloat16), value_head, preferred_element_type=jnp.float32
        )
        return (new_max, sum_head, weighted_head)

    return lax.map(per_head, (queries, key_piece, value_piece, running_max, running_sum, weighted))


def empty_carry(head_count, query_count, head_width):
    return (
        jnp.full((head_count, query_count), -1e30, jnp.float32),
        jnp.zeros((head_count, query_count), jnp.float32),
        jnp.zeros((head_count, query_count, head_width), jnp.float32),
    )


def attend_keys(query_vectors, key_vectors, value_vectors, score_scale):
    head_count, row_count, head_width = query_vectors.shape
    initial = empty_carry(head_count, row_count, head_width)
    running_max, running_sum, weighted = fold_heads(
        initial,
        query_vectors,
        lax.all_gather(key_vectors, "ctx", axis=1, tiled=True),
        lax.all_gather(value_vectors, "ctx", axis=1, tiled=True),
        score_scale,
    )
    return (weighted / running_sum[..., None]).astype(jnp.bfloat16)


def on_device(
    state_rows, query_vectors, key_vectors, value_vectors, halt_counts, out_weight, norm_gain
):
    head_count, row_count, head_width = query_vectors.shape
    score_scale = head_width ** (-0.5)
    attended = attend_keys(query_vectors, key_vectors, value_vectors, score_scale)
    update = jnp.einsum("hqd,hde->qe", attended, out_weight, preferred_element_type=jnp.float32)
    mixed_sum = state_rows.astype(jnp.float32) + update
    normed = (
        mixed_sum
        * lax.rsqrt(jnp.mean(mixed_sum * mixed_sum, axis=-1, keepdims=True) + 1e-06)
        * norm_gain.astype(jnp.float32)
    )
    active = (halt_counts > STEP)[:, None]
    return jnp.where(active, normed.astype(jnp.bfloat16), state_rows)


def solution(mesh):
    n_ctx = mesh.shape["ctx"]

    def per_device(state_rows, q, k, v, halt_counts, out_weight, norm_gain):
        heads, rows, width = q.shape
        one_owner = rows == (n_ctx - 1) * TILE
        if one_owner and heads == LEAD and width == TILE and n_ctx == 4:
            return on_star(state_rows, q, k, v, halt_counts, out_weight, norm_gain)
        return on_device(state_rows, q, k, v, halt_counts, out_weight, norm_gain)

    placed = (
        P(("dp", "ctx"), None),
        P(None, ("dp", "ctx"), None),
        P(None, ("dp", "ctx"), None),
        P(None, ("dp", "ctx"), None),
        P(("dp", "ctx")),
        P(),
        P(),
    )
    return jax.shard_map(
        per_device, mesh=mesh, in_specs=placed, out_specs=P(("dp", "ctx"), None), check_vma=False
    )
```

```python
import functools

import jax
import jax.numpy as jnp
from jax import lax
from jax.experimental import pallas as pl
from jax.experimental.pallas import tpu as pltpu
from jax.sharding import PartitionSpec as P

STEP = 2
TILE = 128
LEAD = 8
STATS = 4
LOG2E = 1.4426950408889634


def head_orders(heads):
    half = heads // 2
    singles = [0, heads - 1, heads - 2]
    first = []
    for j in range(half - 1):
        first += [singles[j], j + 1]
    first.append(half)
    return first, [(h + half) % heads for h in first]


def tile_groups(steps, blocks):
    groups = [(u, min(blocks, LEAD - u)) for u in range(0, LEAD, blocks)]
    opening = len(groups)
    for p in range(steps):
        groups += [(LEAD + blocks * p, 1), (LEAD + blocks * p + 1, blocks - 1)]
    sems, last = [], {}
    for n in range(len(groups)):
        done = blocks * ((n - opening) // 2 - 1) - 1 if n >= opening else -1
        free = [sem for sem, end in last.items() if end <= done]
        sem = free[0] if free else len(last)
        sems.append(sem)
        last[sem] = sum(groups[n]) - 1
    return groups, sems


def star_kernel(
    halt_hbm,
    q_hbm,
    k_hbm,
    v_hbm,
    state_hbm,
    w_hbm,
    gain_hbm,
    first_ref,
    left_ref,
    update,
    w_last,
    state_buf,
    gain_buf,
    active_ref,
    halt,
    flag_out,
    flag_in,
    qkv_buf,
    tile_out,
    tile_in,
    far_part,
    stat_out,
    stat_in,
    own_part,
    own_stat,
    att_buf,
    w_buf,
    halt_sem,
    w_sem,
    flag_send,
    flag_recv,
    tile_send,
    stat_send,
    qkv_sem,
    tile_recv,
    stat_recv,
):
    me = lax.axis_index("ctx")
    bits = (me % 2, me // 2)
    peer = (bits[1] * 2 + 1 - bits[0], (1 - bits[1]) * 2 + bits[0])
    heads, rows, width = q_hbm.shape
    features = state_hbm.shape[1]
    half = heads // 2
    steps = heads - 1
    inputs = heads - 2
    blocks = rows // TILE
    meeting = blocks
    scale = width ** (-0.5) * LOG2E
    axes = (0, 1)
    orders = head_orders(heads)
    f32, bf16 = jnp.float32, jnp.bfloat16

    def local(src, dst, sem):
        copy = pltpu.make_async_copy(src, dst, sem)
        copy.start()
        return copy

    def remote(src, dst, send, recv, axis):
        return pltpu.make_async_remote_copy(
            src_ref=src,
            dst_ref=dst,
            send_sem=send,
            recv_sem=recv,
            device_id={"ctx": peer[axis]},
            device_id_type=pl.DeviceIdType.MESH,
        )

    barrier = pltpu.get_barrier_semaphore()
    for axis in axes:
        pl.semaphore_signal(
            barrier, inc=1, device_id={"ctx": peer[axis]}, device_id_type=pl.DeviceIdType.MESH
        )
    halt_copy = local(halt_hbm, halt, halt_sem)

    def choices(b, axis):
        return (0, orders[axis][b]), (1 + b % 2, orders[1 - axis][2 * (b // 2) + 1])

    group_of = {}
    for b in range(blocks):
        for axis in axes:
            for block in choices(b, axis):
                group_of[block] = min(b, 1)
    for block in [(n, h) for h in range(heads) for n in range(3)]:
        group_of.setdefault(block, 2)
    for (n, h), group in group_of.items():
        local((q_hbm, k_hbm, v_hbm)[n].at[h], qkv_buf.at[n * heads + h], qkv_sem.at[group])
    loaded = set()

    def own(n, h):
        group = group_of[n, h]
        if group not in loaded:
            whole = qkv_buf.at[pl.ds(0, list(group_of.values()).count(group))]
            pltpu.make_async_copy(whole, whole, qkv_sem.at[group]).wait()
            loaded.add(group)
        return qkv_buf[n * heads + h]

    halt_copy.wait()
    flag = jnp.full(flag_out.shape, halt[0] > STEP).astype(f32)
    flag_out[...] = flag

    def mask(value):
        return jnp.broadcast_to(value[0:1, :].astype(bf16), (rows, width)) > 0.5

    is_owner = mask(flag)

    def cut_of(tiles):
        return slice(tiles[0] * TILE, (tiles[-1] + 1) * TILE)

    def input_tile(u, axis):
        b, cut = u // blocks, cut_of([u % blocks])
        if b < inputs:
            mine, other = choices(b, axis)
            return jnp.where(is_owner[cut], own(*mine)[cut], own(*other)[cut])
        return jnp.where(is_owner[cut], own(0, orders[axis][b])[cut], far_part[axis, :, cut])

    groups, group_sems = tile_groups(steps, blocks)

    def send(n):
        start, count = groups[n]
        for axis in axes:
            remote(
                tile_out.at[axis, pl.ds(start, count)],
                tile_in.at[axis, pl.ds(start, count)],
                tile_send,
                tile_recv.at[group_sems[n]],
                axis,
            ).start()

    waited = []

    def wait_tiles(u):
        while sum(count for _, count in groups[: len(waited)]) <= u:
            n = len(waited)
            start, count = groups[n]
            landed = tile_in.at[pl.ds(0, 2), pl.ds(start, count)]
            remote(landed, landed, tile_send, tile_recv.at[group_sems[n]], 0).wait_recv()
            waited.append(n)

    known = []

    def wait_stats(p):
        while len(known) <= p:
            n = len(known)
            remote(
                stat_in.at[n], stat_in.at[n], stat_send, stat_recv.at[n % STATS], 0
            ).wait_recv()
            known.append(n)

    for n, (start, count) in enumerate(groups[: len(range(0, LEAD, blocks))]):
        for axis in axes:
            for u in range(start, start + count):
                tile_out[axis, u] = input_tile(u, axis)
        if n == 0:
            pl.semaphore_wait(barrier, 2)
            for axis in axes:
                remote(flag_out, flag_in.at[axis], flag_send, flag_recv, axis).start()
        send(n)

    for side in (0, 1):
        cut = pl.ds(side * width, width)
        local(w_hbm.at[pl.ds(side * half + 1, half - 1)], w_buf.at[:, cut], qkv_sem.at[1])
        local(w_hbm.at[side * half], w_last.at[cut], w_sem)
    state_copy = local(state_hbm, state_buf, qkv_sem.at[0])
    gain_copy = local(gain_hbm, gain_buf, halt_sem)

    remote(flag_in, flag_in, flag_send, flag_recv, 0).wait_recv()
    owner_at = [mask(flag_in[axis]) for axis in axes]
    beside = flag_in[0] + flag_in[1]
    is_beside = mask(beside)

    def bias(valid):
        return jnp.concatenate([(valid[0:1, :] - 1.0) * 1e30] * blocks, axis=1)

    def received(b, axis):
        return tile_in[axis, b * blocks : (b + 1) * blocks].reshape(rows, width)

    def attend(query, keys, values):
        scores = lax.dot_general(
            keys, query, (((1,), (1,)), ((), ())), preferred_element_type=f32
        )
        top = jnp.max(scores, axis=0, keepdims=True)
        weights = jnp.exp2((scores - top) * scale)
        total = jnp.sum(weights, axis=0, keepdims=True)
        weighted = lax.dot_general(
            values, weights.astype(bf16), (((0,), (0,)), ((), ())), preferred_element_type=f32
        )
        return top * scale + jnp.log2(total), weighted * (1.0 / total)

    def merge(sources):
        top = functools.reduce(jnp.maximum, [level for level, _ in sources])
        sums = [jnp.exp2(level - top) for level, _ in sources]
        total = functools.reduce(jnp.add, sums)
        inverse = 1.0 / total
        parts = [part * (each * inverse) for each, (_, part) in zip(sums, sources)]
        return top + jnp.log2(total), functools.reduce(jnp.add, parts)

    def put(p, level, part, query=None):
        part = part.astype(bf16)
        for axis in axes:
            stat_out[p, axis] = level[axis]
            for tile in range(blocks):
                u, cut = LEAD + blocks * p + tile, cut_of([tile])
                piece = part[:, cut]
                if query is not None:
                    piece = jnp.where(owner_at[1 - axis][cut], query[cut], piece)
                if u < steps * blocks:
                    piece = jnp.where(is_beside[cut], piece, input_tile(u, axis))
                tile_out[axis, u] = piece
            remote(
                stat_out.at[p, axis],
                stat_in.at[p, axis],
                stat_send,
                stat_recv.at[p % STATS],
                axis,
            ).start()
        first = len(groups) - 2 * (steps - p)
        send(first)
        send(first + 1)

    def keep(h, result):
        own_stat[h], own_part[h] = result

    def kept(h, tiles=range(blocks)):
        cut = cut_of(tiles)
        return own_stat[h, :, cut], own_part[h, :, cut]

    def sent(p, axis, tiles=range(blocks), start=None):
        start = LEAD + blocks * p if start is None else start
        block = jnp.concatenate([tile_in[axis, start + tile] for tile in tiles], axis=1)
        return stat_in[p, axis, :, cut_of(tiles)], block.astype(f32)

    def select(value, first, second):
        line = jnp.concatenate([value[0:1, :]] * blocks, axis=1)
        return tuple(
            jnp.where(jnp.broadcast_to(line, a.shape) > 0.5, a, b) for a, b in zip(first, second)
        )

    def step(s):
        high, low = orders[0][s], orders[1][s]
        query = jnp.where(
            owner_at[0], received(s, 0), jnp.where(owner_at[1], received(s, 1), own(0, low))
        )
        key = jnp.where(owner_at[0], own(1, high), own(1, low))
        value = jnp.where(owner_at[0], own(2, high), own(2, low))
        if s % 2 == 0:
            result = attend(query, key, value)
            keep(low, result)
            if s == inputs:
                start, p = s * blocks, meeting
                far = select(
                    flag_in[0], sent(p, 1, start=start), sent(p, 0, start=start)
                )
                result = merge((result, far))
            put(s, [result[0]] * 2, result[1], query if s == 0 else None)
            return
        far_key = jnp.where(owner_at[0], received(s - 1, 1), received(s - 1, 0))
        far_value = jnp.where(owner_at[0], received(s, 1), received(s, 0))
        far_query = query
        valid = beside + flag if s == 1 else beside
        if s == meeting:
            one, two = (
                jnp.concatenate([tile_in[axis, LEAD + tile] for tile in range(blocks)], axis=0)
                for axis in axes
            )
            take = mask(flag + beside)
            query = jnp.where(take, query, two)
            key = jnp.where(take, key, own(1, orders[0][0]))
            value = jnp.where(take, value, own(2, orders[0][0]))
            far_query = jnp.where(take, far_query, one)
            far_key = jnp.where(take, far_key, own(1, orders[1][0]))
            far_value = jnp.where(take, far_value, own(2, orders[1][0]))
        nearby = attend(query, key, value)
        distant = attend(far_query, far_key, far_value)
        result = merge((nearby, (distant[0] + bias(valid), distant[1])))
        keep(low, result)
        level = [result[0]] * 2
        if s == meeting:
            for axis, each in enumerate((nearby, distant)):
                far_part[axis] = each[1].astype(bf16)
                level[axis] = select(beside, result[:1], each[:1])[0]
        put(s, level, result[1])
        if s == 1:
            nearby = attend(own(0, high), own(1, high), own(2, high))
            distant = attend(own(0, high), received(s - 1, 1), received(s, 1))
            keep(high, merge((nearby, distant)))

    def combine(i, tiles=range(blocks)):
        for side in (0, 1):
            h = i + side * half
            sources = [kept(h, tiles)]
            for axis in axes:
                if h in orders[axis]:
                    sources.append(sent(orders[axis].index(h), axis, tiles))
            attended = merge(sources)[1]
            att_buf[i, cut_of(tiles), side * width : (side + 1) * width] = attended.T.astype(bf16)

    chunk = min(4 * TILE, features)

    def project(i, initial):
        left = att_buf[i]

        def body(n, carry):
            cut = pl.ds(pl.multiple_of(n * chunk, chunk), chunk)
            product = jnp.dot(left, w_buf[i - 1, :, cut], preferred_element_type=f32)
            if initial:
                update[:, cut] = state_buf[:, cut].astype(f32) + product
            else:
                update[:, cut] = update[:, cut] + product
            return carry

        lax.fori_loop(0, features // chunk, body, 0)

    def result_tile(p, tile):
        return LEAD + blocks * p + tile

    for s in range(steps):
        wait_tiles((s + 1) * blocks - 1)
        wait_stats(meeting if s == inputs else s - 2)
        step(s)
        if s == half:
            pltpu.make_async_copy(w_buf, w_buf, qkv_sem.at[1]).wait()
            pltpu.make_async_copy(w_last, w_last, w_sem).wait()
            state_copy.wait()
            gain_copy.wait()
            wait_stats(1)
            combine(1)
            project(1, True)
    for i in range(2, half - 1):
        p = max(order.index(i) for order in orders)
        wait_tiles(result_tile(p, blocks - 1))
        wait_stats(p)
        combine(i)
        project(i, False)

    i, p, rest = half - 1, steps - 2, list(range(1, blocks))
    for tiles in ([0], rest):
        wait_tiles(result_tile(p, tiles[-1]))
        wait_stats(p)
        combine(i, tiles)
        cut = cut_of(tiles)
        add_product(att_buf[i, cut, :], w_buf.at[i - 1], update.at[cut], update.at[cut])
        for tile in tiles:
            active = jnp.full(active_ref.shape[1:], halt[tile * TILE] > STEP)
            active_ref[tile] = active.astype(f32)

    p = steps - 1
    wait_stats(p)
    wait_tiles(result_tile(p, 0))
    combine(0, [0])
    cut = cut_of([0])
    squares = add_product(att_buf[0, cut, :], w_last, update.at[cut], update.at[cut])
    normalize(squares, update.at[cut], gain_buf, active_ref[0], state_buf.at[cut], first_ref)
    wait_tiles(result_tile(p, blocks - 1))
    combine(0, rest)
    left_ref[...] = att_buf[0, cut_of(rest), :]

    remote(tile_out, tile_in, tile_send, tile_recv.at[0], 0).wait_send()
    remote(stat_out, stat_in, stat_send, stat_recv.at[0], 0).wait_send()
    remote(flag_in, flag_in, flag_send, flag_recv, 0).wait_send()


def strips_of(ref):
    return [slice(n, n + 4 * TILE) for n in range(0, ref.shape[1], 4 * TILE)]


def add_product(left, weight, base, mixed):
    squares = jnp.zeros((left.shape[0], TILE), jnp.float32)
    for strip in strips_of(base):
        product = jnp.dot(left, weight[:, strip], preferred_element_type=jnp.float32)
        total = base[:, strip] + product
        mixed[:, strip] = total
        for n in range(0, total.shape[1], TILE):
            squares = squares + total[:, n : n + TILE] * total[:, n : n + TILE]
    return squares


def normalize(squares, mixed, gain_ref, active, state, out):
    mean = jnp.sum(squares, axis=-1, keepdims=True) / mixed.shape[1]
    inverse = lax.rsqrt(mean + 1e-06)
    chosen = jnp.broadcast_to(active[0:1, :].astype(jnp.bfloat16), (TILE, TILE))
    chosen = jnp.concatenate([chosen] * 4, axis=1) > 0.5
    for strip in strips_of(mixed):
        gain = gain_ref[strip].astype(jnp.float32).reshape(1, -1)
        normed = (mixed[:, strip] * inverse * gain).astype(jnp.bfloat16)
        out[:, strip] = jnp.where(chosen, normed, state[:, strip])


def finish_kernel(
    first_ref, left_ref, update, w_last, state_ref, gain_ref, active_ref, out_hbm, mixed, done, sem
):
    def store(source, tile):
        copy = pltpu.make_async_copy(source, out_hbm.at[pl.ds(tile * TILE, TILE)], sem.at[tile])
        copy.start()
        return copy

    tiles = range(1, 1 + mixed.shape[0] // TILE)
    first = store(first_ref, 0)
    some_active = jnp.max(active_ref[pl.ds(1, len(tiles))]) > 0.5

    @pl.when(some_active)
    def _():
        squares = add_product(left_ref[...], w_last, update.at[pl.ds(TILE, mixed.shape[0])], mixed)
        copies = []
        for tile in tiles:
            cut = pl.ds((tile - 1) * TILE, TILE)
            normalize(
                squares[(tile - 1) * TILE : tile * TILE],
                mixed.at[cut],
                gain_ref,
                active_ref[tile],
                state_ref.at[pl.ds(tile * TILE, TILE)],
                done.at[cut],
            )
            copies.append(store(done.at[cut], tile))
        for copy in copies:
            copy.wait()

    @pl.when(jnp.logical_not(some_active))
    def _():
        copies = [store(state_ref.at[pl.ds(tile * TILE, TILE)], tile) for tile in tiles]
        for copy in copies:
            copy.wait()

    first.wait()


def on_star(state_rows, q, k, v, halt_counts, out_weight, norm_gain):
    heads, rows, width = q.shape
    features = state_rows.shape[1]
    half, blocks, steps = heads // 2, rows // TILE, heads - 1
    tiles = LEAD + steps * blocks
    landings = 1 + max(tile_groups(steps, blocks)[1])
    bf16, f32 = jnp.bfloat16, jnp.float32
    hbm = pl.BlockSpec(memory_space=pltpu.MemorySpace.HBM)
    vmem = pl.BlockSpec(memory_space=pltpu.VMEM)
    dma = pltpu.SemaphoreType.DMA
    operands = (halt_counts, q, k, v, state_rows, out_weight, norm_gain)
    handed = (
        ((TILE, features), bf16),
        ((rows - TILE, 2 * width), bf16),
        ((rows, features), f32),
        ((2 * width, features), bf16),
        ((rows, features), bf16),
        ((features,), bf16),
        ((blocks, 8, TILE), f32),
    )
    results = pl.pallas_call(
        star_kernel,
        out_shape=[jax.ShapeDtypeStruct(*each) for each in handed],
        in_specs=[hbm] * len(operands),
        out_specs=[vmem] * len(handed),
        scratch_shapes=[
            pltpu.SMEM((rows,), jnp.int32),
            pltpu.VMEM((8, width), f32),
            pltpu.VMEM((2, 8, width), f32),
            pltpu.VMEM((3 * heads, rows, width), bf16),
            pltpu.VMEM((2, tiles, TILE, width), bf16),
            pltpu.VMEM((2, tiles, TILE, width), bf16),
            pltpu.VMEM((2, width, rows), bf16),
            pltpu.VMEM((steps, 2, 1, rows), f32),
            pltpu.VMEM((steps, 2, 1, rows), f32),
            pltpu.VMEM((heads, width, rows), f32),
            pltpu.VMEM((heads, 1, rows), f32),
            pltpu.VMEM((half, rows, 2 * width), bf16),
            pltpu.VMEM((half - 1, 2 * width, features), bf16),
            dma,
            dma,
            dma,
            dma,
            dma,
            dma,
            dma((3,)),
            dma((landings,)),
            dma((STATS,)),
        ],
        compiler_params=pltpu.CompilerParams(
            collective_id=0, has_side_effects=True, vmem_limit_bytes=32 * 1024 * 1024
        ),
    )(*[pltpu.with_memory_space_constraint(x, pltpu.HBM) for x in operands])
    return pl.pallas_call(
        finish_kernel,
        out_shape=jax.ShapeDtypeStruct((rows, features), bf16),
        in_specs=[vmem] * len(handed),
        out_specs=hbm,
        scratch_shapes=[
            pltpu.VMEM((rows - TILE, features), f32),
            pltpu.VMEM((rows - TILE, features), bf16),
            dma((blocks,)),
        ],
        compiler_params=pltpu.CompilerParams(vmem_limit_bytes=8 * 1024 * 1024),
    )(*results)


def fold_heads(carry, queries, key_piece, value_piece, score_scale):
    running_max, running_sum, weighted = carry

    def per_head(head_items):
        query_head, key_head, value_head, max_head, sum_head, weighted_head = head_items
        scores = (
            lax.dot_general(
                query_head, key_head, (((1,), (1,)), ((), ())), preferred_element_type=jnp.float32
            )
            * score_scale
        )
        new_max = jnp.maximum(max_head, jnp.max(scores, axis=1))
        shrink = jnp.exp(max_head - new_max)
        exponents = jnp.exp(scores - new_max[:, None])
        sum_head = sum_head * shrink + jnp.sum(exponents, axis=1)
        weighted_head = weighted_head * shrink[:, None] + jnp.dot(
            exponents.astype(jnp.bfloat16), value_head, preferred_element_type=jnp.float32
        )
        return (new_max, sum_head, weighted_head)

    return lax.map(per_head, (queries, key_piece, value_piece, running_max, running_sum, weighted))


def empty_carry(head_count, query_count, head_width):
    return (
        jnp.full((head_count, query_count), -1e30, jnp.float32),
        jnp.zeros((head_count, query_count), jnp.float32),
        jnp.zeros((head_count, query_count, head_width), jnp.float32),
    )


def attend_keys(query_vectors, key_vectors, value_vectors, score_scale):
    head_count, row_count, head_width = query_vectors.shape
    initial = empty_carry(head_count, row_count, head_width)
    running_max, running_sum, weighted = fold_heads(
        initial,
        query_vectors,
        lax.all_gather(key_vectors, "ctx", axis=1, tiled=True),
        lax.all_gather(value_vectors, "ctx", axis=1, tiled=True),
        score_scale,
    )
    return (weighted / running_sum[..., None]).astype(jnp.bfloat16)


def on_device(
    state_rows, query_vectors, key_vectors, value_vectors, halt_counts, out_weight, norm_gain
):
    head_count, row_count, head_width = query_vectors.shape
    score_scale = head_width ** (-0.5)
    attended = attend_keys(query_vectors, key_vectors, value_vectors, score_scale)
    update = jnp.einsum("hqd,hde->qe", attended, out_weight, preferred_element_type=jnp.float32)
    mixed_sum = state_rows.astype(jnp.float32) + update
    normed = (
        mixed_sum
        * lax.rsqrt(jnp.mean(mixed_sum * mixed_sum, axis=-1, keepdims=True) + 1e-06)
        * norm_gain.astype(jnp.float32)
    )
    active = (halt_counts > STEP)[:, None]
    return jnp.where(active, normed.astype(jnp.bfloat16), state_rows)


def solution(mesh):
    n_ctx = mesh.shape["ctx"]

    def per_device(state_rows, q, k, v, halt_counts, out_weight, norm_gain):
        heads, rows, width = q.shape
        one_owner = rows == (n_ctx - 1) * TILE
        if one_owner and heads == LEAD and width == TILE and n_ctx == 4:
            return on_star(state_rows, q, k, v, halt_counts, out_weight, norm_gain)
        return on_device(state_rows, q, k, v, halt_counts, out_weight, norm_gain)

    placed = (
        P(("dp", "ctx"), None),
        P(None, ("dp", "ctx"), None),
        P(None, ("dp", "ctx"), None),
        P(None, ("dp", "ctx"), None),
        P(("dp", "ctx")),
        P(),
        P(),
    )
    return jax.shard_map(
        per_device, mesh=mesh, in_specs=placed, out_specs=P(("dp", "ctx"), None), check_vma=False
    )
```

```python
import functools

import jax
import jax.numpy as jnp
from jax import lax
from jax.experimental import pallas as pl
from jax.experimental.pallas import tpu as pltpu
from jax.sharding import PartitionSpec as P

STEP = 2
TILE = 128
LEAD = 8
STATS = 4
LOG2E = 1.4426950408889634


def head_orders(heads):
    half = heads // 2
    singles = [0, heads - 1, heads - 2]
    first = []
    for j in range(half - 1):
        first += [singles[j], j + 1]
    first.append(half)
    return first, [(h + half) % heads for h in first]


def tile_groups(steps, blocks):
    groups = [(u, min(blocks, LEAD - u)) for u in range(0, LEAD, blocks)]
    opening = len(groups)
    for p in range(steps):
        groups += [(LEAD + blocks * p, 1), (LEAD + blocks * p + 1, blocks - 1)]
    sems, last = [], {}
    for n in range(len(groups)):
        done = blocks * ((n - opening) // 2 - 1) - 1 if n >= opening else -1
        free = [sem for sem, end in last.items() if end <= done]
        sem = free[0] if free else len(last)
        sems.append(sem)
        last[sem] = sum(groups[n]) - 1
    return groups, sems


def star_kernel(
    halt_hbm,
    q_hbm,
    k_hbm,
    v_hbm,
    state_hbm,
    w_hbm,
    gain_hbm,
    first_ref,
    left_ref,
    update,
    w_last,
    state_buf,
    gain_buf,
    active_ref,
    halt,
    flag_out,
    flag_in,
    qkv_buf,
    tile_out,
    tile_in,
    far_part,
    stat_out,
    stat_in,
    own_part,
    own_stat,
    att_buf,
    w_buf,
    halt_sem,
    w_sem,
    flag_send,
    flag_recv,
    tile_send,
    stat_send,
    qkv_sem,
    tile_recv,
    stat_recv,
):
    me = lax.axis_index("ctx")
    bits = (me % 2, me // 2)
    peer = (bits[1] * 2 + 1 - bits[0], (1 - bits[1]) * 2 + bits[0])
    heads, rows, width = q_hbm.shape
    features = state_hbm.shape[1]
    half = heads // 2
    steps = heads - 1
    inputs = heads - 2
    blocks = rows // TILE
    meeting = blocks
    scale = width ** (-0.5) * LOG2E
    axes = (0, 1)
    orders = head_orders(heads)
    f32, bf16 = jnp.float32, jnp.bfloat16

    def local(src, dst, sem):
        copy = pltpu.make_async_copy(src, dst, sem)
        copy.start()
        return copy

    def remote(src, dst, send, recv, axis):
        return pltpu.make_async_remote_copy(
            src_ref=src,
            dst_ref=dst,
            send_sem=send,
            recv_sem=recv,
            device_id={"ctx": peer[axis]},
            device_id_type=pl.DeviceIdType.MESH,
        )

    barrier = pltpu.get_barrier_semaphore()
    for axis in axes:
        pl.semaphore_signal(
            barrier, inc=1, device_id={"ctx": peer[axis]}, device_id_type=pl.DeviceIdType.MESH
        )
    halt_copy = local(halt_hbm, halt, halt_sem)

    def choices(b, axis):
        return (0, orders[axis][b]), (1 + b % 2, orders[1 - axis][2 * (b // 2) + 1])

    group_of = {}
    for b in range(blocks):
        for axis in axes:
            for block in choices(b, axis):
                group_of[block] = min(b, 1)
    for block in [(n, h) for h in range(heads) for n in range(3)]:
        group_of.setdefault(block, 2)
    for (n, h), group in group_of.items():
        local((q_hbm, k_hbm, v_hbm)[n].at[h], qkv_buf.at[n * heads + h], qkv_sem.at[group])
    loaded = set()

    def own(n, h):
        group = group_of[n, h]
        if group not in loaded:
            whole = qkv_buf.at[pl.ds(0, list(group_of.values()).count(group))]
            pltpu.make_async_copy(whole, whole, qkv_sem.at[group]).wait()
            loaded.add(group)
        return qkv_buf[n * heads + h]

    halt_copy.wait()
    flag = jnp.full(flag_out.shape, halt[0] > STEP).astype(f32)
    flag_out[...] = flag

    def mask(value):
        return jnp.broadcast_to(value[0:1, :].astype(bf16), (rows, width)) > 0.5

    is_owner = mask(flag)

    def cut_of(tiles):
        return slice(tiles[0] * TILE, (tiles[-1] + 1) * TILE)

    def input_tile(u, axis):
        b, cut = u // blocks, cut_of([u % blocks])
        if b < inputs:
            mine, other = choices(b, axis)
            return jnp.where(is_owner[cut], own(*mine)[cut], own(*other)[cut])
        return jnp.where(is_owner[cut], own(0, orders[axis][b])[cut], far_part[axis, :, cut])

    groups, group_sems = tile_groups(steps, blocks)

    def send(n):
        start, count = groups[n]
        for axis in axes:
            remote(
                tile_out.at[axis, pl.ds(start, count)],
                tile_in.at[axis, pl.ds(start, count)],
                tile_send,
                tile_recv.at[group_sems[n]],
                axis,
            ).start()

    waited = []

    def wait_tiles(u):
        while sum(count for _, count in groups[: len(waited)]) <= u:
            n = len(waited)
            start, count = groups[n]
            landed = tile_in.at[pl.ds(0, 2), pl.ds(start, count)]
            remote(landed, landed, tile_send, tile_recv.at[group_sems[n]], 0).wait_recv()
            waited.append(n)

    known = []

    def wait_stats(p):
        while len(known) <= p:
            n = len(known)
            remote(
                stat_in.at[n], stat_in.at[n], stat_send, stat_recv.at[n % STATS], 0
            ).wait_recv()
            known.append(n)

    for n, (start, count) in enumerate(groups[: len(range(0, LEAD, blocks))]):
        for axis in axes:
            for u in range(start, start + count):
                tile_out[axis, u] = input_tile(u, axis)
        if n == 0:
            pl.semaphore_wait(barrier, 2)
            for axis in axes:
                remote(flag_out, flag_in.at[axis], flag_send, flag_recv, axis).start()
        send(n)

    for side in (0, 1):
        cut = pl.ds(side * width, width)
        local(w_hbm.at[pl.ds(side * half + 1, half - 1)], w_buf.at[:, cut], qkv_sem.at[1])
        local(w_hbm.at[side * half], w_last.at[cut], w_sem)
    state_copy = local(state_hbm, state_buf, qkv_sem.at[0])
    gain_copy = local(gain_hbm, gain_buf, halt_sem)

    remote(flag_in, flag_in, flag_send, flag_recv, 0).wait_recv()
    owner_at = [mask(flag_in[axis]) for axis in axes]
    beside = flag_in[0] + flag_in[1]
    is_beside = mask(beside)

    def bias(valid):
        return jnp.concatenate([(valid[0:1, :] - 1.0) * 1e30] * blocks, axis=1)

    def received(b, axis):
        return tile_in[axis, b * blocks : (b + 1) * blocks].reshape(rows, width)

    def attend(query, keys, values):
        scores = lax.dot_general(
            keys, query, (((1,), (1,)), ((), ())), preferred_element_type=f32
        )
        top = jnp.max(scores, axis=0, keepdims=True)
        weights = jnp.exp2((scores - top) * scale)
        total = jnp.sum(weights, axis=0, keepdims=True)
        weighted = lax.dot_general(
            values, weights.astype(bf16), (((0,), (0,)), ((), ())), preferred_element_type=f32
        )
        return top * scale + jnp.log2(total), weighted * (1.0 / total)

    def merge(sources):
        top = functools.reduce(jnp.maximum, [level for level, _ in sources])
        sums = [jnp.exp2(level - top) for level, _ in sources]
        total = functools.reduce(jnp.add, sums)
        inverse = 1.0 / total
        parts = [part * (each * inverse) for each, (_, part) in zip(sums, sources)]
        return top + jnp.log2(total), functools.reduce(jnp.add, parts)

    def put(p, level, part, query=None):
        part = part.astype(bf16)
        for axis in axes:
            stat_out[p, axis] = level[axis]
            for tile in range(blocks):
                u, cut = LEAD + blocks * p + tile, cut_of([tile])
                piece = part[:, cut]
                if query is not None:
                    piece = jnp.where(owner_at[1 - axis][cut], query[cut], piece)
                if u < steps * blocks:
                    piece = jnp.where(is_beside[cut], piece, input_tile(u, axis))
                tile_out[axis, u] = piece
            remote(
                stat_out.at[p, axis],
                stat_in.at[p, axis],
                stat_send,
                stat_recv.at[p % STATS],
                axis,
            ).start()
        first = len(groups) - 2 * (steps - p)
        send(first)
        send(first + 1)

    def keep(h, result):
        own_stat[h], own_part[h] = result

    def kept(h, tiles=range(blocks)):
        cut = cut_of(tiles)
        return own_stat[h, :, cut], own_part[h, :, cut]

    def sent(p, axis, tiles=range(blocks), start=None):
        start = LEAD + blocks * p if start is None else start
        block = jnp.concatenate([tile_in[axis, start + tile] for tile in tiles], axis=1)
        return stat_in[p, axis, :, cut_of(tiles)], block.astype(f32)

    def select(value, first, second):
        line = jnp.concatenate([value[0:1, :]] * blocks, axis=1)
        return tuple(
            jnp.where(jnp.broadcast_to(line, a.shape) > 0.5, a, b) for a, b in zip(first, second)
        )

    def step(s):
        high, low = orders[0][s], orders[1][s]
        query = jnp.where(
            owner_at[0], received(s, 0), jnp.where(owner_at[1], received(s, 1), own(0, low))
        )
        key = jnp.where(owner_at[0], own(1, high), own(1, low))
        value = jnp.where(owner_at[0], own(2, high), own(2, low))
        if s % 2 == 0:
            result = attend(query, key, value)
            keep(low, result)
            if s == inputs:
                start, p = s * blocks, meeting
                far = select(
                    flag_in[0], sent(p, 1, start=start), sent(p, 0, start=start)
                )
                result = merge((result, far))
            put(s, [result[0]] * 2, result[1], query if s == 0 else None)
            return
        far_key = jnp.where(owner_at[0], received(s - 1, 1), received(s - 1, 0))
        far_value = jnp.where(owner_at[0], received(s, 1), received(s, 0))
        far_query = query
        valid = beside + flag if s == 1 else beside
        if s == meeting:
            one, two = (
                jnp.concatenate([tile_in[axis, LEAD + tile] for tile in range(blocks)], axis=0)
                for axis in axes
            )
            take = mask(flag + beside)
            query = jnp.where(take, query, two)
            key = jnp.where(take, key, own(1, orders[0][0]))
            value = jnp.where(take, value, own(2, orders[0][0]))
            far_query = jnp.where(take, far_query, one)
            far_key = jnp.where(take, far_key, own(1, orders[1][0]))
            far_value = jnp.where(take, far_value, own(2, orders[1][0]))
        nearby = attend(query, key, value)
        distant = attend(far_query, far_key, far_value)
        result = merge((nearby, (distant[0] + bias(valid), distant[1])))
        keep(low, result)
        level = [result[0]] * 2
        if s == meeting:
            for axis, each in enumerate((nearby, distant)):
                far_part[axis] = each[1].astype(bf16)
                level[axis] = select(beside, result[:1], each[:1])[0]
        put(s, level, result[1])
        if s == 1:
            nearby = attend(own(0, high), own(1, high), own(2, high))
            distant = attend(own(0, high), received(s - 1, 1), received(s, 1))
            keep(high, merge((nearby, distant)))

    def combine(i, tiles=range(blocks)):
        for side in (0, 1):
            h = i + side * half
            sources = [kept(h, tiles)]
            for axis in axes:
                if h in orders[axis]:
                    sources.append(sent(orders[axis].index(h), axis, tiles))
            attended = merge(sources)[1]
            att_buf[i, cut_of(tiles), side * width : (side + 1) * width] = attended.T.astype(bf16)

    chunk = min(4 * TILE, features)

    def project(i, initial):
        left = att_buf[i]

        def body(n, carry):
            cut = pl.ds(pl.multiple_of(n * chunk, chunk), chunk)
            product = jnp.dot(left, w_buf[i - 1, :, cut], preferred_element_type=f32)
            if initial:
                update[:, cut] = state_buf[:, cut].astype(f32) + product
            else:
                update[:, cut] = update[:, cut] + product
            return carry

        lax.fori_loop(0, features // chunk, body, 0)

    def result_tile(p, tile):
        return LEAD + blocks * p + tile

    for s in range(steps):
        wait_tiles((s + 1) * blocks - 1)
        wait_stats(meeting if s == inputs else s - 2)
        step(s)
        if s == half:
            pltpu.make_async_copy(w_buf, w_buf, qkv_sem.at[1]).wait()
            pltpu.make_async_copy(w_last, w_last, w_sem).wait()
            state_copy.wait()
            gain_copy.wait()
            wait_stats(1)
            combine(1)
            project(1, True)
    for i in range(2, half - 1):
        p = max(order.index(i) for order in orders)
        wait_tiles(result_tile(p, blocks - 1))
        wait_stats(p)
        combine(i)
        project(i, False)

    i, p, rest = half - 1, steps - 2, list(range(1, blocks))
    for tiles in ([0], rest):
        wait_tiles(result_tile(p, tiles[-1]))
        wait_stats(p)
        combine(i, tiles)
        cut = cut_of(tiles)
        add_product(att_buf[i, cut, :], w_buf.at[i - 1], update.at[cut], update.at[cut])
        for tile in tiles:
            active = jnp.full(active_ref.shape[1:], halt[tile * TILE] > STEP)
            active_ref[tile] = active.astype(f32)

    p = steps - 1
    wait_stats(p)
    wait_tiles(result_tile(p, 0))
    combine(0, [0])
    cut = cut_of([0])
    squares = add_product(att_buf[0, cut, :], w_last, update.at[cut], update.at[cut])
    normalize(squares, update.at[cut], gain_buf, active_ref[0], state_buf.at[cut], first_ref)
    wait_tiles(result_tile(p, blocks - 1))
    combine(0, rest)
    left_ref[...] = att_buf[0, cut_of(rest), :]

    remote(tile_out, tile_in, tile_send, tile_recv.at[0], 0).wait_send()
    remote(stat_out, stat_in, stat_send, stat_recv.at[0], 0).wait_send()
    remote(flag_in, flag_in, flag_send, flag_recv, 0).wait_send()


def strips_of(ref):
    return [slice(n, n + 4 * TILE) for n in range(0, ref.shape[1], 4 * TILE)]


def add_product(left, weight, base, mixed):
    squares = jnp.zeros((left.shape[0], TILE), jnp.float32)
    for strip in strips_of(base):
        product = jnp.dot(left, weight[:, strip], preferred_element_type=jnp.float32)
        total = base[:, strip] + product
        mixed[:, strip] = total
        for n in range(0, total.shape[1], TILE):
            squares = squares + total[:, n : n + TILE] * total[:, n : n + TILE]
    return squares


def normalize(squares, mixed, gain_ref, active, state, out):
    mean = jnp.sum(squares, axis=-1, keepdims=True) / mixed.shape[1]
    inverse = lax.rsqrt(mean + 1e-06)
    chosen = jnp.broadcast_to(active[0:1, :].astype(jnp.bfloat16), (TILE, TILE))
    chosen = jnp.concatenate([chosen] * 4, axis=1) > 0.5
    for strip in strips_of(mixed):
        gain = gain_ref[strip].astype(jnp.float32).reshape(1, -1)
        normed = (mixed[:, strip] * inverse * gain).astype(jnp.bfloat16)
        out[:, strip] = jnp.where(chosen, normed, state[:, strip])


def finish_kernel(
    first_ref, left_ref, update, w_last, state_ref, gain_ref, active_ref, out_hbm, mixed, done, sem
):
    def store(source, tile):
        copy = pltpu.make_async_copy(source, out_hbm.at[pl.ds(tile * TILE, TILE)], sem.at[tile])
        copy.start()
        return copy

    tiles = range(1, 1 + mixed.shape[0] // TILE)
    first = store(first_ref, 0)
    some_active = jnp.max(active_ref[pl.ds(1, len(tiles))]) > 0.5

    @pl.when(some_active)
    def _():
        squares = add_product(left_ref[...], w_last, update.at[pl.ds(TILE, mixed.shape[0])], mixed)
        copies = []
        for tile in tiles:
            cut = pl.ds((tile - 1) * TILE, TILE)
            normalize(
                squares[(tile - 1) * TILE : tile * TILE],
                mixed.at[cut],
                gain_ref,
                active_ref[tile],
                state_ref.at[pl.ds(tile * TILE, TILE)],
                done.at[cut],
            )
            copies.append(store(done.at[cut], tile))
        for copy in copies:
            copy.wait()

    @pl.when(jnp.logical_not(some_active))
    def _():
        copies = [store(state_ref.at[pl.ds(tile * TILE, TILE)], tile) for tile in tiles]
        for copy in copies:
            copy.wait()

    first.wait()


def on_star(state_rows, q, k, v, halt_counts, out_weight, norm_gain):
    heads, rows, width = q.shape
    features = state_rows.shape[1]
    half, blocks, steps = heads // 2, rows // TILE, heads - 1
    tiles = LEAD + steps * blocks
    landings = 1 + max(tile_groups(steps, blocks)[1])
    bf16, f32 = jnp.bfloat16, jnp.float32
    hbm = pl.BlockSpec(memory_space=pltpu.MemorySpace.HBM)
    vmem = pl.BlockSpec(memory_space=pltpu.VMEM)
    dma = pltpu.SemaphoreType.DMA
    operands = (halt_counts, q, k, v, state_rows, out_weight, norm_gain)
    handed = (
        ((TILE, features), bf16),
        ((rows - TILE, 2 * width), bf16),
        ((rows, features), f32),
        ((2 * width, features), bf16),
        ((rows, features), bf16),
        ((features,), bf16),
        ((blocks, 8, TILE), f32),
    )
    results = pl.pallas_call(
        star_kernel,
        out_shape=[jax.ShapeDtypeStruct(*each) for each in handed],
        in_specs=[hbm] * len(operands),
        out_specs=[vmem] * len(handed),
        scratch_shapes=[
            pltpu.SMEM((rows,), jnp.int32),
            pltpu.VMEM((1, width), f32),
            pltpu.VMEM((2, 1, width), f32),
            pltpu.VMEM((3 * heads, rows, width), bf16),
            pltpu.VMEM((2, tiles, TILE, width), bf16),
            pltpu.VMEM((2, tiles, TILE, width), bf16),
            pltpu.VMEM((2, width, rows), bf16),
            pltpu.VMEM((steps, 2, 1, rows), f32),
            pltpu.VMEM((steps, 2, 1, rows), f32),
            pltpu.VMEM((heads, width, rows), f32),
            pltpu.VMEM((heads, 1, rows), f32),
            pltpu.VMEM((half, rows, 2 * width), bf16),
            pltpu.VMEM((half - 1, 2 * width, features), bf16),
            dma,
            dma,
            dma,
            dma,
            dma,
            dma,
            dma((3,)),
            dma((landings,)),
            dma((STATS,)),
        ],
        compiler_params=pltpu.CompilerParams(
            collective_id=0, has_side_effects=True, vmem_limit_bytes=32 * 1024 * 1024
        ),
    )(*[pltpu.with_memory_space_constraint(x, pltpu.HBM) for x in operands])
    return pl.pallas_call(
        finish_kernel,
        out_shape=jax.ShapeDtypeStruct((rows, features), bf16),
        in_specs=[vmem] * len(handed),
        out_specs=hbm,
        scratch_shapes=[
            pltpu.VMEM((rows - TILE, features), f32),
            pltpu.VMEM((rows - TILE, features), bf16),
            dma((blocks,)),
        ],
        compiler_params=pltpu.CompilerParams(vmem_limit_bytes=8 * 1024 * 1024),
    )(*results)


def fold_heads(carry, queries, key_piece, value_piece, score_scale):
    running_max, running_sum, weighted = carry

    def per_head(head_items):
        query_head, key_head, value_head, max_head, sum_head, weighted_head = head_items
        scores = (
            lax.dot_general(
                query_head, key_head, (((1,), (1,)), ((), ())), preferred_element_type=jnp.float32
            )
            * score_scale
        )
        new_max = jnp.maximum(max_head, jnp.max(scores, axis=1))
        shrink = jnp.exp(max_head - new_max)
        exponents = jnp.exp(scores - new_max[:, None])
        sum_head = sum_head * shrink + jnp.sum(exponents, axis=1)
        weighted_head = weighted_head * shrink[:, None] + jnp.dot(
            exponents.astype(jnp.bfloat16), value_head, preferred_element_type=jnp.float32
        )
        return (new_max, sum_head, weighted_head)

    return lax.map(per_head, (queries, key_piece, value_piece, running_max, running_sum, weighted))


def empty_carry(head_count, query_count, head_width):
    return (
        jnp.full((head_count, query_count), -1e30, jnp.float32),
        jnp.zeros((head_count, query_count), jnp.float32),
        jnp.zeros((head_count, query_count, head_width), jnp.float32),
    )


def attend_keys(query_vectors, key_vectors, value_vectors, score_scale):
    head_count, row_count, head_width = query_vectors.shape
    initial = empty_carry(head_count, row_count, head_width)
    running_max, running_sum, weighted = fold_heads(
        initial,
        query_vectors,
        lax.all_gather(key_vectors, "ctx", axis=1, tiled=True),
        lax.all_gather(value_vectors, "ctx", axis=1, tiled=True),
        score_scale,
    )
    return (weighted / running_sum[..., None]).astype(jnp.bfloat16)


def on_device(
    state_rows, query_vectors, key_vectors, value_vectors, halt_counts, out_weight, norm_gain
):
    head_count, row_count, head_width = query_vectors.shape
    score_scale = head_width ** (-0.5)
    attended = attend_keys(query_vectors, key_vectors, value_vectors, score_scale)
    update = jnp.einsum("hqd,hde->qe", attended, out_weight, preferred_element_type=jnp.float32)
    mixed_sum = state_rows.astype(jnp.float32) + update
    normed = (
        mixed_sum
        * lax.rsqrt(jnp.mean(mixed_sum * mixed_sum, axis=-1, keepdims=True) + 1e-06)
        * norm_gain.astype(jnp.float32)
    )
    active = (halt_counts > STEP)[:, None]
    return jnp.where(active, normed.astype(jnp.bfloat16), state_rows)


def solution(mesh):
    n_ctx = mesh.shape["ctx"]

    def per_device(state_rows, q, k, v, halt_counts, out_weight, norm_gain):
        heads, rows, width = q.shape
        one_owner = rows == (n_ctx - 1) * TILE
        if one_owner and heads == LEAD and width == TILE and n_ctx == 4:
            return on_star(state_rows, q, k, v, halt_counts, out_weight, norm_gain)
        return on_device(state_rows, q, k, v, halt_counts, out_weight, norm_gain)

    placed = (
        P(("dp", "ctx"), None),
        P(None, ("dp", "ctx"), None),
        P(None, ("dp", "ctx"), None),
        P(None, ("dp", "ctx"), None),
        P(("dp", "ctx")),
        P(),
        P(),
    )
    return jax.shard_map(
        per_device, mesh=mesh, in_specs=placed, out_specs=P(("dp", "ctx"), None), check_vma=False
    )
```
